16 devices in a mesh: replica: 2 (over y, z), model: 8 (over x, core).
Axes of the slice: x: 4, y: 2, z: 1, core: 2. Of those that a mesh axis runs over, the one named last changes fastest.
The devices are a block of a 4x4x8 slice.
Arguments:
- x: bfloat16 [256, 4096], P('replica'), parts along dimension 0
- cache_len: int32 [256], P('replica'), parts along dimension 0
- w_query: bfloat16 [2, 4096, 4096], P(None, None, 'model')
- w_key: bfloat16 [2, 4096, 128], replicated
- w_value: bfloat16 [2, 4096, 128], replicated
- w_out: bfloat16 [2, 4096, 4096], P(None, 'model')
- k_cache: bfloat16 [2, 256, 2048, 128], P(None, ('replica', 'model')), parts along dimension 1
- v_cache: bfloat16 [2, 256, 2048, 128], P(None, ('replica', 'model')), parts along dimension 1
Outputs:
- output 1: bfloat16 [256, 4096], P('replica'), parts along dimension 0
- output 2: bfloat16 [2, 256, 2048, 128], P(None, ('replica', 'model')), parts along dimension 1
- output 3: bfloat16 [2, 256, 2048, 128], P(None, ('replica', 'model')), parts along dimension 1
There are 2 independent parts. The reference program is written for one: setup_inputs(seed, part) draws one part's arguments, and reference() takes and returns one part's arrays. A program takes and returns all parts, laid end to end along the dimension named above; an argument that names none is the same for every part.
All inputs are finite; a program needn't handle non-finite values.
Results may differ from the reference program's by a relative error of at most 0.0044712.
Values are sent between devices in bfloat16 or wider.
A program may use at most 768 MiB of HBM per device.

```python
import jax
import jax.numpy as jnp
from jax import lax

LAYERS = 2
BATCH = 128
D_MODEL = 4096
NUM_HEADS = 32
HEAD_DIM = 128
SEQ_LEN = 2048

SEQ_BITS = SEQ_LEN.bit_length() - 1
Q_WIDTH = NUM_HEADS * HEAD_DIM


def setup_inputs(seed: int = 0, part: int = 0) -> dict:
    root_key = jax.random.key(seed)
    shared = jax.random.split(root_key, 4)
    part_keys = jax.random.split(jax.random.fold_in(root_key, part), 6)
    x = jax.random.normal(part_keys[0], (BATCH, D_MODEL), jnp.float32).astype(jnp.bfloat16)
    raw_len = jax.random.randint(part_keys[1], (BATCH,), 0, SEQ_LEN)
    shift_by = jax.random.randint(part_keys[2], (BATCH,), 0, SEQ_BITS + 1)
    row_order = jax.random.permutation(part_keys[3], BATCH)
    cache_len = jnp.right_shift(raw_len, shift_by)
    cache_len = cache_len.at[row_order[0]].set(SEQ_LEN - 1).at[row_order[1]].set(0)
    w_query = (1.5 * D_MODEL ** -0.5) * jax.random.normal(shared[0], (LAYERS, D_MODEL, Q_WIDTH), jnp.float32)
    w_key = (1.5 * D_MODEL ** -0.5) * jax.random.normal(shared[1], (LAYERS, D_MODEL, HEAD_DIM), jnp.float32)
    w_value = (D_MODEL ** -0.5) * jax.random.normal(shared[2], (LAYERS, D_MODEL, HEAD_DIM), jnp.float32)
    w_out = (2.0 * Q_WIDTH ** -0.5) * jax.random.normal(shared[3], (LAYERS, Q_WIDTH, D_MODEL), jnp.float32)
    k_cache = 1.5 * jax.random.normal(part_keys[4], (LAYERS, BATCH, SEQ_LEN, HEAD_DIM), jnp.float32)
    v_cache = jax.random.normal(part_keys[5], (LAYERS, BATCH, SEQ_LEN, HEAD_DIM), jnp.float32)
    return {
        "x": x,
        "cache_len": cache_len,
        "w_query": w_query.astype(jnp.bfloat16),
        "w_key": w_key.astype(jnp.bfloat16),
        "w_value": w_value.astype(jnp.bfloat16),
        "w_out": w_out.astype(jnp.bfloat16),
        "k_cache": k_cache.astype(jnp.bfloat16),
        "v_cache": v_cache.astype(jnp.bfloat16),
    }


def attend_layer(hidden, cache_len, query_w, key_w, value_w, out_w, k_layer, v_layer):
    query = jnp.dot(hidden, query_w, preferred_element_type=jnp.float32).astype(jnp.bfloat16)
    query = query.reshape(BATCH, NUM_HEADS, HEAD_DIM)
    k_new = jnp.dot(hidden, key_w, preferred_element_type=jnp.float32).astype(jnp.bfloat16)
    v_new = jnp.dot(hidden, value_w, preferred_element_type=jnp.float32).astype(jnp.bfloat16)
    write_here = jnp.arange(SEQ_LEN)[None, :, None] == cache_len[:, None, None]
    k_layer = jnp.where(write_here, k_new[:, None, :], k_layer)
    v_layer = jnp.where(write_here, v_new[:, None, :], v_layer)

    def one_row(row_items):
        q_row, k_row, v_row, row_len = row_items
        scores = jnp.dot(q_row, k_row.T, preferred_element_type=jnp.float32) * (HEAD_DIM ** -0.5)
        visible = jnp.arange(SEQ_LEN)[None, :] <= row_len
        scores = jnp.where(visible, scores, -jnp.inf)
        weights = jax.nn.softmax(scores, axis=-1).astype(jnp.bfloat16)
        context = jnp.dot(weights, v_row, preferred_element_type=jnp.float32)
        return context.astype(jnp.bfloat16)

    context = lax.map(one_row, (query, k_layer, v_layer, cache_len))
    update = jnp.dot(context.reshape(BATCH, Q_WIDTH), out_w, preferred_element_type=jnp.float32)
    hidden = (hidden.astype(jnp.float32) + update).astype(jnp.bfloat16)
    return hidden, k_layer, v_layer


def reference(x, cache_len, w_query, w_key, w_value, w_out, k_cache, v_cache):
    def layer_step(hidden, params):
        query_w, key_w, value_w, out_w, k_layer, v_layer = params
        hidden, k_layer, v_layer = attend_layer(hidden, cache_len, query_w, key_w, value_w, out_w, k_layer, v_layer)
        return hidden, (k_layer, v_layer)

    out, (k_all, v_all) = lax.scan(layer_step, x, (w_query, w_key, w_value, w_out, k_cache, v_cache))
    return out, k_all, v_all
```

```python
import functools

import jax
import jax.numpy as jnp
from jax import lax
from jax.experimental import pallas as pl
from jax.experimental.pallas import tpu as pltpu
from jax.sharding import PartitionSpec as P

MESH = pl.DeviceIdType.MESH
F32 = jnp.float32
BF16 = jnp.bfloat16
CHIPS = 4
CHUNKS = 4
MIB = 1 << 20

ANY_SPEC = pl.BlockSpec(memory_space=pltpu.HBM)
VMEM_SPEC = pl.BlockSpec(memory_space=pltpu.VMEM)
SMEM_SPEC = pl.BlockSpec(memory_space=pltpu.SMEM)


def to_hbm(value):
    return pltpu.with_memory_space_constraint(value, pltpu.HBM)


def to_vmem(value):
    return pltpu.with_memory_space_constraint(value, pltpu.VMEM)


def aligned(index, size):
    return pl.ds(pl.multiple_of(index * size, size), size)


class Place:
    def __init__(self, count):
        self.count = count
        self.me = lax.axis_index("model")
        self.chip = self.me // 2
        self.core = self.me % 2
        self.right = (self.chip + 1) % CHIPS
        self.left = (self.chip + CHIPS - 1) % CHIPS
        self.across = (self.chip + 2) % CHIPS
        self.to_right = self.right * 2 + self.core
        self.to_left = self.left * 2 + self.core
        self.sibling = self.chip * 2 + (1 - self.core)

    def peer(self, offset):
        return (self.me + offset) % self.count

    def origin(self, offset):
        return (self.me + self.count - offset) % self.count


def remote(src, dst, send_sem, recv_sem, device):
    return pltpu.make_async_remote_copy(
        src_ref=src, dst_ref=dst, send_sem=send_sem, recv_sem=recv_sem,
        device_id={"model": device}, device_id_type=MESH)


def signal_all(place):
    barrier = pltpu.get_barrier_semaphore()
    for offset in range(1, place.count):
        pl.semaphore_signal(barrier, inc=1, device_id={"model": place.peer(offset)}, device_id_type=MESH)


def wait_all(place):
    pl.semaphore_wait(pltpu.get_barrier_semaphore(), place.count - 1)


def weight_copies(layer, wq, wk, wv, wq_buf, wkv_buf, sems):
    pieces = sems.shape[0] - 2
    depth = wq_buf.shape[0] // pieces
    head_dim = wk.shape[-1]
    copies = [
        pltpu.make_async_copy(wq.at[layer, pl.ds(i * depth, depth), :], wq_buf.at[pl.ds(i * depth, depth), :], sems.at[i])
        for i in range(pieces)
    ]
    copies.append(pltpu.make_async_copy(wk.at[layer], wkv_buf.at[:, pl.ds(0, head_dim)], sems.at[pieces]))
    copies.append(pltpu.make_async_copy(wv.at[layer], wkv_buf.at[:, pl.ds(head_dim, head_dim)], sems.at[pieces + 1]))
    return copies


def add_query(piece, first, hidden, wq_buf, q_acc):
    depth = hidden.shape[-1]
    part = jnp.dot(hidden[piece], wq_buf[aligned(piece, depth), :], preferred_element_type=F32)
    q_acc[...] = part if first else q_acc[...] + part


def new_rows(place, hidden, wkv_buf, kv_new):
    pieces, rows, depth = hidden.shape
    local_rows = rows // place.count
    total = None
    for piece in range(pieces):
        mine = hidden[piece, aligned(place.me, local_rows), :]
        part = jnp.dot(mine, wkv_buf[pl.ds(piece * depth, depth), :], preferred_element_type=F32)
        total = part if total is None else total + part
    kv_new[...] = total.astype(BF16).astype(F32)


def query_copies(place, q_send, q_out, send_sems, recv_sems, incoming):
    heads = q_send.shape[0]
    local_rows = q_out.shape[1]
    copies = []
    for offset in range(1, place.count):
        source = place.origin(offset) if incoming else place.me
        target = place.peer(offset)
        copies.append(remote(
            q_send.at[:, aligned(target, local_rows), :], q_out.at[pl.ds(source * heads, heads)],
            send_sems.at[offset], recv_sems.at[offset], target))
    return copies


def send_order(count):
    return sorted(range(1, count), key=lambda offset: -min(offset, count - offset))


def exchange_query(place, q_acc, q_send, q_out, send_sems, recv_sems):
    heads, rows, head_dim = q_send.shape
    local_rows = q_out.shape[1]
    for head in range(heads):
        q_send[head] = q_acc[:, head * head_dim:(head + 1) * head_dim].astype(BF16)
    outgoing = query_copies(place, q_send, q_out, send_sems, recv_sems, False)
    for offset in send_order(place.count):
        outgoing[offset - 1].start()
    q_out[pl.ds(place.me * heads, heads)] = q_send[:, aligned(place.me, local_rows), :]
    return outgoing


def first_kernel(count, x, wq, wk, wv, k_cache, v_cache,
                 q_out, kv_new, residual, k_vmem, v_vmem,
                 hidden, wq_buf, wkv_buf, q_acc, q_send,
                 x_sems, w_sems, cache_sems, q_ssem, q_rsem):
    place = Place(count)
    pieces, rows, depth = hidden.shape
    x_copies = [
        pltpu.make_async_copy(x.at[:, pl.ds(i * depth, depth)], hidden.at[i], x_sems.at[i]) for i in range(pieces)
    ]
    w_copies = weight_copies(0, wq, wk, wv, wq_buf, wkv_buf, w_sems)
    cache_copies = [
        pltpu.make_async_copy(k_cache.at[0], k_vmem, cache_sems.at[0]),
        pltpu.make_async_copy(v_cache.at[0], v_vmem, cache_sems.at[1]),
    ]
    for i in range(pieces):
        x_copies[i].start()
        w_copies[i].start()
    w_copies[pieces].start()
    w_copies[pieces + 1].start()
    for copy in cache_copies:
        copy.start()
    signal_all(place)
    for i in range(pieces):
        x_copies[i].wait()
        w_copies[i].wait()
        add_query(i, i == 0, hidden, wq_buf, q_acc)
    wait_all(place)
    outgoing = exchange_query(place, q_acc, q_send, q_out, q_ssem, q_rsem)
    chip_rows = residual.shape[1]
    for j in range(CHUNKS):
        residual[j] = hidden[place.core * CHUNKS + j, aligned(place.chip, chip_rows), :]
    w_copies[pieces].wait()
    w_copies[pieces + 1].wait()
    new_rows(place, hidden, wkv_buf, kv_new)
    for copy in query_copies(place, q_send, q_out, q_ssem, q_rsem, True):
        copy.wait_recv()
    for copy in outgoing:
        copy.wait_send()
    for copy in cache_copies:
        copy.wait()


def mix_kernel(count, last, layer, *refs):
    refs = list(refs)
    take = lambda k: [refs.pop(0) for _ in range(k)]
    context, residual, wo = take(3)
    if not last:
        wq, wk, wv, k_cache, v_cache = take(5)
        q_out, kv_new, next_residual, k_vmem, v_vmem = take(5)
    else:
        (hidden,) = take(1)
    c_recv, wo_far, wo_own, p_send, p_recv, total, s1_recv, comb, s2_left, s2_right = take(10)
    wo_sems, c_ssem, c_rsem, p_ssem, p_rsem, s1_ssem, s1_rsem = take(7)
    s2_ssem, s2_rsem, ag_ssem, ag_rsem, fw_ssem, fw_rsem, d2d_ssem, d2d_rsem = take(8)
    if not last:
        hidden, wq_buf, wkv_buf, q_acc, q_send, w_sems, cache_sems, q_ssem, q_rsem = take(9)
    place = Place(count)
    heads, rows, head_dim = c_recv.shape
    local_rows = rows // count
    chip_rows = rows // CHIPS
    depth = hidden.shape[-1]
    half = depth * CHUNKS

    wo_copies = []
    for j in range(CHUNKS):
        wo_copies.append(pltpu.make_async_copy(
            wo.at[layer, :, aligned((1 - place.core) * CHUNKS + j, depth)], wo_far.at[j], wo_sems.at[j]))
    for j in range(CHUNKS):
        wo_copies.append(pltpu.make_async_copy(
            wo.at[layer, :, aligned(place.core * CHUNKS + j, depth)], wo_own.at[j], wo_sems.at[CHUNKS + j]))
    for copy in wo_copies:
        copy.start()
    if not last:
        w_copies = weight_copies(layer + 1, wq, wk, wv, wq_buf, wkv_buf, w_sems)
        cache_copies = [
            pltpu.make_async_copy(k_cache.at[layer + 1], k_vmem, cache_sems.at[0]),
            pltpu.make_async_copy(v_cache.at[layer + 1], v_vmem, cache_sems.at[1]),
        ]
        for copy in w_copies + cache_copies:
            copy.start()

    signal_all(place)
    c_recv[:, aligned(place.me, local_rows), :] = context[pl.ds(place.me * heads, heads)]
    wait_all(place)

    def context_copy(offset, source):
        target = place.peer(offset)
        return remote(
            context.at[pl.ds(target * heads, heads)], c_recv.at[:, aligned(source, local_rows), :],
            c_ssem.at[offset], c_rsem.at[offset], target)

    sends = []

    def send(copy):
        copy.start()
        sends.append(copy)

    for offset in send_order(count):
        send(context_copy(offset, place.me))
    for offset in range(1, count):
        context_copy(offset, place.origin(offset)).wait_recv()

    def product(weights):
        acc = None
        for pair in range(heads // 2):
            lhs = jnp.concatenate([c_recv[2 * pair], c_recv[2 * pair + 1]], axis=1)
            part = jnp.dot(lhs, weights[pl.ds(pair * 2 * head_dim, 2 * head_dim), :], preferred_element_type=F32)
            acc = part if acc is None else acc + part
        return acc

    def pair_copy(j):
        return remote(p_send.at[j], p_recv.at[j], p_ssem.at[j], p_rsem.at[j], place.sibling)

    def block(chip):
        return aligned(chip, chip_rows)

    for j in range(CHUNKS):
        wo_copies[j].wait()
        p_send[j] = product(wo_far.at[j])
        send(pair_copy(j))

    def step_one(j):
        target = place.to_right if j % 2 == 0 else place.to_left
        return remote(total.at[j, block(place.across), :], s1_recv.at[j], s1_ssem.at[j], s1_rsem.at[j], target)

    def step_two(j, rightward, source):
        target = place.to_right if rightward else place.to_left
        inbox = s2_left if rightward else s2_right
        slot = j if rightward else CHUNKS + j
        return remote(source, inbox.at[j], s2_ssem.at[slot], s2_rsem.at[slot], target)

    for j in range(CHUNKS):
        wo_copies[CHUNKS + j].wait()
        own = product(wo_own.at[j])
        pair_copy(j).wait_recv()
        total[j] = own + p_recv[j]
        send(step_one(j))
        rightward = j % 2 == 1
        send(step_two(j, rightward, total.at[j, block(place.right if rightward else place.left), :]))
    for j in range(CHUNKS):
        step_one(j).wait_recv()
        rightward = j % 2 == 0
        comb[j] = total[j, block(place.right if rightward else place.left), :] + s1_recv[j]
        send(step_two(j, rightward, comb.at[j]))

    def piece(core, j):
        return core * CHUNKS + j

    def gather_copy(j, way, chip):
        target = place.to_right if way == 0 else place.to_left
        region = hidden.at[piece(place.core, j), block(chip), :]
        return remote(region, region, ag_ssem.at[way * CHUNKS + j], ag_rsem.at[way * CHUNKS + j], target)

    def forward_copy(j, chip):
        target = place.to_right if j % 2 == 0 else place.to_left
        region = hidden.at[piece(place.core, j), block(chip), :]
        return remote(region, region, fw_ssem.at[j], fw_rsem.at[j], target)

    def twin_copy(j, kind, core):
        chip = (place.chip, place.left, place.right, place.across)[kind]
        region = hidden.at[piece(core, j), block(chip), :]
        slot = kind * CHUNKS + j
        return remote(region, region, d2d_ssem.at[slot], d2d_rsem.at[slot], place.sibling)

    def finish(j):
        step_two(j, True, comb.at[j]).wait_recv()
        step_two(j, False, comb.at[j]).wait_recv()
        summed = total[j, block(place.chip), :] + s2_left[j] + s2_right[j]
        value = (residual[j].astype(F32) + summed).astype(BF16)
        hidden[piece(place.core, j), block(place.chip), :] = value
        if not last:
            next_residual[j] = value
        send(gather_copy(j, 0, place.chip))
        send(gather_copy(j, 1, place.chip))
        send(twin_copy(j, 0, place.core))

    def pass_on(j):
        gather_copy(j, 0, place.left).wait_recv()
        if j % 2 == 0:
            send(forward_copy(j, place.left))
        send(twin_copy(j, 1, place.core))
        gather_copy(j, 1, place.right).wait_recv()
        if j % 2 == 1:
            send(forward_copy(j, place.right))
        send(twin_copy(j, 2, place.core))

    def far_block(j):
        forward_copy(j, place.across).wait_recv()
        send(twin_copy(j, 3, place.core))

    for j in range(CHUNKS):
        finish(j)
        if j >= 1:
            pass_on(j - 1)
        if j >= 2:
            far_block(j - 2)
            if not last:
                w_copies[2 * (j - 2)].wait()
                w_copies[2 * (j - 2) + 1].wait()
    pass_on(CHUNKS - 1)
    if not last:
        for i in range(2 * (CHUNKS - 2), len(w_copies)):
            w_copies[i].wait()
        for j in range(CHUNKS - 2):
            add_query(piece(place.core, j), j == 0, hidden, wq_buf, q_acc)
    far_block(CHUNKS - 2)
    if not last:
        add_query(piece(place.core, CHUNKS - 2), False, hidden, wq_buf, q_acc)
    far_block(CHUNKS - 1)
    if not last:
        add_query(piece(place.core, CHUNKS - 1), False, hidden, wq_buf, q_acc)
    for j in range(CHUNKS):
        for kind in range(4):
            twin_copy(j, kind, 1 - place.core).wait_recv()
        if not last:
            add_query(piece(1 - place.core, j), False, hidden, wq_buf, q_acc)
    if not last:
        outgoing = exchange_query(place, q_acc, q_send, q_out, q_ssem, q_rsem)
        new_rows(place, hidden, wkv_buf, kv_new)
        for copy in query_copies(place, q_send, q_out, q_ssem, q_rsem, True):
            copy.wait_recv()
        sends.extend(outgoing)
        for copy in cache_copies:
            copy.wait()
    for copy in sends:
        copy.wait_send()


GROUP = 4


def attention_kernel(layer, *refs):
    lens, q, kv_new, k_in, v_in = refs[:5]
    refs = refs[5:]
    if layer > 0:
        refs = refs[2:]
    k_out, v_out, k_buf, v_buf, context, q_rows, c_rows, sems = refs
    del k_in, v_in
    heads, local_rows, head_dim = q.shape
    seq_len = k_buf.shape[1]
    tile = 16

    for b in range(local_rows):
        start = pl.multiple_of((lens[b] // tile) * tile, tile)
        here = lax.broadcasted_iota(jnp.int32, (tile, head_dim), 0) == lens[b] - start
        for buf, column in ((k_buf, 0), (v_buf, head_dim)):
            fresh = jnp.broadcast_to(kv_new[b:b + 1, column:column + head_dim], (tile, head_dim))
            old = buf[b, pl.ds(start, tile), :].astype(F32)
            buf[b, pl.ds(start, tile), :] = jnp.where(here, fresh, old).astype(BF16)
    q_rows[...] = q[...].astype(F32).reshape(heads * local_rows, head_dim)
    writes = [
        pltpu.make_async_copy(k_buf, k_out.at[layer], sems.at[0]),
        pltpu.make_async_copy(v_buf, v_out.at[layer], sems.at[1]),
    ]
    for copy in writes:
        copy.start()

    def attend(b, span):
        rows = pl.ds(b, heads, stride=local_rows)
        query = q_rows[rows, :].astype(BF16)
        scores = lax.dot_general(
            query, k_buf[b, pl.ds(0, span), :], (((1,), (1,)), ((), ())), preferred_element_type=F32)
        scores = scores * (head_dim ** -0.5)
        visible = lax.broadcasted_iota(jnp.int32, (heads, span), 1) <= lens[b]
        scores = jnp.where(visible, scores, -jnp.inf)
        top = jnp.max(scores, axis=1, keepdims=True)
        powers = jnp.exp(scores - top)
        weights = (powers / jnp.sum(powers, axis=1, keepdims=True)).astype(BF16)
        out = jnp.dot(weights, v_buf[b, pl.ds(0, span), :], preferred_element_type=F32)
        c_rows[rows, :] = out.astype(BF16).astype(F32)

    spans = []
    span = 256
    while span < seq_len:
        spans.append(span)
        span *= 2
    spans.append(seq_len)

    def one_group(g, _):
        longest = lens[g * GROUP]
        for i in range(1, GROUP):
            longest = jnp.maximum(longest, lens[g * GROUP + i])
        low = 0
        for span in spans:
            @pl.when(jnp.logical_and(longest >= low, longest < span))
            def _(span=span):
                for i in range(GROUP):
                    attend(g * GROUP + i, span)
            low = span
        return 0

    lax.fori_loop(0, local_rows // GROUP, one_group, 0)
    context[...] = c_rows[...].reshape(heads, local_rows, head_dim).astype(BF16)
    for copy in writes:
        copy.wait()


def store_kernel(hidden, out, sems):
    pieces, rows, depth = hidden.shape
    copies = [pltpu.make_async_copy(hidden.at[i], out.at[:, pl.ds(i * depth, depth)], sems.at[i]) for i in range(pieces)]
    for copy in copies:
        copy.start()
    for copy in copies:
        copy.wait()


def solution(mesh):
    count = mesh.shape["model"]
    assert count == 2 * CHIPS
    row_axes = ("replica", "model")
    cache_spec = P(None, row_axes, None, None)
    DMA = pltpu.SemaphoreType.DMA

    def device_step(x, cache_len, w_query, w_key, w_value, w_out, k_cache, v_cache):
        rows, width = x.shape
        layers, local_rows, seq_len, head_dim = k_cache.shape
        local_width = w_query.shape[-1]
        local_heads = local_width // head_dim
        heads = local_heads * count
        pieces = 2 * CHUNKS
        depth = width // pieces
        chip_rows = rows // CHIPS
        my_len = lax.dynamic_slice_in_dim(cache_len, lax.axis_index("model") * local_rows, local_rows)
        w_query, w_key, w_value, w_out = map(to_hbm, (w_query, w_key, w_value, w_out))
        x, k_cache, v_cache = map(to_hbm, (x, k_cache, v_cache))

        project_out = (
            pltpu.VMEM((heads, local_rows, head_dim), BF16),
            pltpu.VMEM((local_rows, 2 * head_dim), F32),
            pltpu.VMEM((CHUNKS, chip_rows, depth), BF16),
            pltpu.VMEM(k_cache.shape[1:], BF16),
            pltpu.VMEM(v_cache.shape[1:], BF16),
        )
        project_scratch = [
            pltpu.VMEM((pieces, rows, depth), BF16),
            pltpu.VMEM((width, local_width), BF16),
            pltpu.VMEM((width, 2 * head_dim), BF16),
            pltpu.VMEM((rows, local_width), F32),
            pltpu.VMEM((local_heads, rows, head_dim), BF16),
        ]
        project_sems = [DMA((pieces + 2,)), DMA((2,)), DMA((count,)), DMA((count,))]
        mix_scratch = [
            pltpu.VMEM((local_heads, rows, head_dim), BF16),
            pltpu.VMEM((CHUNKS, local_width, depth), BF16),
            pltpu.VMEM((CHUNKS, local_width, depth), BF16),
            pltpu.VMEM((CHUNKS, rows, depth), F32),
            pltpu.VMEM((CHUNKS, rows, depth), F32),
            pltpu.VMEM((CHUNKS, rows, depth), F32),
            pltpu.VMEM((CHUNKS, chip_rows, depth), F32),
            pltpu.VMEM((CHUNKS, chip_rows, depth), F32),
            pltpu.VMEM((CHUNKS, chip_rows, depth), F32),
            pltpu.VMEM((CHUNKS, chip_rows, depth), F32),
            DMA((pieces,)), DMA((count,)), DMA((count,)), DMA((CHUNKS,)), DMA((CHUNKS,)), DMA((CHUNKS,)), DMA((CHUNKS,)),
            DMA((2 * CHUNKS,)), DMA((2 * CHUNKS,)), DMA((2 * CHUNKS,)), DMA((2 * CHUNKS,)),
            DMA((CHUNKS,)), DMA((CHUNKS,)), DMA((4 * CHUNKS,)), DMA((4 * CHUNKS,)),
        ]

        def params(collective_id, limit):
            return pltpu.CompilerParams(collective_id=collective_id, has_side_effects=True, vmem_limit_bytes=limit * MIB)

        query, kv_new, residual, k_vmem, v_vmem = pl.pallas_call(
            functools.partial(first_kernel, count),
            out_shape=project_out,
            in_specs=[ANY_SPEC] * 6,
            out_specs=(VMEM_SPEC,) * 5,
            scratch_shapes=project_scratch + [DMA((pieces,))] + project_sems,
            compiler_params=params(0, 16),
            name="first",
        )(x, w_query, w_key, w_value, k_cache, v_cache)

        k_new_cache = v_new_cache = None
        for layer in range(layers):
            last = layer == layers - 1
            operands = [my_len, query, kv_new, k_vmem, v_vmem]
            specs = [SMEM_SPEC] + [VMEM_SPEC] * 4
            aliases = {3: 2, 4: 3}
            if layer > 0:
                operands += [k_new_cache, v_new_cache]
                specs += [ANY_SPEC] * 2
                aliases |= {5: 0, 6: 1}
            k_new_cache, v_new_cache, _, _, context = pl.pallas_call(
                functools.partial(attention_kernel, layer),
                out_shape=(
                    pltpu.HBM(k_cache.shape, BF16),
                    pltpu.HBM(v_cache.shape, BF16),
                    pltpu.VMEM(k_cache.shape[1:], BF16),
                    pltpu.VMEM(v_cache.shape[1:], BF16),
                    pltpu.VMEM((heads, local_rows, head_dim), BF16),
                ),
                in_specs=specs,
                out_specs=(ANY_SPEC, ANY_SPEC, VMEM_SPEC, VMEM_SPEC, VMEM_SPEC),
                input_output_aliases=aliases,
                scratch_shapes=[
                    pltpu.VMEM((heads * local_rows, head_dim), F32),
                    pltpu.VMEM((heads * local_rows, head_dim), F32),
                    DMA((2,)),
                ],
                compiler_params=pltpu.CompilerParams(vmem_limit_bytes=16 * MIB),
                name=f"attend{layer}",
            )(*operands)
            if not last:
                query, kv_new, residual, k_vmem, v_vmem = pl.pallas_call(
                    functools.partial(mix_kernel, count, False, layer),
                    out_shape=project_out,
                    in_specs=[VMEM_SPEC] * 2 + [ANY_SPEC] * 6,
                    out_specs=(VMEM_SPEC,) * 5,
                    scratch_shapes=mix_scratch + project_scratch + project_sems,
                    compiler_params=params(1 + layer, 28),
                    name=f"mix{layer}",
                )(context, residual, w_out, w_query, w_key, w_value, k_cache, v_cache)
            else:
                hidden = pl.pallas_call(
                    functools.partial(mix_kernel, count, True, layer),
                    out_shape=pltpu.VMEM((pieces, rows, depth), BF16),
                    in_specs=[VMEM_SPEC] * 2 + [ANY_SPEC],
                    out_specs=VMEM_SPEC,
                    scratch_shapes=mix_scratch,
                    compiler_params=params(1 + layer, 20),
                    name=f"mix{layer}",
                )(context, residual, w_out)
        out = pl.pallas_call(
            store_kernel,
            out_shape=jax.ShapeDtypeStruct((rows, width), BF16),
            in_specs=[VMEM_SPEC],
            out_specs=ANY_SPEC,
            scratch_shapes=[DMA((pieces,))],
            name="store",
        )(hidden)
        return out, k_new_cache, v_new_cache

    return jax.shard_map(
        device_step,
        mesh=mesh,
        in_specs=(P("replica", None), P("replica"), P(None, None, "model"), P(), P(), P(None, "model", None), cache_spec, cache_spec),
        out_specs=(P("replica", None), cache_spec, cache_spec),
        check_vma=False,
    )
```

```python
import functools

import jax
import jax.numpy as jnp
from jax import lax
from jax.experimental import pallas as pl
from jax.experimental.pallas import tpu as pltpu
from jax.sharding import PartitionSpec as P

MESH = pl.DeviceIdType.MESH
F32 = jnp.float32
BF16 = jnp.bfloat16
CHIPS = 4
CHUNKS = 4
PARTS = 8
RING = 0
MIB = 1 << 20

ANY_SPEC = pl.BlockSpec(memory_space=pltpu.HBM)
VMEM_SPEC = pl.BlockSpec(memory_space=pltpu.VMEM)
SMEM_SPEC = pl.BlockSpec(memory_space=pltpu.SMEM)


def to_hbm(value):
    return pltpu.with_memory_space_constraint(value, pltpu.HBM)


def to_vmem(value):
    return pltpu.with_memory_space_constraint(value, pltpu.VMEM)


def aligned(index, size):
    return pl.ds(pl.multiple_of(index * size, size), size)


class Place:
    def __init__(self, count):
        self.count = count
        self.me = lax.axis_index("model")
        self.chip = self.me // 2
        self.core = self.me % 2
        self.right = (self.chip + 1) % CHIPS
        self.left = (self.chip + CHIPS - 1) % CHIPS
        self.across = (self.chip + 2) % CHIPS
        self.to_right = self.right * 2 + self.core
        self.to_left = self.left * 2 + self.core
        self.sibling = self.chip * 2 + (1 - self.core)

    def peer(self, offset):
        return (self.me + offset) % self.count

    def origin(self, offset):
        return (self.me + self.count - offset) % self.count


def remote(src, dst, send_sem, recv_sem, device):
    return pltpu.make_async_remote_copy(
        src_ref=src, dst_ref=dst, send_sem=send_sem, recv_sem=recv_sem,
        device_id={"model": device}, device_id_type=MESH)


def signal_all(place):
    barrier = pltpu.get_barrier_semaphore()
    for offset in send_order(place.count):
        pl.semaphore_signal(barrier, inc=1, device_id={"model": place.peer(offset)}, device_id_type=MESH)


def wait_all(place):
    pl.semaphore_wait(pltpu.get_barrier_semaphore(), place.count - 1)


def weight_copies(layer, wq, wk, wv, wq_buf, wkv_buf, sems):
    pieces = sems.shape[0] - 2
    depth = wq_buf.shape[0] // pieces
    head_dim = wk.shape[-1]
    copies = [
        pltpu.make_async_copy(wq.at[layer, pl.ds(i * depth, depth), :], wq_buf.at[pl.ds(i * depth, depth), :], sems.at[i])
        for i in range(pieces)
    ]
    copies.append(pltpu.make_async_copy(wk.at[layer], wkv_buf.at[:, pl.ds(0, head_dim)], sems.at[pieces]))
    copies.append(pltpu.make_async_copy(wv.at[layer], wkv_buf.at[:, pl.ds(head_dim, head_dim)], sems.at[pieces + 1]))
    return copies


def cache_loads(layer, k_cache, v_cache, k_vmem, v_vmem, sems):
    parts = sems.shape[0] // 2
    step = k_vmem.shape[0] // parts
    copies = []
    for i in range(parts):
        part = pl.ds(i * step, step)
        copies.append(pltpu.make_async_copy(k_cache.at[layer, part], k_vmem.at[part], sems.at[2 * i]))
        copies.append(pltpu.make_async_copy(v_cache.at[layer, part], v_vmem.at[part], sems.at[2 * i + 1]))
    return copies


def add_query(piece, first, hidden, wq_buf, q_acc):
    depth = hidden.shape[-1]
    part = jnp.dot(hidden[piece], wq_buf[aligned(piece, depth), :], preferred_element_type=F32)
    q_acc[...] = part if first else q_acc[...] + part


def new_rows(place, hidden, wkv_buf, kv_new):
    pieces, rows, depth = hidden.shape
    local_rows = rows // place.count
    total = None
    for piece in range(pieces):
        mine = hidden[piece, aligned(place.me, local_rows), :]
        part = jnp.dot(mine, wkv_buf[pl.ds(piece * depth, depth), :], preferred_element_type=F32)
        total = part if total is None else total + part
    kv_new[...] = total.astype(BF16).astype(F32)


def query_copies(place, q_send, q_out, send_sems, recv_sems, incoming):
    heads = q_send.shape[0]
    local_rows = q_out.shape[1]
    copies = []
    for offset in range(1, place.count):
        source = place.origin(offset) if incoming else place.me
        target = place.peer(offset)
        copies.append(remote(
            q_send.at[:, aligned(target, local_rows), :], q_out.at[pl.ds(source * heads, heads)],
            send_sems.at[offset], recv_sems.at[offset], target))
    return copies


def send_order(count):
    return sorted(range(1, count), key=lambda offset: -min(offset, count - offset))


def exchange_query(place, q_acc, q_send, q_out, send_sems, recv_sems):
    heads, rows, head_dim = q_send.shape
    local_rows = q_out.shape[1]
    for head in range(heads):
        q_send[head] = q_acc[:, head * head_dim:(head + 1) * head_dim].astype(BF16)
    outgoing = query_copies(place, q_send, q_out, send_sems, recv_sems, False)
    for offset in send_order(place.count):
        outgoing[offset - 1].start()
    q_out[pl.ds(place.me * heads, heads)] = q_send[:, aligned(place.me, local_rows), :]
    return outgoing


def first_kernel(count, x, wq, wk, wv, k_cache, v_cache,
                 q_out, kv_new, residual, k_vmem, v_vmem,
                 hidden, wq_buf, wkv_buf, q_acc, q_send,
                 x_sems, w_sems, cache_sems, q_ssem, q_rsem):
    place = Place(count)
    pieces, rows, depth = hidden.shape
    x_copies = [
        pltpu.make_async_copy(x.at[:, pl.ds(i * depth, depth)], hidden.at[i], x_sems.at[i]) for i in range(pieces)
    ]
    w_copies = weight_copies(0, wq, wk, wv, wq_buf, wkv_buf, w_sems)
    cache_copies = cache_loads(0, k_cache, v_cache, k_vmem, v_vmem, cache_sems)
    for i in range(pieces):
        x_copies[i].start()
        w_copies[i].start()
    signal_all(place)
    w_copies[pieces].start()
    w_copies[pieces + 1].start()
    for copy in cache_copies:
        copy.start()
    for i in range(pieces):
        x_copies[i].wait()
        w_copies[i].wait()
        add_query(i, i == 0, hidden, wq_buf, q_acc)
    wait_all(place)
    outgoing = exchange_query(place, q_acc, q_send, q_out, q_ssem, q_rsem)
    chip_rows = residual.shape[1]
    for j in range(CHUNKS):
        residual[j] = hidden[place.core * CHUNKS + j, aligned(place.chip, chip_rows), :]
    w_copies[pieces].wait()
    w_copies[pieces + 1].wait()
    new_rows(place, hidden, wkv_buf, kv_new)
    for copy in query_copies(place, q_send, q_out, q_ssem, q_rsem, True):
        copy.wait_recv()
    for copy in outgoing:
        copy.wait_send()
    for copy in cache_copies:
        copy.wait()


def mix_kernel(count, last, layer, *refs):
    refs = list(refs)
    take = lambda k: [refs.pop(0) for _ in range(k)]
    context, residual, wo = take(3)
    if not last:
        wq, wk, wv, k_cache, v_cache = take(5)
        q_out, kv_new, next_residual, k_vmem, v_vmem = take(5)
    else:
        (hidden,) = take(1)
    c_recv, wo_far, wo_own, p_send, p_recv, total, s1_recv, comb, s2_left, s2_right = take(10)
    wo_sems, c_ssem, c_rsem, p_ssem, p_rsem, s1_ssem, s1_rsem = take(7)
    s2_ssem, s2_rsem, ag_ssem, ag_rsem, d2d_ssem, d2d_rsem = take(6)
    if not last:
        hidden, wq_buf, wkv_buf, q_acc, q_send, w_sems, cache_sems, q_ssem, q_rsem = take(9)
    place = Place(count)
    heads, rows, head_dim = c_recv.shape
    local_rows = rows // count
    chip_rows = rows // CHIPS
    depth = total.shape[-1]

    signal_all(place)
    wo_copies = []
    for j in range(CHUNKS):
        wo_copies.append(pltpu.make_async_copy(
            wo.at[layer, :, aligned((1 - place.core) * CHUNKS + j, depth)], wo_far.at[j], wo_sems.at[j]))
    for j in range(CHUNKS):
        wo_copies.append(pltpu.make_async_copy(
            wo.at[layer, :, aligned(place.core * CHUNKS + j, depth)], wo_own.at[j], wo_sems.at[CHUNKS + j]))
    for copy in wo_copies:
        copy.start()
    if not last:
        w_copies = weight_copies(layer + 1, wq, wk, wv, wq_buf, wkv_buf, w_sems)
        cache_copies = cache_loads(layer + 1, k_cache, v_cache, k_vmem, v_vmem, cache_sems)
        for copy in w_copies + cache_copies:
            copy.start()

    c_recv[:, aligned(place.me, local_rows), :] = context[pl.ds(place.me * heads, heads)]
    wait_all(place)

    def context_copy(offset, source):
        target = place.peer(offset)
        return remote(
            context.at[pl.ds(target * heads, heads)], c_recv.at[:, aligned(source, local_rows), :],
            c_ssem.at[offset], c_rsem.at[offset], target)

    sends = []

    def send(copy):
        copy.start()
        sends.append(copy)

    for offset in send_order(count):
        send(context_copy(offset, place.me))
    for offset in range(1, count):
        context_copy(offset, place.origin(offset)).wait_recv()

    def product(weights):
        acc = None
        for pair in range(heads // 2):
            lhs = jnp.concatenate([c_recv[2 * pair], c_recv[2 * pair + 1]], axis=1)
            part = jnp.dot(lhs, weights[pl.ds(pair * 2 * head_dim, 2 * head_dim), :], preferred_element_type=F32)
            acc = part if acc is None else acc + part
        return acc

    def pair_copy(j):
        return remote(p_send.at[j], p_recv.at[j], p_ssem.at[j], p_rsem.at[j], place.sibling)

    def block(chip):
        return aligned(chip, chip_rows)

    for j in range(CHUNKS):
        wo_copies[j].wait()
        p_send[j] = product(wo_far.at[j])
        send(pair_copy(j))

    def step_one(j):
        target = place.to_right if j % 2 == 0 else place.to_left
        return remote(total.at[j, block(place.across), :], s1_recv.at[j], s1_ssem.at[j], s1_rsem.at[j], target)

    def step_two(j, rightward, source):
        target = place.to_right if rightward else place.to_left
        inbox = s2_left if rightward else s2_right
        slot = j if rightward else CHUNKS + j
        return remote(source, inbox.at[j], s2_ssem.at[slot], s2_rsem.at[slot], target)

    def direct(j):
        rightward = j % 2 == 1
        send(step_two(j, rightward, total.at[j, block(place.right if rightward else place.left), :]))

    def combine(j):
        step_one(j).wait_recv()
        rightward = j % 2 == 0
        comb[j] = total[j, block(place.right if rightward else place.left), :] + s1_recv[j]
        send(step_two(j, rightward, comb.at[j]))

    for j in range(CHUNKS):
        wo_copies[CHUNKS + j].wait()
        own = product(wo_own.at[j])
        pair_copy(j).wait_recv()
        total[j] = own + p_recv[j]
        send(step_one(j))
        if j == 0:
            direct(0)
        elif j >= 2:
            direct(j - 1)
    combine(0)
    combine(1)
    direct(CHUNKS - 1)
    for j in range(2, CHUNKS):
        combine(j)

    def piece(core, j):
        return core * CHUNKS + j

    def region(core, j, chip):
        if last:
            return hidden.at[block(chip), aligned(piece(core, j), depth)]
        return hidden.at[piece(core, j), block(chip), :]

    def gather_copy(j, way, chip):
        target = (place.to_right, place.to_left, place.across * 2 + place.core)[way]
        part = region(place.core, j, chip)
        slot = way * CHUNKS + j
        return remote(part, part, ag_ssem.at[slot], ag_rsem.at[slot], target)

    def forward_copy(j, chip):
        target = place.to_right if j % 2 == 0 else place.to_left
        part = region(place.core, j, chip)
        return remote(part, part, ag_ssem.at[2 * CHUNKS + j], ag_rsem.at[2 * CHUNKS + j], target)

    def twin_copy(j, kind, core):
        chip = (place.chip, place.left, place.right, place.across)[kind]
        part = region(core, j, chip)
        slot = kind * CHUNKS + j
        return remote(part, part, d2d_ssem.at[slot], d2d_rsem.at[slot], place.sibling)

    def finish(j):
        step_two(j, True, comb.at[j]).wait_recv()
        step_two(j, False, comb.at[j]).wait_recv()
        summed = total[j, block(place.chip), :] + s2_left[j] + s2_right[j]
        value = (residual[j].astype(F32) + summed).astype(BF16)
        if last:
            hidden[block(place.chip), aligned(piece(place.core, j), depth)] = value
        else:
            hidden[piece(place.core, j), block(place.chip), :] = value
            next_residual[j] = value
        if j >= RING:
            send(gather_copy(j, 2, place.chip))
        send(gather_copy(j, 0, place.chip))
        send(gather_copy(j, 1, place.chip))
        send(twin_copy(j, 0, place.core))

    def pass_on(j):
        gather_copy(j, 0, place.left).wait_recv()
        if j < RING and j % 2 == 0:
            send(forward_copy(j, place.left))
        send(twin_copy(j, 1, place.core))
        gather_copy(j, 1, place.right).wait_recv()
        if j < RING and j % 2 == 1:
            send(forward_copy(j, place.right))
        send(twin_copy(j, 2, place.core))

    def far_block(j):
        gather_copy(j, 2, place.across).wait_recv()
        send(twin_copy(j, 3, place.core))

    for j in range(CHUNKS):
        finish(j)
        if j >= 2:
            pass_on(j - 2)
    for j in range(CHUNKS):
        if j >= 2:
            pass_on(j)
        far_block(j)
        if not last:
            for copy in w_copies if j == 0 else ():
                copy.wait()
            add_query(piece(place.core, j), j == 0, hidden, wq_buf, q_acc)
    for j in range(CHUNKS):
        for kind in range(4):
            twin_copy(j, kind, 1 - place.core).wait_recv()
        if not last:
            add_query(piece(1 - place.core, j), False, hidden, wq_buf, q_acc)
    if not last:
        outgoing = exchange_query(place, q_acc, q_send, q_out, q_ssem, q_rsem)
        new_rows(place, hidden, wkv_buf, kv_new)
        for copy in query_copies(place, q_send, q_out, q_ssem, q_rsem, True):
            copy.wait_recv()
        sends.extend(outgoing)
        for copy in cache_copies:
            copy.wait()
    for copy in sends:
        copy.wait_send()


GROUP = 8
SHORT = 256


def attention_kernel(layer, *refs):
    all_lens, q, kv_new, k_in, v_in = refs[:5]
    refs = refs[5:]
    if layer > 0:
        refs = refs[2:]
    k_out, v_out, k_buf, v_buf, context, q_rows, c_rows, sems = refs
    del k_in, v_in
    heads, local_rows, head_dim = q.shape
    seq_len = k_buf.shape[1]
    tile = 16
    first_row = lax.axis_index("model") * local_rows

    def length(b):
        return all_lens[first_row + b]

    for b in range(local_rows):
        start = pl.multiple_of((length(b) // tile) * tile, tile)
        here = lax.broadcasted_iota(jnp.int32, (tile, head_dim), 0) == length(b) - start
        for buf, column in ((k_buf, 0), (v_buf, head_dim)):
            fresh = jnp.broadcast_to(kv_new[b:b + 1, column:column + head_dim], (tile, head_dim))
            old = buf[b, pl.ds(start, tile), :].astype(F32)
            buf[b, pl.ds(start, tile), :] = jnp.where(here, fresh, old).astype(BF16)

    q_rows[...] = q[...].astype(F32).reshape(heads * local_rows, head_dim)
    writes = []
    parts = sems.shape[0] // 2
    step = local_rows // parts
    for i in range(parts):
        part = pl.ds(i * step, step)
        writes.append(pltpu.make_async_copy(k_buf.at[part], k_out.at[layer, part], sems.at[2 * i]))
        writes.append(pltpu.make_async_copy(v_buf.at[part], v_out.at[layer, part], sems.at[2 * i + 1]))
    for copy in writes:
        copy.start()

    def attend(members, span):
        rows = [pl.ds(b, heads, stride=local_rows) for b in members]
        scores = [
            lax.dot_general(
                q_rows[r, :].astype(BF16), k_buf[b, pl.ds(0, span), :], (((1,), (1,)), ((), ())),
                preferred_element_type=F32)
            for b, r in zip(members, rows)
        ]
        positions = lax.broadcasted_iota(jnp.int32, (heads, span), 1)
        scores = [jnp.where(positions <= length(b), s * (head_dim ** -0.5), -jnp.inf) for b, s in zip(members, scores)]
        tops = [jnp.max(s, axis=1, keepdims=True) for s in scores]
        powers = [jnp.exp(s - t) for s, t in zip(scores, tops)]
        sums = [jnp.sum(p, axis=1, keepdims=True) for p in powers]
        weights = [(p / t).astype(BF16) for p, t in zip(powers, sums)]
        outs = [
            jnp.dot(w, v_buf[b, pl.ds(0, span), :], preferred_element_type=F32) for b, w in zip(members, weights)
        ]
        for r, out in zip(rows, outs):
            c_rows[r, :] = out.astype(BF16).astype(F32)

    for first in range(0, local_rows, GROUP):
        attend(list(range(first, first + GROUP)), SHORT)

    spans = []
    span = 2 * SHORT
    while span < seq_len:
        spans.append(span)
        span *= 2
    spans.append(seq_len)

    def longer(b, _):
        @pl.when(length(b) >= SHORT)
        def _():
            low = SHORT
            for span in spans:
                @pl.when(jnp.logical_and(length(b) >= low, length(b) < span))
                def _(span=span):
                    attend([b], span)
                low = span
        return 0

    lax.fori_loop(0, local_rows, longer, 0)
    context[...] = c_rows[...].reshape(heads, local_rows, head_dim).astype(BF16)
    for copy in writes:
        copy.wait()


def solution(mesh):
    count = mesh.shape["model"]
    assert count == 2 * CHIPS
    row_axes = ("replica", "model")
    cache_spec = P(None, row_axes, None, None)
    DMA = pltpu.SemaphoreType.DMA

    def device_step(x, cache_len, w_query, w_key, w_value, w_out, k_cache, v_cache):
        rows, width = x.shape
        layers, local_rows, seq_len, head_dim = k_cache.shape
        local_width = w_query.shape[-1]
        local_heads = local_width // head_dim
        heads = local_heads * count
        pieces = 2 * CHUNKS
        depth = width // pieces
        chip_rows = rows // CHIPS
        w_query, w_key, w_value, w_out = map(to_hbm, (w_query, w_key, w_value, w_out))
        x, k_cache, v_cache = map(to_hbm, (x, k_cache, v_cache))

        project_out = (
            pltpu.VMEM((heads, local_rows, head_dim), BF16),
            pltpu.VMEM((local_rows, 2 * head_dim), F32),
            pltpu.VMEM((CHUNKS, chip_rows, depth), BF16),
            pltpu.VMEM(k_cache.shape[1:], BF16),
            pltpu.VMEM(v_cache.shape[1:], BF16),
        )
        project_scratch = [
            pltpu.VMEM((pieces, rows, depth), BF16),
            pltpu.VMEM((width, local_width), BF16),
            pltpu.VMEM((width, 2 * head_dim), BF16),
            pltpu.VMEM((rows, local_width), F32),
            pltpu.VMEM((local_heads, rows, head_dim), BF16),
        ]
        project_sems = [DMA((pieces + 2,)), DMA((2 * PARTS,)), DMA((count,)), DMA((count,))]
        mix_scratch = [
            pltpu.VMEM((local_heads, rows, head_dim), BF16),
            pltpu.VMEM((CHUNKS, local_width, depth), BF16),
            pltpu.VMEM((CHUNKS, local_width, depth), BF16),
            pltpu.VMEM((CHUNKS, rows, depth), F32),
            pltpu.VMEM((CHUNKS, rows, depth), F32),
            pltpu.VMEM((CHUNKS, rows, depth), F32),
            pltpu.VMEM((CHUNKS, chip_rows, depth), F32),
            pltpu.VMEM((CHUNKS, chip_rows, depth), F32),
            pltpu.VMEM((CHUNKS, chip_rows, depth), F32),
            pltpu.VMEM((CHUNKS, chip_rows, depth), F32),
            DMA((pieces,)), DMA((count,)), DMA((count,)), DMA((CHUNKS,)), DMA((CHUNKS,)), DMA((CHUNKS,)), DMA((CHUNKS,)),
            DMA((2 * CHUNKS,)), DMA((2 * CHUNKS,)), DMA((3 * CHUNKS,)), DMA((3 * CHUNKS,)),
            DMA((4 * CHUNKS,)), DMA((4 * CHUNKS,)),
        ]

        def params(collective_id, limit):
            return pltpu.CompilerParams(collective_id=collective_id, has_side_effects=True, vmem_limit_bytes=limit * MIB)

        query, kv_new, residual, k_vmem, v_vmem = pl.pallas_call(
            functools.partial(first_kernel, count),
            out_shape=project_out,
            in_specs=[ANY_SPEC] * 6,
            out_specs=(VMEM_SPEC,) * 5,
            scratch_shapes=project_scratch + [DMA((pieces,))] + project_sems,
            compiler_params=params(0, 16),
            name="first",
        )(x, w_query, w_key, w_value, k_cache, v_cache)

        k_new_cache = v_new_cache = None
        for layer in range(layers):
            last = layer == layers - 1
            operands = [cache_len, query, kv_new, k_vmem, v_vmem]
            specs = [SMEM_SPEC] + [VMEM_SPEC] * 4
            aliases = {3: 2, 4: 3}
            if layer > 0:
                operands += [k_new_cache, v_new_cache]
                specs += [ANY_SPEC] * 2
                aliases |= {5: 0, 6: 1}
            k_new_cache, v_new_cache, _, _, context = pl.pallas_call(
                functools.partial(attention_kernel, layer),
                out_shape=(
                    pltpu.HBM(k_cache.shape, BF16),
                    pltpu.HBM(v_cache.shape, BF16),
                    pltpu.VMEM(k_cache.shape[1:], BF16),
                    pltpu.VMEM(v_cache.shape[1:], BF16),
                    pltpu.VMEM((heads, local_rows, head_dim), BF16),
                ),
                in_specs=specs,
                out_specs=(ANY_SPEC, ANY_SPEC, VMEM_SPEC, VMEM_SPEC, VMEM_SPEC),
                input_output_aliases=aliases,
                scratch_shapes=[
                    pltpu.VMEM((heads * local_rows, head_dim), F32),
                    pltpu.VMEM((heads * local_rows, head_dim), F32),
                    DMA((2 * PARTS,)),
                ],
                compiler_params=pltpu.CompilerParams(vmem_limit_bytes=16 * MIB),
                name=f"attend{layer}",
            )(*operands)
            if not last:
                query, kv_new, residual, k_vmem, v_vmem = pl.pallas_call(
                    functools.partial(mix_kernel, count, False, layer),
                    out_shape=project_out,
                    in_specs=[VMEM_SPEC] * 2 + [ANY_SPEC] * 6,
                    out_specs=(VMEM_SPEC,) * 5,
                    scratch_shapes=mix_scratch + project_scratch + project_sems,
                    compiler_params=params(1 + layer, 28),
                    name=f"mix{layer}",
                )(context, residual, w_out, w_query, w_key, w_value, k_cache, v_cache)
            else:
                hidden = pl.pallas_call(
                    functools.partial(mix_kernel, count, True, layer),
                    out_shape=pltpu.VMEM((rows, width), BF16),
                    in_specs=[VMEM_SPEC] * 2 + [ANY_SPEC],
                    out_specs=VMEM_SPEC,
                    scratch_shapes=mix_scratch,
                    compiler_params=params(1 + layer, 20),
                    name=f"mix{layer}",
                )(context, residual, w_out)
        return hidden, k_new_cache, v_new_cache

    return jax.shard_map(
        device_step,
        mesh=mesh,
        in_specs=(P("replica", None), P("replica"), P(None, None, "model"), P(), P(), P(None, "model", None), cache_spec, cache_spec),
        out_specs=(P("replica", None), cache_spec, cache_spec),
        check_vma=False,
    )
```

```python
import functools

import jax
import jax.numpy as jnp
from jax import lax
from jax.experimental import pallas as pl
from jax.experimental.pallas import tpu as pltpu
from jax.sharding import PartitionSpec as P

MESH = pl.DeviceIdType.MESH
F32 = jnp.float32
BF16 = jnp.bfloat16
CHIPS = 4
CHUNKS = 4
PARTS = 8
RING = 3
MIB = 1 << 20

ANY_SPEC = pl.BlockSpec(memory_space=pltpu.HBM)
VMEM_SPEC = pl.BlockSpec(memory_space=pltpu.VMEM)
SMEM_SPEC = pl.BlockSpec(memory_space=pltpu.SMEM)


def to_hbm(value):
    return pltpu.with_memory_space_constraint(value, pltpu.HBM)


def to_vmem(value):
    return pltpu.with_memory_space_constraint(value, pltpu.VMEM)


def aligned(index, size):
    return pl.ds(pl.multiple_of(index * size, size), size)


class Place:
    def __init__(self, count):
        self.count = count
        self.me = lax.axis_index("model")
        self.chip = self.me // 2
        self.core = self.me % 2
        self.right = (self.chip + 1) % CHIPS
        self.left = (self.chip + CHIPS - 1) % CHIPS
        self.across = (self.chip + 2) % CHIPS
        self.to_right = self.right * 2 + self.core
        self.to_left = self.left * 2 + self.core
        self.sibling = self.chip * 2 + (1 - self.core)

    def peer(self, offset):
        return (self.me + offset) % self.count

    def origin(self, offset):
        return (self.me + self.count - offset) % self.count


def remote(src, dst, send_sem, recv_sem, device):
    return pltpu.make_async_remote_copy(
        src_ref=src, dst_ref=dst, send_sem=send_sem, recv_sem=recv_sem,
        device_id={"model": device}, device_id_type=MESH)


def signal_all(place):
    barrier = pltpu.get_barrier_semaphore()
    for offset in send_order(place.count):
        pl.semaphore_signal(barrier, inc=1, device_id={"model": place.peer(offset)}, device_id_type=MESH)


def wait_all(place):
    pl.semaphore_wait(pltpu.get_barrier_semaphore(), place.count - 1)


def weight_copies(layer, wq, wk, wv, wq_buf, wkv_buf, sems):
    pieces = sems.shape[0] - 2
    depth = wq_buf.shape[0] // pieces
    head_dim = wk.shape[-1]
    copies = [
        pltpu.make_async_copy(wq.at[layer, pl.ds(i * depth, depth), :], wq_buf.at[pl.ds(i * depth, depth), :], sems.at[i])
        for i in range(pieces)
    ]
    copies.append(pltpu.make_async_copy(wk.at[layer], wkv_buf.at[:, pl.ds(0, head_dim)], sems.at[pieces]))
    copies.append(pltpu.make_async_copy(wv.at[layer], wkv_buf.at[:, pl.ds(head_dim, head_dim)], sems.at[pieces + 1]))
    return copies


def cache_loads(layer, k_cache, v_cache, k_vmem, v_vmem, sems):
    parts = sems.shape[0] // 2
    step = k_vmem.shape[0] // parts
    copies = []
    for i in range(parts):
        part = pl.ds(i * step, step)
        copies.append(pltpu.make_async_copy(k_cache.at[layer, part], k_vmem.at[part], sems.at[2 * i]))
        copies.append(pltpu.make_async_copy(v_cache.at[layer, part], v_vmem.at[part], sems.at[2 * i + 1]))
    return copies


def add_query(piece, first, hidden, wq_buf, q_acc):
    depth = hidden.shape[-1]
    part = jnp.dot(hidden[piece], wq_buf[aligned(piece, depth), :], preferred_element_type=F32)
    q_acc[...] = part if first else q_acc[...] + part


def new_rows(place, hidden, wkv_buf, kv_new):
    pieces, rows, depth = hidden.shape
    local_rows = rows // place.count
    total = None
    for piece in range(pieces):
        mine = hidden[piece, aligned(place.me, local_rows), :]
        part = jnp.dot(mine, wkv_buf[pl.ds(piece * depth, depth), :], preferred_element_type=F32)
        total = part if total is None else total + part
    kv_new[...] = total.astype(BF16).astype(F32)


def query_copies(place, q_send, q_out, send_sems, recv_sems, incoming):
    heads = q_send.shape[0]
    local_rows = q_out.shape[1]
    copies = []
    for offset in range(1, place.count):
        source = place.origin(offset) if incoming else place.me
        target = place.peer(offset)
        copies.append(remote(
            q_send.at[:, aligned(target, local_rows), :], q_out.at[pl.ds(source * heads, heads)],
            send_sems.at[offset], recv_sems.at[offset], target))
    return copies


def send_order(count):
    return sorted(range(1, count), key=lambda offset: -min(offset, count - offset))


def exchange_query(place, q_acc, q_send, q_out, send_sems, recv_sems):
    heads, rows, head_dim = q_send.shape
    local_rows = q_out.shape[1]
    for head in range(heads):
        q_send[head] = q_acc[:, head * head_dim:(head + 1) * head_dim].astype(BF16)
    outgoing = query_copies(place, q_send, q_out, send_sems, recv_sems, False)
    for offset in send_order(place.count):
        outgoing[offset - 1].start()
    q_out[pl.ds(place.me * heads, heads)] = q_send[:, aligned(place.me, local_rows), :]
    return outgoing


def first_kernel(count, x, wq, wk, wv, k_cache, v_cache,
                 q_out, kv_new, residual, k_vmem, v_vmem,
                 hidden, wq_buf, wkv_buf, q_acc, q_send,
                 x_sems, w_sems, cache_sems, q_ssem, q_rsem):
    place = Place(count)
    pieces, rows, depth = hidden.shape
    x_copies = [
        pltpu.make_async_copy(x.at[:, pl.ds(i * depth, depth)], hidden.at[i], x_sems.at[i]) for i in range(pieces)
    ]
    w_copies = weight_copies(0, wq, wk, wv, wq_buf, wkv_buf, w_sems)
    cache_copies = cache_loads(0, k_cache, v_cache, k_vmem, v_vmem, cache_sems)
    for i in range(pieces):
        x_copies[i].start()
        w_copies[i].start()
    signal_all(place)
    w_copies[pieces].start()
    w_copies[pieces + 1].start()
    for copy in cache_copies:
        copy.start()
    for i in range(pieces):
        x_copies[i].wait()
        w_copies[i].wait()
        add_query(i, i == 0, hidden, wq_buf, q_acc)
    wait_all(place)
    outgoing = exchange_query(place, q_acc, q_send, q_out, q_ssem, q_rsem)
    chip_rows = residual.shape[1]
    for j in range(CHUNKS):
        residual[j] = hidden[place.core * CHUNKS + j, aligned(place.chip, chip_rows), :]
    w_copies[pieces].wait()
    w_copies[pieces + 1].wait()
    new_rows(place, hidden, wkv_buf, kv_new)
    for copy in query_copies(place, q_send, q_out, q_ssem, q_rsem, True):
        copy.wait_recv()
    for copy in outgoing:
        copy.wait_send()
    for copy in cache_copies:
        copy.wait()


def mix_kernel(count, last, layer, *refs):
    refs = list(refs)
    take = lambda k: [refs.pop(0) for _ in range(k)]
    context, residual, wo = take(3)
    if not last:
        wq, wk, wv, k_cache, v_cache = take(5)
        q_out, kv_new, next_residual, k_vmem, v_vmem = take(5)
    else:
        (hidden,) = take(1)
    c_recv, wo_far, wo_own, p_send, p_recv, total, s1_recv, comb, s2_left, s2_right = take(10)
    wo_sems, c_ssem, c_rsem, p_ssem, p_rsem, s1_ssem, s1_rsem = take(7)
    s2_ssem, s2_rsem, ag_ssem, ag_rsem, d2d_ssem, d2d_rsem = take(6)
    if not last:
        hidden, wq_buf, wkv_buf, q_acc, q_send, w_sems, cache_sems, q_ssem, q_rsem = take(9)
    place = Place(count)
    heads, rows, head_dim = c_recv.shape
    local_rows = rows // count
    chip_rows = rows // CHIPS
    depth = total.shape[-1]

    signal_all(place)
    wo_copies = []
    for j in range(CHUNKS):
        wo_copies.append(pltpu.make_async_copy(
            wo.at[layer, :, aligned((1 - place.core) * CHUNKS + j, depth)], wo_far.at[j], wo_sems.at[j]))
    for j in range(CHUNKS):
        wo_copies.append(pltpu.make_async_copy(
            wo.at[layer, :, aligned(place.core * CHUNKS + j, depth)], wo_own.at[j], wo_sems.at[CHUNKS + j]))
    for copy in wo_copies:
        copy.start()
    if not last:
        w_copies = weight_copies(layer + 1, wq, wk, wv, wq_buf, wkv_buf, w_sems)
        cache_copies = cache_loads(layer + 1, k_cache, v_cache, k_vmem, v_vmem, cache_sems)
        for copy in w_copies + cache_copies:
            copy.start()

    c_recv[:, aligned(place.me, local_rows), :] = context[pl.ds(place.me * heads, heads)]
    wait_all(place)

    def context_copy(offset, source):
        target = place.peer(offset)
        return remote(
            context.at[pl.ds(target * heads, heads)], c_recv.at[:, aligned(source, local_rows), :],
            c_ssem.at[offset], c_rsem.at[offset], target)

    sends = []

    def send(copy):
        copy.start()
        sends.append(copy)

    for offset in send_order(count):
        send(context_copy(offset, place.me))
    for offset in range(1, count):
        context_copy(offset, place.origin(offset)).wait_recv()

    def product(weights):
        acc = None
        for pair in range(heads // 2):
            lhs = jnp.concatenate([c_recv[2 * pair], c_recv[2 * pair + 1]], axis=1)
            part = jnp.dot(lhs, weights[pl.ds(pair * 2 * head_dim, 2 * head_dim), :], preferred_element_type=F32)
            acc = part if acc is None else acc + part
        return acc

    def pair_copy(j):
        return remote(p_send.at[j], p_recv.at[j], p_ssem.at[j], p_rsem.at[j], place.sibling)

    def block(chip):
        return aligned(chip, chip_rows)

    for j in range(CHUNKS):
        wo_copies[j].wait()
        p_send[j] = product(wo_far.at[j])
        send(pair_copy(j))

    def step_one(j):
        target = place.to_right if j % 2 == 0 else place.to_left
        return remote(total.at[j, block(place.across), :], s1_recv.at[j], s1_ssem.at[j], s1_rsem.at[j], target)

    def step_two(j, rightward, source):
        target = place.to_right if rightward else place.to_left
        inbox = s2_left if rightward else s2_right
        slot = j if rightward else CHUNKS + j
        return remote(source, inbox.at[j], s2_ssem.at[slot], s2_rsem.at[slot], target)

    def direct(j):
        rightward = j % 2 == 1
        send(step_two(j, rightward, total.at[j, block(place.right if rightward else place.left), :]))

    def combine(j):
        step_one(j).wait_recv()
        rightward = j % 2 == 0
        comb[j] = total[j, block(place.right if rightward else place.left), :] + s1_recv[j]
        send(step_two(j, rightward, comb.at[j]))

    for j in range(CHUNKS):
        wo_copies[CHUNKS + j].wait()
        total[j] = product(wo_own.at[j])
    for j in range(CHUNKS):
        pair_copy(j).wait_recv()
        total[j] += p_recv[j]
        send(step_one(j))
        if j == 0:
            direct(0)
        elif j >= 2:
            direct(j - 1)
    combine(0)
    combine(1)
    direct(CHUNKS - 1)
    for j in range(2, CHUNKS):
        combine(j)

    def piece(core, j):
        return core * CHUNKS + j

    def region(core, j, chip):
        if last:
            return hidden.at[block(chip), aligned(piece(core, j), depth)]
        return hidden.at[piece(core, j), block(chip), :]

    def gather_copy(j, way, chip):
        target = (place.to_right, place.to_left, place.across * 2 + place.core)[way]
        part = region(place.core, j, chip)
        slot = way * CHUNKS + j
        return remote(part, part, ag_ssem.at[slot], ag_rsem.at[slot], target)

    def forward_copy(j, chip):
        target = place.to_right if j % 2 == 0 else place.to_left
        part = region(place.core, j, chip)
        return remote(part, part, ag_ssem.at[2 * CHUNKS + j], ag_rsem.at[2 * CHUNKS + j], target)

    def twin_copy(j, kind, core):
        chip = (place.chip, place.left, place.right, place.across)[kind]
        part = region(core, j, chip)
        slot = kind * CHUNKS + j
        return remote(part, part, d2d_ssem.at[slot], d2d_rsem.at[slot], place.sibling)

    def finish(j):
        step_two(j, True, comb.at[j]).wait_recv()
        step_two(j, False, comb.at[j]).wait_recv()
        summed = total[j, block(place.chip), :] + s2_left[j] + s2_right[j]
        value = (residual[j].astype(F32) + summed).astype(BF16)
        if last:
            hidden[block(place.chip), aligned(piece(place.core, j), depth)] = value
        else:
            hidden[piece(place.core, j), block(place.chip), :] = value
            next_residual[j] = value
        if j >= RING:
            send(gather_copy(j, 2, place.chip))
        send(gather_copy(j, 0, place.chip))
        send(gather_copy(j, 1, place.chip))
        send(twin_copy(j, 0, place.core))

    def pass_on(j):
        gather_copy(j, 0, place.left).wait_recv()
        if j < RING and j % 2 == 0:
            send(forward_copy(j, place.left))
        send(twin_copy(j, 1, place.core))
        gather_copy(j, 1, place.right).wait_recv()
        if j < RING and j % 2 == 1:
            send(forward_copy(j, place.right))
        send(twin_copy(j, 2, place.core))

    def far_block(j):
        gather_copy(j, 2, place.across).wait_recv()
        send(twin_copy(j, 3, place.core))

    for j in range(CHUNKS):
        finish(j)
    for j in range(RING):
        pass_on(j)
    for j in range(CHUNKS):
        if j >= RING:
            pass_on(j)
        far_block(j)
        if not last:
            for copy in w_copies if j == 0 else ():
                copy.wait()
            add_query(piece(place.core, j), j == 0, hidden, wq_buf, q_acc)
    for j in range(CHUNKS):
        for kind in range(4):
            twin_copy(j, kind, 1 - place.core).wait_recv()
        if not last:
            add_query(piece(1 - place.core, j), False, hidden, wq_buf, q_acc)
    if not last:
        outgoing = exchange_query(place, q_acc, q_send, q_out, q_ssem, q_rsem)
        new_rows(place, hidden, wkv_buf, kv_new)
        for copy in query_copies(place, q_send, q_out, q_ssem, q_rsem, True):
            copy.wait_recv()
        sends.extend(outgoing)
        for copy in cache_copies:
            copy.wait()
    for copy in sends:
        copy.wait_send()


GROUP = 8
SHORT = 256


def attention_kernel(layer, *refs):
    all_lens, q, kv_new, k_in, v_in = refs[:5]
    refs = refs[5:]
    if layer > 0:
        refs = refs[2:]
    k_out, v_out, k_buf, v_buf, context, q_rows, c_rows, sems = refs
    del k_in, v_in
    heads, local_rows, head_dim = q.shape
    seq_len = k_buf.shape[1]
    tile = 16
    first_row = lax.axis_index("model") * local_rows

    def length(b):
        return all_lens[first_row + b]

    writes = []
    parts = sems.shape[0] // 2
    step = local_rows // parts
    for i in range(parts):
        for b in range(i * step, (i + 1) * step):
            start = pl.multiple_of((length(b) // tile) * tile, tile)
            here = lax.broadcasted_iota(jnp.int32, (tile, head_dim), 0) == length(b) - start
            for buf, column in ((k_buf, 0), (v_buf, head_dim)):
                fresh = jnp.broadcast_to(kv_new[b:b + 1, column:column + head_dim], (tile, head_dim))
                old = buf[b, pl.ds(start, tile), :].astype(F32)
                buf[b, pl.ds(start, tile), :] = jnp.where(here, fresh, old).astype(BF16)
        part = pl.ds(i * step, step)
        writes.append(pltpu.make_async_copy(k_buf.at[part], k_out.at[layer, part], sems.at[2 * i]))
        writes.append(pltpu.make_async_copy(v_buf.at[part], v_out.at[layer, part], sems.at[2 * i + 1]))
        if i > 0:
            writes[2 * i - 2].start()
            writes[2 * i - 1].start()
    q_rows[...] = q[...].astype(F32).reshape(heads * local_rows, head_dim)
    writes[-2].start()
    writes[-1].start()

    def attend(members, span):
        rows = [pl.ds(b, heads, stride=local_rows) for b in members]
        scores = [
            lax.dot_general(
                q_rows[r, :].astype(BF16), k_buf[b, pl.ds(0, span), :], (((1,), (1,)), ((), ())),
                preferred_element_type=F32)
            for b, r in zip(members, rows)
        ]
        positions = lax.broadcasted_iota(jnp.int32, (heads, span), 1)
        scores = [jnp.where(positions <= length(b), s * (head_dim ** -0.5), -jnp.inf) for b, s in zip(members, scores)]
        tops = [jnp.max(s, axis=1, keepdims=True) for s in scores]
        powers = [jnp.exp(s - t) for s, t in zip(scores, tops)]
        sums = [jnp.sum(p, axis=1, keepdims=True) for p in powers]
        weights = [(p / t).astype(BF16) for p, t in zip(powers, sums)]
        outs = [
            jnp.dot(w, v_buf[b, pl.ds(0, span), :], preferred_element_type=F32) for b, w in zip(members, weights)
        ]
        for r, out in zip(rows, outs):
            c_rows[r, :] = out.astype(BF16).astype(F32)

    for first in range(0, local_rows, GROUP):
        attend(list(range(first, first + GROUP)), SHORT)

    spans = []
    span = 2 * SHORT
    while span < seq_len:
        spans.append(span)
        span *= 2
    spans.append(seq_len)

    def longer(b, _):
        @pl.when(length(b) >= SHORT)
        def _():
            low = SHORT
            for span in spans:
                @pl.when(jnp.logical_and(length(b) >= low, length(b) < span))
                def _(span=span):
                    attend([b], span)
                low = span
        return 0

    lax.fori_loop(0, local_rows, longer, 0)
    context[...] = c_rows[...].reshape(heads, local_rows, head_dim).astype(BF16)
    for copy in writes:
        copy.wait()


def solution(mesh):
    count = mesh.shape["model"]
    assert count == 2 * CHIPS
    row_axes = ("replica", "model")
    cache_spec = P(None, row_axes, None, None)
    DMA = pltpu.SemaphoreType.DMA

    def device_step(x, cache_len, w_query, w_key, w_value, w_out, k_cache, v_cache):
        rows, width = x.shape
        layers, local_rows, seq_len, head_dim = k_cache.shape
        local_width = w_query.shape[-1]
        local_heads = local_width // head_dim
        heads = local_heads * count
        pieces = 2 * CHUNKS
        depth = width // pieces
        chip_rows = rows // CHIPS
        w_query, w_key, w_value, w_out = map(to_hbm, (w_query, w_key, w_value, w_out))
        x, k_cache, v_cache = map(to_hbm, (x, k_cache, v_cache))

        project_out = (
            pltpu.VMEM((heads, local_rows, head_dim), BF16),
            pltpu.VMEM((local_rows, 2 * head_dim), F32),
            pltpu.VMEM((CHUNKS, chip_rows, depth), BF16),
            pltpu.VMEM(k_cache.shape[1:], BF16),
            pltpu.VMEM(v_cache.shape[1:], BF16),
        )
        project_scratch = [
            pltpu.VMEM((pieces, rows, depth), BF16),
            pltpu.VMEM((width, local_width), BF16),
            pltpu.VMEM((width, 2 * head_dim), BF16),
            pltpu.VMEM((rows, local_width), F32),
            pltpu.VMEM((local_heads, rows, head_dim), BF16),
        ]
        project_sems = [DMA((pieces + 2,)), DMA((2 * PARTS,)), DMA((count,)), DMA((count,))]
        mix_scratch = [
            pltpu.VMEM((local_heads, rows, head_dim), BF16),
            pltpu.VMEM((CHUNKS, local_width, depth), BF16),
            pltpu.VMEM((CHUNKS, local_width, depth), BF16),
            pltpu.VMEM((CHUNKS, rows, depth), F32),
            pltpu.VMEM((CHUNKS, rows, depth), F32),
            pltpu.VMEM((CHUNKS, rows, depth), F32),
            pltpu.VMEM((CHUNKS, chip_rows, depth), F32),
            pltpu.VMEM((CHUNKS, chip_rows, depth), F32),
            pltpu.VMEM((CHUNKS, chip_rows, depth), F32),
            pltpu.VMEM((CHUNKS, chip_rows, depth), F32),
            DMA((pieces,)), DMA((count,)), DMA((count,)), DMA((CHUNKS,)), DMA((CHUNKS,)), DMA((CHUNKS,)), DMA((CHUNKS,)),
            DMA((2 * CHUNKS,)), DMA((2 * CHUNKS,)), DMA((3 * CHUNKS,)), DMA((3 * CHUNKS,)),
            DMA((4 * CHUNKS,)), DMA((4 * CHUNKS,)),
        ]

        def params(collective_id, limit):
            return pltpu.CompilerParams(collective_id=collective_id, has_side_effects=True, vmem_limit_bytes=limit * MIB)

        query, kv_new, residual, k_vmem, v_vmem = pl.pallas_call(
            functools.partial(first_kernel, count),
            out_shape=project_out,
            in_specs=[ANY_SPEC] * 6,
            out_specs=(VMEM_SPEC,) * 5,
            scratch_shapes=project_scratch + [DMA((pieces,))] + project_sems,
            compiler_params=params(0, 16),
            name="first",
        )(x, w_query, w_key, w_value, k_cache, v_cache)

        k_new_cache = v_new_cache = None
        for layer in range(layers):
            last = layer == layers - 1
            operands = [cache_len, query, kv_new, k_vmem, v_vmem]
            specs = [SMEM_SPEC] + [VMEM_SPEC] * 4
            aliases = {3: 2, 4: 3}
            if layer > 0:
                operands += [k_new_cache, v_new_cache]
                specs += [ANY_SPEC] * 2
                aliases |= {5: 0, 6: 1}
            k_new_cache, v_new_cache, _, _, context = pl.pallas_call(
                functools.partial(attention_kernel, layer),
                out_shape=(
                    pltpu.HBM(k_cache.shape, BF16),
                    pltpu.HBM(v_cache.shape, BF16),
                    pltpu.VMEM(k_cache.shape[1:], BF16),
                    pltpu.VMEM(v_cache.shape[1:], BF16),
                    pltpu.VMEM((heads, local_rows, head_dim), BF16),
                ),
                in_specs=specs,
                out_specs=(ANY_SPEC, ANY_SPEC, VMEM_SPEC, VMEM_SPEC, VMEM_SPEC),
                input_output_aliases=aliases,
                scratch_shapes=[
                    pltpu.VMEM((heads * local_rows, head_dim), F32),
                    pltpu.VMEM((heads * local_rows, head_dim), F32),
                    DMA((2 * PARTS,)),
                ],
                compiler_params=pltpu.CompilerParams(vmem_limit_bytes=16 * MIB),
                name=f"attend{layer}",
            )(*operands)
            if not last:
                query, kv_new, residual, k_vmem, v_vmem = pl.pallas_call(
                    functools.partial(mix_kernel, count, False, layer),
                    out_shape=project_out,
                    in_specs=[VMEM_SPEC] * 2 + [ANY_SPEC] * 6,
                    out_specs=(VMEM_SPEC,) * 5,
                    scratch_shapes=mix_scratch + project_scratch + project_sems,
                    compiler_params=params(1 + layer, 28),
                    name=f"mix{layer}",
                )(context, residual, w_out, w_query, w_key, w_value, k_cache, v_cache)
            else:
                hidden = pl.pallas_call(
                    functools.partial(mix_kernel, count, True, layer),
                    out_shape=pltpu.VMEM((rows, width), BF16),
                    in_specs=[VMEM_SPEC] * 2 + [ANY_SPEC],
                    out_specs=VMEM_SPEC,
                    scratch_shapes=mix_scratch,
                    compiler_params=params(1 + layer, 20),
                    name=f"mix{layer}",
                )(context, residual, w_out)
        return hidden, k_new_cache, v_new_cache

    return jax.shard_map(
        device_step,
        mesh=mesh,
        in_specs=(P("replica", None), P("replica"), P(None, None, "model"), P(), P(), P(None, "model", None), cache_spec, cache_spec),
        out_specs=(P("replica", None), cache_spec, cache_spec),
        check_vma=False,
    )
```

```python
import functools

import jax
import jax.numpy as jnp
from jax import lax
from jax.experimental import pallas as pl
from jax.experimental.pallas import tpu as pltpu
from jax.sharding import PartitionSpec as P

MESH = pl.DeviceIdType.MESH
F32 = jnp.float32
BF16 = jnp.bfloat16
CHIPS = 4
CHUNKS = 4
PARTS = 8
RING = 0
RELAYED = 4
MIB = 1 << 20

ANY_SPEC = pl.BlockSpec(memory_space=pltpu.HBM)
VMEM_SPEC = pl.BlockSpec(memory_space=pltpu.VMEM)
SMEM_SPEC = pl.BlockSpec(memory_space=pltpu.SMEM)


def to_hbm(value):
    return pltpu.with_memory_space_constraint(value, pltpu.HBM)


def to_vmem(value):
    return pltpu.with_memory_space_constraint(value, pltpu.VMEM)


def aligned(index, size):
    return pl.ds(pl.multiple_of(index * size, size), size)


class Place:
    def __init__(self, count):
        self.count = count
        self.me = lax.axis_index("model")
        self.chip = self.me // 2
        self.core = self.me % 2
        self.right = (self.chip + 1) % CHIPS
        self.left = (self.chip + CHIPS - 1) % CHIPS
        self.across = (self.chip + 2) % CHIPS
        self.to_right = self.right * 2 + self.core
        self.to_left = self.left * 2 + self.core
        self.sibling = self.chip * 2 + (1 - self.core)

    def peer(self, offset):
        return (self.me + offset) % self.count

    def origin(self, offset):
        return (self.me + self.count - offset) % self.count


def remote(src, dst, send_sem, recv_sem, device):
    return pltpu.make_async_remote_copy(
        src_ref=src, dst_ref=dst, send_sem=send_sem, recv_sem=recv_sem,
        device_id={"model": device}, device_id_type=MESH)


def signal_all(place):
    barrier = pltpu.get_barrier_semaphore()
    for offset in send_order(place.count):
        pl.semaphore_signal(barrier, inc=1, device_id={"model": place.peer(offset)}, device_id_type=MESH)


def wait_all(place):
    pl.semaphore_wait(pltpu.get_barrier_semaphore(), place.count - 1)


def weight_copies(layer, wq, wk, wv, wq_buf, wkv_buf, sems):
    pieces = sems.shape[0] - 2
    depth = wq_buf.shape[0] // pieces
    head_dim = wk.shape[-1]
    copies = [
        pltpu.make_async_copy(wq.at[layer, pl.ds(i * depth, depth), :], wq_buf.at[pl.ds(i * depth, depth), :], sems.at[i])
        for i in range(pieces)
    ]
    copies.append(pltpu.make_async_copy(wk.at[layer], wkv_buf.at[:, pl.ds(0, head_dim)], sems.at[pieces]))
    copies.append(pltpu.make_async_copy(wv.at[layer], wkv_buf.at[:, pl.ds(head_dim, head_dim)], sems.at[pieces + 1]))
    return copies


def cache_loads(layer, k_cache, v_cache, k_vmem, v_vmem, sems):
    parts = sems.shape[0] // 2
    step = k_vmem.shape[0] // parts
    copies = []
    for i in range(parts):
        part = pl.ds(i * step, step)
        copies.append(pltpu.make_async_copy(k_cache.at[layer, part], k_vmem.at[part], sems.at[2 * i]))
        copies.append(pltpu.make_async_copy(v_cache.at[layer, part], v_vmem.at[part], sems.at[2 * i + 1]))
    return copies


def add_query(piece, first, hidden, wq_buf, q_acc):
    depth = hidden.shape[-1]
    part = jnp.dot(hidden[piece], wq_buf[aligned(piece, depth), :], preferred_element_type=F32)
    q_acc[...] = part if first else q_acc[...] + part


def new_rows(place, hidden, wkv_buf, kv_new):
    pieces, rows, depth = hidden.shape
    local_rows = rows // place.count
    total = None
    for piece in range(pieces):
        mine = hidden[piece, aligned(place.me, local_rows), :]
        part = jnp.dot(mine, wkv_buf[pl.ds(piece * depth, depth), :], preferred_element_type=F32)
        total = part if total is None else total + part
    kv_new[...] = total.astype(BF16).astype(F32)


def query_copies(place, q_send, q_out, send_sems, recv_sems, incoming):
    heads = q_send.shape[0]
    local_rows = q_out.shape[1]
    copies = []
    for offset in range(1, place.count):
        source = place.origin(offset) if incoming else place.me
        target = place.peer(offset)
        copies.append(remote(
            q_send.at[:, aligned(target, local_rows), :], q_out.at[pl.ds(source * heads, heads)],
            send_sems.at[offset], recv_sems.at[offset], target))
    return copies


def send_order(count):
    return sorted(range(1, count), key=lambda offset: -min(offset, count - offset))


def exchange_query(place, q_acc, q_send, q_out, send_sems, recv_sems):
    heads, rows, head_dim = q_send.shape
    local_rows = q_out.shape[1]
    for head in range(heads):
        q_send[head] = q_acc[:, head * head_dim:(head + 1) * head_dim].astype(BF16)
    outgoing = query_copies(place, q_send, q_out, send_sems, recv_sems, False)
    for offset in send_order(place.count):
        outgoing[offset - 1].start()
    q_out[pl.ds(place.me * heads, heads)] = q_send[:, aligned(place.me, local_rows), :]
    return outgoing


def first_kernel(count, x, wq, wk, wv, k_cache, v_cache,
                 q_out, kv_new, residual, k_vmem, v_vmem,
                 hidden, wq_buf, wkv_buf, q_acc, q_send,
                 x_sems, w_sems, cache_sems, q_ssem, q_rsem):
    place = Place(count)
    pieces, rows, depth = hidden.shape
    x_copies = [
        pltpu.make_async_copy(x.at[:, pl.ds(i * depth, depth)], hidden.at[i], x_sems.at[i]) for i in range(pieces)
    ]
    w_copies = weight_copies(0, wq, wk, wv, wq_buf, wkv_buf, w_sems)
    cache_copies = cache_loads(0, k_cache, v_cache, k_vmem, v_vmem, cache_sems)
    for i in range(pieces):
        x_copies[i].start()
        w_copies[i].start()
    signal_all(place)
    w_copies[pieces].start()
    w_copies[pieces + 1].start()
    for copy in cache_copies:
        copy.start()
    for i in range(pieces):
        x_copies[i].wait()
        w_copies[i].wait()
        add_query(i, i == 0, hidden, wq_buf, q_acc)
    wait_all(place)
    outgoing = exchange_query(place, q_acc, q_send, q_out, q_ssem, q_rsem)
    chip_rows = residual.shape[1]
    for j in range(CHUNKS):
        residual[j] = hidden[place.core * CHUNKS + j, aligned(place.chip, chip_rows), :]
    w_copies[pieces].wait()
    w_copies[pieces + 1].wait()
    new_rows(place, hidden, wkv_buf, kv_new)
    for copy in query_copies(place, q_send, q_out, q_ssem, q_rsem, True):
        copy.wait_recv()
    for copy in outgoing:
        copy.wait_send()
    for copy in cache_copies:
        copy.wait()


def mix_kernel(count, last, layer, *refs):
    refs = list(refs)
    take = lambda k: [refs.pop(0) for _ in range(k)]
    context, residual, wo = take(3)
    if not last:
        wq, wk, wv, k_cache, v_cache = take(5)
        q_out, kv_new, next_residual, k_vmem, v_vmem = take(5)
    else:
        (hidden,) = take(1)
    c_recv, wo_far, wo_own, p_send, p_recv, total, s1_recv, comb, s2_left, s2_right = take(10)
    wo_sems, c_ssem, c_rsem, p_ssem, p_rsem, s1_ssem, s1_rsem = take(7)
    s2_ssem, s2_rsem, ag_ssem, ag_rsem, d2d_ssem, d2d_rsem = take(6)
    if not last:
        hidden, wq_buf, wkv_buf, q_acc, q_send, w_sems, cache_sems, q_ssem, q_rsem = take(9)
    place = Place(count)
    heads, rows, head_dim = c_recv.shape
    local_rows = rows // count
    chip_rows = rows // CHIPS
    depth = total.shape[-1]

    signal_all(place)
    wo_copies = []
    for j in range(CHUNKS):
        wo_copies.append(pltpu.make_async_copy(
            wo.at[layer, :, aligned((1 - place.core) * CHUNKS + j, depth)], wo_far.at[j], wo_sems.at[j]))
    for j in range(CHUNKS):
        wo_copies.append(pltpu.make_async_copy(
            wo.at[layer, :, aligned(place.core * CHUNKS + j, depth)], wo_own.at[j], wo_sems.at[CHUNKS + j]))
    for copy in wo_copies:
        copy.start()
    if not last:
        w_copies = weight_copies(layer + 1, wq, wk, wv, wq_buf, wkv_buf, w_sems)
        cache_copies = cache_loads(layer + 1, k_cache, v_cache, k_vmem, v_vmem, cache_sems)
        for copy in w_copies + cache_copies:
            copy.start()

    c_recv[:, aligned(place.me, local_rows), :] = context[pl.ds(place.me * heads, heads)]
    wait_all(place)

    def context_copy(offset, source):
        target = place.peer(offset)
        return remote(
            context.at[pl.ds(target * heads, heads)], c_recv.at[:, aligned(source, local_rows), :],
            c_ssem.at[offset], c_rsem.at[offset], target)

    sends = []

    def send(copy):
        copy.start()
        sends.append(copy)

    for offset in send_order(count):
        send(context_copy(offset, place.me))
    for offset in range(1, count):
        context_copy(offset, place.origin(offset)).wait_recv()

    def product(weights):
        acc = None
        for pair in range(heads // 2):
            lhs = jnp.concatenate([c_recv[2 * pair], c_recv[2 * pair + 1]], axis=1)
            part = jnp.dot(lhs, weights[pl.ds(pair * 2 * head_dim, 2 * head_dim), :], preferred_element_type=F32)
            acc = part if acc is None else acc + part
        return acc

    def pair_copy(j):
        return remote(p_send.at[j], p_recv.at[j], p_ssem.at[j], p_rsem.at[j], place.sibling)

    def block(chip):
        return aligned(chip, chip_rows)

    for j in range(CHUNKS):
        wo_copies[j].wait()
        p_send[j] = product(wo_far.at[j])
        send(pair_copy(j))

    def step_one(j):
        target = place.to_right if j % 2 == 0 else place.to_left
        if j >= RELAYED:
            target = place.across * 2 + place.core
        return remote(total.at[j, block(place.across), :], s1_recv.at[j], s1_ssem.at[j], s1_rsem.at[j], target)

    def step_two(j, rightward, source):
        target = place.to_right if rightward else place.to_left
        inbox = s2_left if rightward else s2_right
        slot = j if rightward else CHUNKS + j
        return remote(source, inbox.at[j], s2_ssem.at[slot], s2_rsem.at[slot], target)

    def direct(j):
        for rightward in (j % 2 == 1, j % 2 == 0) if j >= RELAYED else (j % 2 == 1,):
            send(step_two(j, rightward, total.at[j, block(place.right if rightward else place.left), :]))

    def combine(j):
        step_one(j).wait_recv()
        rightward = j % 2 == 0
        comb[j] = total[j, block(place.right if rightward else place.left), :] + s1_recv[j]
        send(step_two(j, rightward, comb.at[j]))

    for j in range(CHUNKS):
        wo_copies[CHUNKS + j].wait()
        total[j] = product(wo_own.at[j])
    for j in range(CHUNKS):
        pair_copy(j).wait_recv()
        total[j] += p_recv[j]
        send(step_one(j))
        if j == 0 or j >= RELAYED:
            direct(j)
        elif j >= 2:
            direct(j - 1)
    for j in range(min(RELAYED, 2)):
        combine(j)
    if RELAYED == CHUNKS:
        direct(CHUNKS - 1)
    for j in range(2, RELAYED):
        combine(j)

    def piece(core, j):
        return core * CHUNKS + j

    def region(core, j, chip):
        if last:
            return hidden.at[block(chip), aligned(piece(core, j), depth)]
        return hidden.at[piece(core, j), block(chip), :]

    def gather_copy(j, way, chip):
        target = (place.to_right, place.to_left, place.across * 2 + place.core)[way]
        part = region(place.core, j, chip)
        slot = way * CHUNKS + j
        return remote(part, part, ag_ssem.at[slot], ag_rsem.at[slot], target)

    def forward_copy(j, chip):
        target = place.to_right if j % 2 == 0 else place.to_left
        part = region(place.core, j, chip)
        return remote(part, part, ag_ssem.at[2 * CHUNKS + j], ag_rsem.at[2 * CHUNKS + j], target)

    def twin_copy(j, kind, core):
        chip = (place.chip, place.left, place.right, place.across)[kind]
        part = region(core, j, chip)
        slot = kind * CHUNKS + j
        return remote(part, part, d2d_ssem.at[slot], d2d_rsem.at[slot], place.sibling)

    def finish(j):
        step_two(j, True, comb.at[j]).wait_recv()
        step_two(j, False, comb.at[j]).wait_recv()
        summed = total[j, block(place.chip), :] + s2_left[j] + s2_right[j]
        if j >= RELAYED:
            step_one(j).wait_recv()
            summed = summed + s1_recv[j]
        value = (residual[j].astype(F32) + summed).astype(BF16)
        if last:
            hidden[block(place.chip), aligned(piece(place.core, j), depth)] = value
        else:
            hidden[piece(place.core, j), block(place.chip), :] = value
            next_residual[j] = value
        if j >= RING:
            send(gather_copy(j, 2, place.chip))
        send(gather_copy(j, 0, place.chip))
        send(gather_copy(j, 1, place.chip))
        send(twin_copy(j, 0, place.core))

    def pass_on(j):
        gather_copy(j, 0, place.left).wait_recv()
        if j < RING and j % 2 == 0:
            send(forward_copy(j, place.left))
        send(twin_copy(j, 1, place.core))
        gather_copy(j, 1, place.right).wait_recv()
        if j < RING and j % 2 == 1:
            send(forward_copy(j, place.right))
        send(twin_copy(j, 2, place.core))

    def far_block(j):
        gather_copy(j, 2, place.across).wait_recv()
        send(twin_copy(j, 3, place.core))

    for j in range(CHUNKS):
        finish(j)
    for j in range(RING):
        pass_on(j)
    for j in range(CHUNKS):
        if j >= RING:
            pass_on(j)
        far_block(j)
        if not last:
            for copy in w_copies if j == 0 else ():
                copy.wait()
            add_query(piece(place.core, j), j == 0, hidden, wq_buf, q_acc)
    for j in range(CHUNKS):
        for kind in range(4):
            twin_copy(j, kind, 1 - place.core).wait_recv()
        if not last:
            add_query(piece(1 - place.core, j), False, hidden, wq_buf, q_acc)
    if not last:
        outgoing = exchange_query(place, q_acc, q_send, q_out, q_ssem, q_rsem)
        new_rows(place, hidden, wkv_buf, kv_new)
        for copy in query_copies(place, q_send, q_out, q_ssem, q_rsem, True):
            copy.wait_recv()
        sends.extend(outgoing)
        for copy in cache_copies:
            copy.wait()
    for copy in sends:
        copy.wait_send()


GROUP = 8
SHORT = 256


def attention_kernel(layer, *refs):
    all_lens, q, kv_new, k_in, v_in = refs[:5]
    refs = refs[5:]
    if layer > 0:
        refs = refs[2:]
    k_out, v_out, k_buf, v_buf, context, q_rows, c_rows, sems = refs
    del k_in, v_in
    heads, local_rows, head_dim = q.shape
    seq_len = k_buf.shape[1]
    tile = 16
    first_row = lax.axis_index("model") * local_rows

    def length(b):
        return all_lens[first_row + b]

    writes = []
    parts = sems.shape[0] // 2
    step = local_rows // parts
    for i in range(parts):
        for b in range(i * step, (i + 1) * step):
            start = pl.multiple_of((length(b) // tile) * tile, tile)
            here = lax.broadcasted_iota(jnp.int32, (tile, head_dim), 0) == length(b) - start
            for buf, column in ((k_buf, 0), (v_buf, head_dim)):
                fresh = jnp.broadcast_to(kv_new[b:b + 1, column:column + head_dim], (tile, head_dim))
                old = buf[b, pl.ds(start, tile), :].astype(F32)
                buf[b, pl.ds(start, tile), :] = jnp.where(here, fresh, old).astype(BF16)
        part = pl.ds(i * step, step)
        writes.append(pltpu.make_async_copy(k_buf.at[part], k_out.at[layer, part], sems.at[2 * i]))
        writes.append(pltpu.make_async_copy(v_buf.at[part], v_out.at[layer, part], sems.at[2 * i + 1]))
        if i > 0:
            writes[2 * i - 2].start()
            writes[2 * i - 1].start()
    q_rows[...] = q[...].astype(F32).reshape(heads * local_rows, head_dim)
    writes[-2].start()
    writes[-1].start()

    def attend(members, span):
        rows = [pl.ds(b, heads, stride=local_rows) for b in members]
        scores = [
            lax.dot_general(
                q_rows[r, :].astype(BF16), k_buf[b, pl.ds(0, span), :], (((1,), (1,)), ((), ())),
                preferred_element_type=F32)
            for b, r in zip(members, rows)
        ]
        positions = lax.broadcasted_iota(jnp.int32, (heads, span), 1)
        scores = [jnp.where(positions <= length(b), s * (head_dim ** -0.5), -jnp.inf) for b, s in zip(members, scores)]
        tops = [jnp.max(s, axis=1, keepdims=True) for s in scores]
        powers = [jnp.exp(s - t) for s, t in zip(scores, tops)]
        sums = [jnp.sum(p, axis=1, keepdims=True) for p in powers]
        weights = [(p / t).astype(BF16) for p, t in zip(powers, sums)]
        outs = [
            jnp.dot(w, v_buf[b, pl.ds(0, span), :], preferred_element_type=F32) for b, w in zip(members, weights)
        ]
        for r, out in zip(rows, outs):
            c_rows[r, :] = out.astype(BF16).astype(F32)

    for first in range(0, local_rows, GROUP):
        attend(list(range(first, first + GROUP)), SHORT)

    spans = []
    span = 2 * SHORT
    while span < seq_len:
        spans.append(span)
        span *= 2
    spans.append(seq_len)

    def longer(b, _):
        @pl.when(length(b) >= SHORT)
        def _():
            low = SHORT
            for span in spans:
                @pl.when(jnp.logical_and(length(b) >= low, length(b) < span))
                def _(span=span):
                    attend([b], span)
                low = span
        return 0

    lax.fori_loop(0, local_rows, longer, 0)
    context[...] = c_rows[...].reshape(heads, local_rows, head_dim).astype(BF16)
    for copy in writes:
        copy.wait()


def solution(mesh):
    count = mesh.shape["model"]
    assert count == 2 * CHIPS
    row_axes = ("replica", "model")
    cache_spec = P(None, row_axes, None, None)
    DMA = pltpu.SemaphoreType.DMA

    def device_step(x, cache_len, w_query, w_key, w_value, w_out, k_cache, v_cache):
        rows, width = x.shape
        layers, local_rows, seq_len, head_dim = k_cache.shape
        local_width = w_query.shape[-1]
        local_heads = local_width // head_dim
        heads = local_heads * count
        pieces = 2 * CHUNKS
        depth = width // pieces
        chip_rows = rows // CHIPS
        w_query, w_key, w_value, w_out = map(to_hbm, (w_query, w_key, w_value, w_out))
        x, k_cache, v_cache = map(to_hbm, (x, k_cache, v_cache))

        project_out = (
            pltpu.VMEM((heads, local_rows, head_dim), BF16),
            pltpu.VMEM((local_rows, 2 * head_dim), F32),
            pltpu.VMEM((CHUNKS, chip_rows, depth), BF16),
            pltpu.VMEM(k_cache.shape[1:], BF16),
            pltpu.VMEM(v_cache.shape[1:], BF16),
        )
        project_scratch = [
            pltpu.VMEM((pieces, rows, depth), BF16),
            pltpu.VMEM((width, local_width), BF16),
            pltpu.VMEM((width, 2 * head_dim), BF16),
            pltpu.VMEM((rows, local_width), F32),
            pltpu.VMEM((local_heads, rows, head_dim), BF16),
        ]
        project_sems = [DMA((pieces + 2,)), DMA((2 * PARTS,)), DMA((count,)), DMA((count,))]
        mix_scratch = [
            pltpu.VMEM((local_heads, rows, head_dim), BF16),
            pltpu.VMEM((CHUNKS, local_width, depth), BF16),
            pltpu.VMEM((CHUNKS, local_width, depth), BF16),
            pltpu.VMEM((CHUNKS, rows, depth), F32),
            pltpu.VMEM((CHUNKS, rows, depth), F32),
            pltpu.VMEM((CHUNKS, rows, depth), F32),
            pltpu.VMEM((CHUNKS, chip_rows, depth), F32),
            pltpu.VMEM((CHUNKS, chip_rows, depth), F32),
            pltpu.VMEM((CHUNKS, chip_rows, depth), F32),
            pltpu.VMEM((CHUNKS, chip_rows, depth), F32),
            DMA((pieces,)), DMA((count,)), DMA((count,)), DMA((CHUNKS,)), DMA((CHUNKS,)), DMA((CHUNKS,)), DMA((CHUNKS,)),
            DMA((2 * CHUNKS,)), DMA((2 * CHUNKS,)), DMA((3 * CHUNKS,)), DMA((3 * CHUNKS,)),
            DMA((4 * CHUNKS,)), DMA((4 * CHUNKS,)),
        ]

        def params(collective_id, limit):
            return pltpu.CompilerParams(collective_id=collective_id, has_side_effects=True, vmem_limit_bytes=limit * MIB)

        query, kv_new, residual, k_vmem, v_vmem = pl.pallas_call(
            functools.partial(first_kernel, count),
            out_shape=project_out,
            in_specs=[ANY_SPEC] * 6,
            out_specs=(VMEM_SPEC,) * 5,
            scratch_shapes=project_scratch + [DMA((pieces,))] + project_sems,
            compiler_params=params(0, 16),
            name="first",
        )(x, w_query, w_key, w_value, k_cache, v_cache)

        k_new_cache = v_new_cache = None
        for layer in range(layers):
            last = layer == layers - 1
            operands = [cache_len, query, kv_new, k_vmem, v_vmem]
            specs = [SMEM_SPEC] + [VMEM_SPEC] * 4
            aliases = {3: 2, 4: 3}
            if layer > 0:
                operands += [k_new_cache, v_new_cache]
                specs += [ANY_SPEC] * 2
                aliases |= {5: 0, 6: 1}
            k_new_cache, v_new_cache, _, _, context = pl.pallas_call(
                functools.partial(attention_kernel, layer),
                out_shape=(
                    pltpu.HBM(k_cache.shape, BF16),
                    pltpu.HBM(v_cache.shape, BF16),
                    pltpu.VMEM(k_cache.shape[1:], BF16),
                    pltpu.VMEM(v_cache.shape[1:], BF16),
                    pltpu.VMEM((heads, local_rows, head_dim), BF16),
                ),
                in_specs=specs,
                out_specs=(ANY_SPEC, ANY_SPEC, VMEM_SPEC, VMEM_SPEC, VMEM_SPEC),
                input_output_aliases=aliases,
                scratch_shapes=[
                    pltpu.VMEM((heads * local_rows, head_dim), F32),
                    pltpu.VMEM((heads * local_rows, head_dim), F32),
                    DMA((2 * PARTS,)),
                ],
                compiler_params=pltpu.CompilerParams(vmem_limit_bytes=16 * MIB),
                name=f"attend{layer}",
            )(*operands)
            if not last:
                query, kv_new, residual, k_vmem, v_vmem = pl.pallas_call(
                    functools.partial(mix_kernel, count, False, layer),
                    out_shape=project_out,
                    in_specs=[VMEM_SPEC] * 2 + [ANY_SPEC] * 6,
                    out_specs=(VMEM_SPEC,) * 5,
                    scratch_shapes=mix_scratch + project_scratch + project_sems,
                    compiler_params=params(1 + layer, 28),
                    name=f"mix{layer}",
                )(context, residual, w_out, w_query, w_key, w_value, k_cache, v_cache)
            else:
                hidden = pl.pallas_call(
                    functools.partial(mix_kernel, count, True, layer),
                    out_shape=pltpu.VMEM((rows, width), BF16),
                    in_specs=[VMEM_SPEC] * 2 + [ANY_SPEC],
                    out_specs=VMEM_SPEC,
                    scratch_shapes=mix_scratch,
                    compiler_params=params(1 + layer, 20),
                    name=f"mix{layer}",
                )(context, residual, w_out)
        return hidden, k_new_cache, v_new_cache

    return jax.shard_map(
        device_step,
        mesh=mesh,
        in_specs=(P("replica", None), P("replica"), P(None, None, "model"), P(), P(), P(None, "model", None), cache_spec, cache_spec),
        out_specs=(P("replica", None), cache_spec, cache_spec),
        check_vma=False,
    )
```

```python
import functools

import jax
import jax.numpy as jnp
from jax import lax
from jax.experimental import pallas as pl
from jax.experimental.pallas import tpu as pltpu
from jax.sharding import PartitionSpec as P

MESH = pl.DeviceIdType.MESH
F32 = jnp.float32
BF16 = jnp.bfloat16
CHIPS = 4
CHUNKS = 8
PARTS = 8
RING = 0
RELAYED = CHUNKS
MIB = 1 << 20

ANY_SPEC = pl.BlockSpec(memory_space=pltpu.HBM)
VMEM_SPEC = pl.BlockSpec(memory_space=pltpu.VMEM)
SMEM_SPEC = pl.BlockSpec(memory_space=pltpu.SMEM)


def to_hbm(value):
    return pltpu.with_memory_space_constraint(value, pltpu.HBM)


def to_vmem(value):
    return pltpu.with_memory_space_constraint(value, pltpu.VMEM)


def aligned(index, size):
    return pl.ds(pl.multiple_of(index * size, size), size)


class Place:
    def __init__(self, count):
        self.count = count
        self.me = lax.axis_index("model")
        self.chip = self.me // 2
        self.core = self.me % 2
        self.right = (self.chip + 1) % CHIPS
        self.left = (self.chip + CHIPS - 1) % CHIPS
        self.across = (self.chip + 2) % CHIPS
        self.to_right = self.right * 2 + self.core
        self.to_left = self.left * 2 + self.core
        self.sibling = self.chip * 2 + (1 - self.core)

    def peer(self, offset):
        return (self.me + offset) % self.count

    def origin(self, offset):
        return (self.me + self.count - offset) % self.count


def remote(src, dst, send_sem, recv_sem, device):
    return pltpu.make_async_remote_copy(
        src_ref=src, dst_ref=dst, send_sem=send_sem, recv_sem=recv_sem,
        device_id={"model": device}, device_id_type=MESH)


def signal_all(place):
    barrier = pltpu.get_barrier_semaphore()
    for offset in send_order(place.count):
        pl.semaphore_signal(barrier, inc=1, device_id={"model": place.peer(offset)}, device_id_type=MESH)


def wait_all(place):
    pl.semaphore_wait(pltpu.get_barrier_semaphore(), place.count - 1)


def weight_copies(layer, wq, wk, wv, wq_buf, wkv_buf, sems):
    pieces = sems.shape[0] - 2
    depth = wq_buf.shape[0] // pieces
    head_dim = wk.shape[-1]
    copies = [
        pltpu.make_async_copy(wq.at[layer, pl.ds(i * depth, depth), :], wq_buf.at[pl.ds(i * depth, depth), :], sems.at[i])
        for i in range(pieces)
    ]
    copies.append(pltpu.make_async_copy(wk.at[layer], wkv_buf.at[:, pl.ds(0, head_dim)], sems.at[pieces]))
    copies.append(pltpu.make_async_copy(wv.at[layer], wkv_buf.at[:, pl.ds(head_dim, head_dim)], sems.at[pieces + 1]))
    return copies


def cache_loads(layer, k_cache, v_cache, k_vmem, v_vmem, sems):
    parts = sems.shape[0] // 2
    step = k_vmem.shape[0] // parts
    copies = []
    for i in range(parts):
        part = pl.ds(i * step, step)
        copies.append(pltpu.make_async_copy(k_cache.at[layer, part], k_vmem.at[part], sems.at[2 * i]))
        copies.append(pltpu.make_async_copy(v_cache.at[layer, part], v_vmem.at[part], sems.at[2 * i + 1]))
    return copies


def add_query(piece, first, hidden, wq_buf, q_acc):
    depth = hidden.shape[-1]
    part = jnp.dot(hidden[piece], wq_buf[aligned(piece, depth), :], preferred_element_type=F32)
    q_acc[...] = part if first else q_acc[...] + part


def new_rows(place, hidden, wkv_buf, kv_new):
    pieces, rows, depth = hidden.shape
    local_rows = rows // place.count
    total = None
    for piece in range(pieces):
        mine = hidden[piece, aligned(place.me, local_rows), :]
        part = jnp.dot(mine, wkv_buf[pl.ds(piece * depth, depth), :], preferred_element_type=F32)
        total = part if total is None else total + part
    kv_new[...] = total.astype(BF16).astype(F32)


def query_copies(place, q_send, q_out, send_sems, recv_sems, incoming):
    heads = q_send.shape[0]
    local_rows = q_out.shape[1]
    copies = []
    for offset in range(1, place.count):
        source = place.origin(offset) if incoming else place.me
        target = place.peer(offset)
        copies.append(remote(
            q_send.at[:, aligned(target, local_rows), :], q_out.at[pl.ds(source * heads, heads)],
            send_sems.at[offset], recv_sems.at[offset], target))
    return copies


def send_order(count):
    return sorted(range(1, count), key=lambda offset: -min(offset, count - offset))


def exchange_query(place, q_acc, q_send, q_out, send_sems, recv_sems):
    heads, rows, head_dim = q_send.shape
    local_rows = q_out.shape[1]
    for head in range(heads):
        q_send[head] = q_acc[:, head * head_dim:(head + 1) * head_dim].astype(BF16)
    outgoing = query_copies(place, q_send, q_out, send_sems, recv_sems, False)
    for offset in send_order(place.count):
        outgoing[offset - 1].start()
    q_out[pl.ds(place.me * heads, heads)] = q_send[:, aligned(place.me, local_rows), :]
    return outgoing


def first_kernel(count, x, wq, wk, wv, k_cache, v_cache,
                 q_out, kv_new, residual, k_vmem, v_vmem,
                 hidden, wq_buf, wkv_buf, q_acc, q_send,
                 x_sems, w_sems, cache_sems, q_ssem, q_rsem):
    place = Place(count)
    pieces, rows, depth = hidden.shape
    x_copies = [
        pltpu.make_async_copy(x.at[:, pl.ds(i * depth, depth)], hidden.at[i], x_sems.at[i]) for i in range(pieces)
    ]
    w_copies = weight_copies(0, wq, wk, wv, wq_buf, wkv_buf, w_sems)
    cache_copies = cache_loads(0, k_cache, v_cache, k_vmem, v_vmem, cache_sems)
    for i in range(pieces):
        x_copies[i].start()
        w_copies[i].start()
    signal_all(place)
    w_copies[pieces].start()
    w_copies[pieces + 1].start()
    for copy in cache_copies:
        copy.start()
    for i in range(pieces):
        x_copies[i].wait()
        w_copies[i].wait()
        add_query(i, i == 0, hidden, wq_buf, q_acc)
    wait_all(place)
    outgoing = exchange_query(place, q_acc, q_send, q_out, q_ssem, q_rsem)
    chip_rows = residual.shape[1]
    for j in range(CHUNKS):
        residual[j] = hidden[place.core * CHUNKS + j, aligned(place.chip, chip_rows), :]
    w_copies[pieces].wait()
    w_copies[pieces + 1].wait()
    new_rows(place, hidden, wkv_buf, kv_new)
    for copy in query_copies(place, q_send, q_out, q_ssem, q_rsem, True):
        copy.wait_recv()
    for copy in outgoing:
        copy.wait_send()
    for copy in cache_copies:
        copy.wait()


def mix_kernel(count, last, layer, *refs):
    refs = list(refs)
    take = lambda k: [refs.pop(0) for _ in range(k)]
    context, residual, wo = take(3)
    if not last:
        wq, wk, wv, k_cache, v_cache = take(5)
        q_out, kv_new, next_residual, k_vmem, v_vmem = take(5)
    else:
        (hidden,) = take(1)
    c_recv, wo_far, wo_own, p_send, p_recv, total, s1_recv, comb, s2_left, s2_right = take(10)
    wo_sems, c_ssem, c_rsem, p_ssem, p_rsem, s1_ssem, s1_rsem = take(7)
    s2_ssem, s2_rsem, ag_ssem, ag_rsem, d2d_ssem, d2d_rsem = take(6)
    if not last:
        hidden, wq_buf, wkv_buf, q_acc, q_send, w_sems, cache_sems, q_ssem, q_rsem = take(9)
    place = Place(count)
    heads, rows, head_dim = c_recv.shape
    local_rows = rows // count
    chip_rows = rows // CHIPS
    depth = total.shape[-1]

    signal_all(place)
    wo_copies = []
    for j in range(CHUNKS):
        wo_copies.append(pltpu.make_async_copy(
            wo.at[layer, :, aligned((1 - place.core) * CHUNKS + j, depth)], wo_far.at[j], wo_sems.at[j]))
    for j in range(CHUNKS):
        wo_copies.append(pltpu.make_async_copy(
            wo.at[layer, :, aligned(place.core * CHUNKS + j, depth)], wo_own.at[j], wo_sems.at[CHUNKS + j]))
    for copy in wo_copies:
        copy.start()
    if not last:
        w_copies = weight_copies(layer + 1, wq, wk, wv, wq_buf, wkv_buf, w_sems)
        cache_copies = cache_loads(layer + 1, k_cache, v_cache, k_vmem, v_vmem, cache_sems)
        for copy in w_copies + cache_copies:
            copy.start()

    c_recv[:, aligned(place.me, local_rows), :] = context[pl.ds(place.me * heads, heads)]
    wait_all(place)

    def context_copy(offset, source):
        target = place.peer(offset)
        return remote(
            context.at[pl.ds(target * heads, heads)], c_recv.at[:, aligned(source, local_rows), :],
            c_ssem.at[offset], c_rsem.at[offset], target)

    sends = []

    def send(copy):
        copy.start()
        sends.append(copy)

    for offset in send_order(count):
        send(context_copy(offset, place.me))
    for offset in range(1, count):
        context_copy(offset, place.origin(offset)).wait_recv()

    def product(weights):
        acc = None
        for pair in range(heads // 2):
            lhs = jnp.concatenate([c_recv[2 * pair], c_recv[2 * pair + 1]], axis=1)
            part = jnp.dot(lhs, weights[pl.ds(pair * 2 * head_dim, 2 * head_dim), :], preferred_element_type=F32)
            acc = part if acc is None else acc + part
        return acc

    def pair_copy(j):
        return remote(p_send.at[j], p_recv.at[j], p_ssem.at[j], p_rsem.at[j], place.sibling)

    def block(chip):
        return aligned(chip, chip_rows)

    for j in range(CHUNKS):
        wo_copies[j].wait()
        p_send[j] = product(wo_far.at[j])
        send(pair_copy(j))

    def step_one(j):
        target = place.to_right if j % 2 == 0 else place.to_left
        if j >= RELAYED:
            target = place.across * 2 + place.core
        return remote(total.at[j, block(place.across), :], s1_recv.at[j], s1_ssem.at[j], s1_rsem.at[j], target)

    def step_two(j, rightward, source):
        target = place.to_right if rightward else place.to_left
        inbox = s2_left if rightward else s2_right
        slot = j if rightward else CHUNKS + j
        return remote(source, inbox.at[j], s2_ssem.at[slot], s2_rsem.at[slot], target)

    def direct(j):
        for rightward in (j % 2 == 1, j % 2 == 0) if j >= RELAYED else (j % 2 == 1,):
            send(step_two(j, rightward, total.at[j, block(place.right if rightward else place.left), :]))

    def combine(j):
        step_one(j).wait_recv()
        rightward = j % 2 == 0
        comb[j] = total[j, block(place.right if rightward else place.left), :] + s1_recv[j]
        send(step_two(j, rightward, comb.at[j]))

    for j in range(CHUNKS):
        wo_copies[CHUNKS + j].wait()
        total[j] = product(wo_own.at[j])
    pending = []
    for j in range(CHUNKS):
        pair_copy(j).wait_recv()
        total[j] += p_recv[j]
        send(step_one(j))
        while pending:
            direct(pending.pop())
        if 0 < j < RELAYED:
            pending.append(j)
        else:
            direct(j)
    for j in range(min(RELAYED, 2)):
        combine(j)
    while pending:
        direct(pending.pop())
    for j in range(2, RELAYED):
        combine(j)

    def piece(core, j):
        return core * CHUNKS + j

    def region(core, j, chip):
        if last:
            return hidden.at[block(chip), aligned(piece(core, j), depth)]
        return hidden.at[piece(core, j), block(chip), :]

    def gather_copy(j, way, chip):
        target = (place.to_right, place.to_left, place.across * 2 + place.core)[way]
        part = region(place.core, j, chip)
        slot = way * CHUNKS + j
        return remote(part, part, ag_ssem.at[slot], ag_rsem.at[slot], target)

    def forward_copy(j, chip):
        target = place.to_right if j % 2 == 0 else place.to_left
        part = region(place.core, j, chip)
        return remote(part, part, ag_ssem.at[2 * CHUNKS + j], ag_rsem.at[2 * CHUNKS + j], target)

    def twin_copy(j, kind, core):
        chip = (place.chip, place.left, place.right, place.across)[kind]
        part = region(core, j, chip)
        slot = kind * CHUNKS + j
        return remote(part, part, d2d_ssem.at[slot], d2d_rsem.at[slot], place.sibling)

    def finish(j):
        step_two(j, True, comb.at[j]).wait_recv()
        step_two(j, False, comb.at[j]).wait_recv()
        summed = total[j, block(place.chip), :] + s2_left[j] + s2_right[j]
        if j >= RELAYED:
            step_one(j).wait_recv()
            summed = summed + s1_recv[j]
        value = (residual[j].astype(F32) + summed).astype(BF16)
        if last:
            hidden[block(place.chip), aligned(piece(place.core, j), depth)] = value
        else:
            hidden[piece(place.core, j), block(place.chip), :] = value
            next_residual[j] = value
        if j >= RING:
            send(gather_copy(j, 2, place.chip))
        send(gather_copy(j, 0, place.chip))
        send(gather_copy(j, 1, place.chip))
        send(twin_copy(j, 0, place.core))

    def pass_on(j):
        gather_copy(j, 0, place.left).wait_recv()
        if j < RING and j % 2 == 0:
            send(forward_copy(j, place.left))
        send(twin_copy(j, 1, place.core))
        gather_copy(j, 1, place.right).wait_recv()
        if j < RING and j % 2 == 1:
            send(forward_copy(j, place.right))
        send(twin_copy(j, 2, place.core))

    def far_block(j):
        gather_copy(j, 2, place.across).wait_recv()
        send(twin_copy(j, 3, place.core))

    for j in range(CHUNKS):
        finish(j)
    for j in range(RING):
        pass_on(j)
    for j in range(CHUNKS):
        if j >= RING:
            pass_on(j)
        far_block(j)
        if not last:
            for copy in w_copies if j == 0 else ():
                copy.wait()
            add_query(piece(place.core, j), j == 0, hidden, wq_buf, q_acc)
    for j in range(CHUNKS):
        for kind in range(4):
            twin_copy(j, kind, 1 - place.core).wait_recv()
        if not last:
            add_query(piece(1 - place.core, j), False, hidden, wq_buf, q_acc)
    if not last:
        outgoing = exchange_query(place, q_acc, q_send, q_out, q_ssem, q_rsem)
        new_rows(place, hidden, wkv_buf, kv_new)
        for copy in query_copies(place, q_send, q_out, q_ssem, q_rsem, True):
            copy.wait_recv()
        sends.extend(outgoing)
        for copy in cache_copies:
            copy.wait()
    for copy in sends:
        copy.wait_send()


GROUP = 8
SHORT = 256


def attention_kernel(layer, *refs):
    all_lens, q, kv_new, k_in, v_in = refs[:5]
    refs = refs[5:]
    if layer > 0:
        refs = refs[2:]
    k_out, v_out, k_buf, v_buf, context, q_rows, c_rows, sems = refs
    del k_in, v_in
    heads, local_rows, head_dim = q.shape
    seq_len = k_buf.shape[1]
    tile = 16
    first_row = lax.axis_index("model") * local_rows

    def length(b):
        return all_lens[first_row + b]

    writes = []
    parts = sems.shape[0] // 2
    step = local_rows // parts
    for i in range(parts):
        for b in range(i * step, (i + 1) * step):
            start = pl.multiple_of((length(b) // tile) * tile, tile)
            here = lax.broadcasted_iota(jnp.int32, (tile, head_dim), 0) == length(b) - start
            for buf, column in ((k_buf, 0), (v_buf, head_dim)):
                fresh = jnp.broadcast_to(kv_new[b:b + 1, column:column + head_dim], (tile, head_dim))
                old = buf[b, pl.ds(start, tile), :].astype(F32)
                buf[b, pl.ds(start, tile), :] = jnp.where(here, fresh, old).astype(BF16)
        part = pl.ds(i * step, step)
        writes.append(pltpu.make_async_copy(k_buf.at[part], k_out.at[layer, part], sems.at[2 * i]))
        writes.append(pltpu.make_async_copy(v_buf.at[part], v_out.at[layer, part], sems.at[2 * i + 1]))
        if i > 0:
            writes[2 * i - 2].start()
            writes[2 * i - 1].start()
    q_rows[...] = q[...].astype(F32).reshape(heads * local_rows, head_dim)
    writes[-2].start()
    writes[-1].start()

    def attend(members, span):
        rows = [pl.ds(b, heads, stride=local_rows) for b in members]
        scores = [
            lax.dot_general(
                q_rows[r, :].astype(BF16), k_buf[b, pl.ds(0, span), :], (((1,), (1,)), ((), ())),
                preferred_element_type=F32)
            for b, r in zip(members, rows)
        ]
        positions = lax.broadcasted_iota(jnp.int32, (heads, span), 1)
        scores = [jnp.where(positions <= length(b), s * (head_dim ** -0.5), -jnp.inf) for b, s in zip(members, scores)]
        tops = [jnp.max(s, axis=1, keepdims=True) for s in scores]
        powers = [jnp.exp(s - t) for s, t in zip(scores, tops)]
        sums = [jnp.sum(p, axis=1, keepdims=True) for p in powers]
        weights = [(p / t).astype(BF16) for p, t in zip(powers, sums)]
        outs = [
            jnp.dot(w, v_buf[b, pl.ds(0, span), :], preferred_element_type=F32) for b, w in zip(members, weights)
        ]
        for r, out in zip(rows, outs):
            c_rows[r, :] = out.astype(BF16).astype(F32)

    for first in range(0, local_rows, GROUP):
        attend(list(range(first, first + GROUP)), SHORT)

    spans = []
    span = 2 * SHORT
    while span < seq_len:
        spans.append(span)
        span *= 2
    spans.append(seq_len)

    def longer(b, _):
        @pl.when(length(b) >= SHORT)
        def _():
            low = SHORT
            for span in spans:
                @pl.when(jnp.logical_and(length(b) >= low, length(b) < span))
                def _(span=span):
                    attend([b], span)
                low = span
        return 0

    lax.fori_loop(0, local_rows, longer, 0)
    context[...] = c_rows[...].reshape(heads, local_rows, head_dim).astype(BF16)
    for copy in writes:
        copy.wait()


def solution(mesh):
    count = mesh.shape["model"]
    assert count == 2 * CHIPS
    row_axes = ("replica", "model")
    cache_spec = P(None, row_axes, None, None)
    DMA = pltpu.SemaphoreType.DMA

    def device_step(x, cache_len, w_query, w_key, w_value, w_out, k_cache, v_cache):
        rows, width = x.shape
        layers, local_rows, seq_len, head_dim = k_cache.shape
        local_width = w_query.shape[-1]
        local_heads = local_width // head_dim
        heads = local_heads * count
        pieces = 2 * CHUNKS
        depth = width // pieces
        chip_rows = rows // CHIPS
        w_query, w_key, w_value, w_out = map(to_hbm, (w_query, w_key, w_value, w_out))
        x, k_cache, v_cache = map(to_hbm, (x, k_cache, v_cache))

        project_out = (
            pltpu.VMEM((heads, local_rows, head_dim), BF16),
            pltpu.VMEM((local_rows, 2 * head_dim), F32),
            pltpu.VMEM((CHUNKS, chip_rows, depth), BF16),
            pltpu.VMEM(k_cache.shape[1:], BF16),
            pltpu.VMEM(v_cache.shape[1:], BF16),
        )
        project_scratch = [
            pltpu.VMEM((pieces, rows, depth), BF16),
            pltpu.VMEM((width, local_width), BF16),
            pltpu.VMEM((width, 2 * head_dim), BF16),
            pltpu.VMEM((rows, local_width), F32),
            pltpu.VMEM((local_heads, rows, head_dim), BF16),
        ]
        project_sems = [DMA((pieces + 2,)), DMA((2 * PARTS,)), DMA((count,)), DMA((count,))]
        mix_scratch = [
            pltpu.VMEM((local_heads, rows, head_dim), BF16),
            pltpu.VMEM((CHUNKS, local_width, depth), BF16),
            pltpu.VMEM((CHUNKS, local_width, depth), BF16),
            pltpu.VMEM((CHUNKS, rows, depth), F32),
            pltpu.VMEM((CHUNKS, rows, depth), F32),
            pltpu.VMEM((CHUNKS, rows, depth), F32),
            pltpu.VMEM((CHUNKS, chip_rows, depth), F32),
            pltpu.VMEM((CHUNKS, chip_rows, depth), F32),
            pltpu.VMEM((CHUNKS, chip_rows, depth), F32),
            pltpu.VMEM((CHUNKS, chip_rows, depth), F32),
            DMA((pieces,)), DMA((count,)), DMA((count,)), DMA((CHUNKS,)), DMA((CHUNKS,)), DMA((CHUNKS,)), DMA((CHUNKS,)),
            DMA((2 * CHUNKS,)), DMA((2 * CHUNKS,)), DMA((3 * CHUNKS,)), DMA((3 * CHUNKS,)),
            DMA((4 * CHUNKS,)), DMA((4 * CHUNKS,)),
        ]

        def params(collective_id, limit):
            return pltpu.CompilerParams(collective_id=collective_id, has_side_effects=True, vmem_limit_bytes=limit * MIB)

        query, kv_new, residual, k_vmem, v_vmem = pl.pallas_call(
            functools.partial(first_kernel, count),
            out_shape=project_out,
            in_specs=[ANY_SPEC] * 6,
            out_specs=(VMEM_SPEC,) * 5,
            scratch_shapes=project_scratch + [DMA((pieces,))] + project_sems,
            compiler_params=params(0, 16),
            name="first",
        )(x, w_query, w_key, w_value, k_cache, v_cache)

        k_new_cache = v_new_cache = None
        for layer in range(layers):
            last = layer == layers - 1
            operands = [cache_len, query, kv_new, k_vmem, v_vmem]
            specs = [SMEM_SPEC] + [VMEM_SPEC] * 4
            aliases = {3: 2, 4: 3}
            if layer > 0:
                operands += [k_new_cache, v_new_cache]
                specs += [ANY_SPEC] * 2
                aliases |= {5: 0, 6: 1}
            k_new_cache, v_new_cache, _, _, context = pl.pallas_call(
                functools.partial(attention_kernel, layer),
                out_shape=(
                    pltpu.HBM(k_cache.shape, BF16),
                    pltpu.HBM(v_cache.shape, BF16),
                    pltpu.VMEM(k_cache.shape[1:], BF16),
                    pltpu.VMEM(v_cache.shape[1:], BF16),
                    pltpu.VMEM((heads, local_rows, head_dim), BF16),
                ),
                in_specs=specs,
                out_specs=(ANY_SPEC, ANY_SPEC, VMEM_SPEC, VMEM_SPEC, VMEM_SPEC),
                input_output_aliases=aliases,
                scratch_shapes=[
                    pltpu.VMEM((heads * local_rows, head_dim), F32),
                    pltpu.VMEM((heads * local_rows, head_dim), F32),
                    DMA((2 * PARTS,)),
                ],
                compiler_params=pltpu.CompilerParams(vmem_limit_bytes=16 * MIB),
                name=f"attend{layer}",
            )(*operands)
            if not last:
                query, kv_new, residual, k_vmem, v_vmem = pl.pallas_call(
                    functools.partial(mix_kernel, count, False, layer),
                    out_shape=project_out,
                    in_specs=[VMEM_SPEC] * 2 + [ANY_SPEC] * 6,
                    out_specs=(VMEM_SPEC,) * 5,
                    scratch_shapes=mix_scratch + project_scratch + project_sems,
                    compiler_params=params(1 + layer, 28),
                    name=f"mix{layer}",
                )(context, residual, w_out, w_query, w_key, w_value, k_cache, v_cache)
            else:
                hidden = pl.pallas_call(
                    functools.partial(mix_kernel, count, True, layer),
                    out_shape=pltpu.VMEM((rows, width), BF16),
                    in_specs=[VMEM_SPEC] * 2 + [ANY_SPEC],
                    out_specs=VMEM_SPEC,
                    scratch_shapes=mix_scratch,
                    compiler_params=params(1 + layer, 20),
                    name=f"mix{layer}",
                )(context, residual, w_out)
        return hidden, k_new_cache, v_new_cache

    return jax.shard_map(
        device_step,
        mesh=mesh,
        in_specs=(P("replica", None), P("replica"), P(None, None, "model"), P(), P(), P(None, "model", None), cache_spec, cache_spec),
        out_specs=(P("replica", None), cache_spec, cache_spec),
        check_vma=False,
    )
```

```python
import functools

import jax
import jax.numpy as jnp
from jax import lax
from jax.experimental import pallas as pl
from jax.experimental.pallas import tpu as pltpu
from jax.sharding import PartitionSpec as P

MESH = pl.DeviceIdType.MESH
F32 = jnp.float32
BF16 = jnp.bfloat16
CHIPS = 4
CHUNKS = 4
PARTS = 8
RING = 0
RELAYED = 4
MIB = 1 << 20

ANY_SPEC = pl.BlockSpec(memory_space=pltpu.HBM)
VMEM_SPEC = pl.BlockSpec(memory_space=pltpu.VMEM)
SMEM_SPEC = pl.BlockSpec(memory_space=pltpu.SMEM)


def to_hbm(value):
    return pltpu.with_memory_space_constraint(value, pltpu.HBM)


def to_vmem(value):
    return pltpu.with_memory_space_constraint(value, pltpu.VMEM)


def aligned(index, size):
    return pl.ds(pl.multiple_of(index * size, size), size)


class Place:
    def __init__(self, count):
        self.count = count
        self.me = lax.axis_index("model")
        self.chip = self.me // 2
        self.core = self.me % 2
        self.right = (self.chip + 1) % CHIPS
        self.left = (self.chip + CHIPS - 1) % CHIPS
        self.across = (self.chip + 2) % CHIPS
        self.to_right = self.right * 2 + self.core
        self.to_left = self.left * 2 + self.core
        self.sibling = self.chip * 2 + (1 - self.core)

    def peer(self, offset):
        return (self.me + offset) % self.count

    def origin(self, offset):
        return (self.me + self.count - offset) % self.count


def remote(src, dst, send_sem, recv_sem, device):
    return pltpu.make_async_remote_copy(
        src_ref=src, dst_ref=dst, send_sem=send_sem, recv_sem=recv_sem,
        device_id={"model": device}, device_id_type=MESH)


def signal_all(place):
    barrier = pltpu.get_barrier_semaphore()
    for offset in send_order(place.count):
        pl.semaphore_signal(barrier, inc=1, device_id={"model": place.peer(offset)}, device_id_type=MESH)


def wait_all(place):
    pl.semaphore_wait(pltpu.get_barrier_semaphore(), place.count - 1)


def weight_copies(layer, wq, wk, wv, wq_buf, wkv_buf, sems):
    pieces = sems.shape[0] - 2
    depth = wq_buf.shape[0] // pieces
    head_dim = wk.shape[-1]
    copies = [
        pltpu.make_async_copy(wq.at[layer, pl.ds(i * depth, depth), :], wq_buf.at[pl.ds(i * depth, depth), :], sems.at[i])
        for i in range(pieces)
    ]
    copies.append(pltpu.make_async_copy(wk.at[layer], wkv_buf.at[:, pl.ds(0, head_dim)], sems.at[pieces]))
    copies.append(pltpu.make_async_copy(wv.at[layer], wkv_buf.at[:, pl.ds(head_dim, head_dim)], sems.at[pieces + 1]))
    return copies


def cache_loads(layer, k_cache, v_cache, k_vmem, v_vmem, sems):
    parts = sems.shape[0] // 2
    step = k_vmem.shape[0] // parts
    copies = []
    for i in range(parts):
        part = pl.ds(i * step, step)
        copies.append(pltpu.make_async_copy(k_cache.at[layer, part], k_vmem.at[part], sems.at[2 * i]))
        copies.append(pltpu.make_async_copy(v_cache.at[layer, part], v_vmem.at[part], sems.at[2 * i + 1]))
    return copies


def add_query(piece, first, hidden, wq_buf, q_acc):
    depth = hidden.shape[-1]
    part = jnp.dot(hidden[piece], wq_buf[aligned(piece, depth), :], preferred_element_type=F32)
    q_acc[...] = part if first else q_acc[...] + part


def new_rows(place, hidden, wkv_buf, kv_new):
    pieces, rows, depth = hidden.shape
    local_rows = rows // place.count
    total = None
    for piece in range(pieces):
        mine = hidden[piece, aligned(place.me, local_rows), :]
        part = jnp.dot(mine, wkv_buf[pl.ds(piece * depth, depth), :], preferred_element_type=F32)
        total = part if total is None else total + part
    kv_new[...] = total.astype(BF16).astype(F32)


def query_copies(place, q_send, q_out, send_sems, recv_sems, incoming):
    heads = q_send.shape[0]
    local_rows = q_out.shape[1]
    copies = []
    for offset in range(1, place.count):
        source = place.origin(offset) if incoming else place.me
        target = place.peer(offset)
        copies.append(remote(
            q_send.at[:, aligned(target, local_rows), :], q_out.at[pl.ds(source * heads, heads)],
            send_sems.at[offset], recv_sems.at[offset], target))
    return copies


def send_order(count):
    return sorted(range(1, count), key=lambda offset: -min(offset, count - offset))


def exchange_query(place, q_acc, q_send, q_out, send_sems, recv_sems):
    heads, rows, head_dim = q_send.shape
    local_rows = q_out.shape[1]
    for head in range(heads):
        q_send[head] = q_acc[:, head * head_dim:(head + 1) * head_dim].astype(BF16)
    outgoing = query_copies(place, q_send, q_out, send_sems, recv_sems, False)
    for offset in send_order(place.count):
        outgoing[offset - 1].start()
    q_out[pl.ds(place.me * heads, heads)] = q_send[:, aligned(place.me, local_rows), :]
    return outgoing


def first_kernel(count, x, wq, wk, wv, k_cache, v_cache,
                 q_out, kv_new, residual, k_vmem, v_vmem,
                 hidden, wq_buf, wkv_buf, q_acc, q_send,
                 x_sems, w_sems, cache_sems, q_ssem, q_rsem):
    place = Place(count)
    pieces, rows, depth = hidden.shape
    x_copies = [
        pltpu.make_async_copy(x.at[:, pl.ds(i * depth, depth)], hidden.at[i], x_sems.at[i]) for i in range(pieces)
    ]
    w_copies = weight_copies(0, wq, wk, wv, wq_buf, wkv_buf, w_sems)
    cache_copies = cache_loads(0, k_cache, v_cache, k_vmem, v_vmem, cache_sems)
    for i in range(pieces):
        x_copies[i].start()
        w_copies[i].start()
    signal_all(place)
    w_copies[pieces].start()
    w_copies[pieces + 1].start()
    for copy in cache_copies:
        copy.start()
    for i in range(pieces):
        x_copies[i].wait()
        w_copies[i].wait()
        add_query(i, i == 0, hidden, wq_buf, q_acc)
    wait_all(place)
    outgoing = exchange_query(place, q_acc, q_send, q_out, q_ssem, q_rsem)
    chip_rows = residual.shape[1]
    for j in range(CHUNKS):
        residual[j] = hidden[place.core * CHUNKS + j, aligned(place.chip, chip_rows), :]
    w_copies[pieces].wait()
    w_copies[pieces + 1].wait()
    new_rows(place, hidden, wkv_buf, kv_new)
    for copy in query_copies(place, q_send, q_out, q_ssem, q_rsem, True):
        copy.wait_recv()
    for copy in outgoing:
        copy.wait_send()
    for copy in cache_copies:
        copy.wait()


def mix_kernel(count, last, layer, *refs):
    refs = list(refs)
    take = lambda k: [refs.pop(0) for _ in range(k)]
    context, residual, wo = take(3)
    if not last:
        wq, wk, wv, k_cache, v_cache = take(5)
        q_out, kv_new, next_residual, k_vmem, v_vmem = take(5)
    else:
        (hidden,) = take(1)
    c_recv, wo_far, wo_own, p_send, p_recv, total, s1_recv, comb, s2_left, s2_right = take(10)
    wo_sems, c_ssem, c_rsem, p_ssem, p_rsem, s1_ssem, s1_rsem = take(7)
    s2_ssem, s2_rsem, ag_ssem, ag_rsem, d2d_ssem, d2d_rsem = take(6)
    if not last:
        hidden, wq_buf, wkv_buf, q_acc, q_send, w_sems, cache_sems, q_ssem, q_rsem = take(9)
    place = Place(count)
    heads, rows, head_dim = c_recv.shape
    local_rows = rows // count
    chip_rows = rows // CHIPS
    depth = total.shape[-1]

    signal_all(place)
    wo_copies = []
    for j in range(CHUNKS):
        wo_copies.append(pltpu.make_async_copy(
            wo.at[layer, :, aligned((1 - place.core) * CHUNKS + j, depth)], wo_far.at[j], wo_sems.at[j]))
    for j in range(CHUNKS):
        wo_copies.append(pltpu.make_async_copy(
            wo.at[layer, :, aligned(place.core * CHUNKS + j, depth)], wo_own.at[j], wo_sems.at[CHUNKS + j]))
    for copy in wo_copies:
        copy.start()
    if not last:
        w_copies = weight_copies(layer + 1, wq, wk, wv, wq_buf, wkv_buf, w_sems)
        cache_copies = cache_loads(layer + 1, k_cache, v_cache, k_vmem, v_vmem, cache_sems)
        for copy in w_copies + cache_copies:
            copy.start()

    c_recv[:, aligned(place.me, local_rows), :] = context[pl.ds(place.me * heads, heads)]
    wait_all(place)

    def context_copy(offset, source):
        target = place.peer(offset)
        return remote(
            context.at[pl.ds(target * heads, heads)], c_recv.at[:, aligned(source, local_rows), :],
            c_ssem.at[offset], c_rsem.at[offset], target)

    sends = []

    def send(copy):
        copy.start()
        sends.append(copy)

    for offset in send_order(count):
        send(context_copy(offset, place.me))
    for offset in range(1, count):
        context_copy(offset, place.origin(offset)).wait_recv()

    def product(weights):
        acc = None
        for pair in range(heads // 2):
            lhs = jnp.concatenate([c_recv[2 * pair], c_recv[2 * pair + 1]], axis=1)
            part = jnp.dot(lhs, weights[pl.ds(pair * 2 * head_dim, 2 * head_dim), :], preferred_element_type=F32)
            acc = part if acc is None else acc + part
        return acc

    def pair_copy(j):
        return remote(p_send.at[j], p_recv.at[j], p_ssem.at[j], p_rsem.at[j], place.sibling)

    def block(chip):
        return aligned(chip, chip_rows)

    for j in range(CHUNKS):
        wo_copies[j].wait()
        p_send[j] = product(wo_far.at[j])
        send(pair_copy(j))

    def step_one(j):
        target = place.to_right if j % 2 == 0 else place.to_left
        if j >= RELAYED:
            target = place.across * 2 + place.core
        return remote(total.at[j, block(place.across), :], s1_recv.at[j], s1_ssem.at[j], s1_rsem.at[j], target)

    def step_two(j, rightward, source):
        target = place.to_right if rightward else place.to_left
        inbox = s2_left if rightward else s2_right
        slot = j if rightward else CHUNKS + j
        return remote(source, inbox.at[j], s2_ssem.at[slot], s2_rsem.at[slot], target)

    def direct(j):
        for rightward in (j % 2 == 1, j % 2 == 0) if j >= RELAYED else (j % 2 == 1,):
            send(step_two(j, rightward, total.at[j, block(place.right if rightward else place.left), :]))

    def combine(j):
        step_one(j).wait_recv()
        rightward = j % 2 == 0
        comb[j] = total[j, block(place.right if rightward else place.left), :] + s1_recv[j]
        send(step_two(j, rightward, comb.at[j]))

    for j in range(CHUNKS):
        wo_copies[CHUNKS + j].wait()
        total[j] = product(wo_own.at[j])
    pending = []
    for j in range(CHUNKS):
        pair_copy(j).wait_recv()
        total[j] += p_recv[j]
        send(step_one(j))
        while pending:
            direct(pending.pop())
        if 0 < j < RELAYED:
            pending.append(j)
        else:
            direct(j)
    for j in range(min(RELAYED, 2)):
        combine(j)
    while pending:
        direct(pending.pop())
    for j in range(2, RELAYED):
        combine(j)

    def piece(core, j):
        return core * CHUNKS + j

    def region(core, j, chip):
        if last:
            return hidden.at[block(chip), aligned(piece(core, j), depth)]
        return hidden.at[piece(core, j), block(chip), :]

    def gather_copy(j, way, chip):
        target = (place.to_right, place.to_left, place.across * 2 + place.core)[way]
        part = region(place.core, j, chip)
        slot = way * CHUNKS + j
        return remote(part, part, ag_ssem.at[slot], ag_rsem.at[slot], target)

    def forward_copy(j, chip):
        target = place.to_right if j % 2 == 0 else place.to_left
        part = region(place.core, j, chip)
        return remote(part, part, ag_ssem.at[2 * CHUNKS + j], ag_rsem.at[2 * CHUNKS + j], target)

    def twin_copy(j, core):
        part = hidden.at[:, aligned(piece(core, j), depth)] if last else hidden.at[piece(core, j)]
        return remote(part, part, d2d_ssem.at[j], d2d_rsem.at[j], place.sibling)

    def finish(j):
        step_two(j, True, comb.at[j]).wait_recv()
        step_two(j, False, comb.at[j]).wait_recv()
        summed = total[j, block(place.chip), :] + s2_left[j] + s2_right[j]
        if j >= RELAYED:
            step_one(j).wait_recv()
            summed = summed + s1_recv[j]
        value = (residual[j].astype(F32) + summed).astype(BF16)
        if last:
            hidden[block(place.chip), aligned(piece(place.core, j), depth)] = value
        else:
            hidden[piece(place.core, j), block(place.chip), :] = value
            next_residual[j] = value
        if j >= RING:
            send(gather_copy(j, 2, place.chip))
        send(gather_copy(j, 0, place.chip))
        send(gather_copy(j, 1, place.chip))

    def pass_on(j):
        gather_copy(j, 0, place.left).wait_recv()
        if j < RING and j % 2 == 0:
            send(forward_copy(j, place.left))
        gather_copy(j, 1, place.right).wait_recv()
        if j < RING and j % 2 == 1:
            send(forward_copy(j, place.right))

    def far_block(j):
        gather_copy(j, 2, place.across).wait_recv()
        send(twin_copy(j, place.core))

    for j in range(CHUNKS):
        finish(j)
    for j in range(RING):
        pass_on(j)
    for j in range(CHUNKS):
        if j >= RING:
            pass_on(j)
        far_block(j)
        if not last:
            for copy in w_copies if j == 0 else ():
                copy.wait()
            add_query(piece(place.core, j), j == 0, hidden, wq_buf, q_acc)
    for j in range(CHUNKS):
        twin_copy(j, 1 - place.core).wait_recv()
        if not last:
            add_query(piece(1 - place.core, j), False, hidden, wq_buf, q_acc)
    if not last:
        outgoing = exchange_query(place, q_acc, q_send, q_out, q_ssem, q_rsem)
        new_rows(place, hidden, wkv_buf, kv_new)
        for copy in query_copies(place, q_send, q_out, q_ssem, q_rsem, True):
            copy.wait_recv()
        sends.extend(outgoing)
        for copy in cache_copies:
            copy.wait()
    for copy in sends:
        copy.wait_send()


GROUP = 8
SHORT = 256


def attention_kernel(layer, *refs):
    all_lens, q, kv_new, k_in, v_in = refs[:5]
    refs = refs[5:]
    if layer > 0:
        refs = refs[2:]
    k_out, v_out, k_buf, v_buf, context, q_rows, c_rows, sems = refs
    del k_in, v_in
    heads, local_rows, head_dim = q.shape
    seq_len = k_buf.shape[1]
    tile = 16
    first_row = lax.axis_index("model") * local_rows

    def length(b):
        return all_lens[first_row + b]

    writes = []
    parts = sems.shape[0] // 2
    step = local_rows // parts
    for i in range(parts):
        for b in range(i * step, (i + 1) * step):
            start = pl.multiple_of((length(b) // tile) * tile, tile)
            here = lax.broadcasted_iota(jnp.int32, (tile, head_dim), 0) == length(b) - start
            for buf, column in ((k_buf, 0), (v_buf, head_dim)):
                fresh = jnp.broadcast_to(kv_new[b:b + 1, column:column + head_dim], (tile, head_dim))
                old = buf[b, pl.ds(start, tile), :].astype(F32)
                buf[b, pl.ds(start, tile), :] = jnp.where(here, fresh, old).astype(BF16)
        part = pl.ds(i * step, step)
        writes.append(pltpu.make_async_copy(k_buf.at[part], k_out.at[layer, part], sems.at[2 * i]))
        writes.append(pltpu.make_async_copy(v_buf.at[part], v_out.at[layer, part], sems.at[2 * i + 1]))
        if i > 0:
            writes[2 * i - 2].start()
            writes[2 * i - 1].start()
    q_rows[...] = q[...].astype(F32).reshape(heads * local_rows, head_dim)
    writes[-2].start()
    writes[-1].start()

    def attend(members, span):
        rows = [pl.ds(b, heads, stride=local_rows) for b in members]
        scores = [
            lax.dot_general(
                q_rows[r, :].astype(BF16), k_buf[b, pl.ds(0, span), :], (((1,), (1,)), ((), ())),
                preferred_element_type=F32)
            for b, r in zip(members, rows)
        ]
        positions = lax.broadcasted_iota(jnp.int32, (heads, span), 1)
        scores = [jnp.where(positions <= length(b), s * (head_dim ** -0.5), -jnp.inf) for b, s in zip(members, scores)]
        tops = [jnp.max(s, axis=1, keepdims=True) for s in scores]
        powers = [jnp.exp(s - t) for s, t in zip(scores, tops)]
        sums = [jnp.sum(p, axis=1, keepdims=True) for p in powers]
        weights = [(p / t).astype(BF16) for p, t in zip(powers, sums)]
        outs = [
            jnp.dot(w, v_buf[b, pl.ds(0, span), :], preferred_element_type=F32) for b, w in zip(members, weights)
        ]
        for r, out in zip(rows, outs):
            c_rows[r, :] = out.astype(BF16).astype(F32)

    for first in range(0, local_rows, GROUP):
        attend(list(range(first, first + GROUP)), SHORT)

    spans = []
    span = 2 * SHORT
    while span < seq_len:
        spans.append(span)
        span *= 2
    spans.append(seq_len)

    def longer(b, _):
        @pl.when(length(b) >= SHORT)
        def _():
            low = SHORT
            for span in spans:
                @pl.when(jnp.logical_and(length(b) >= low, length(b) < span))
                def _(span=span):
                    attend([b], span)
                low = span
        return 0

    lax.fori_loop(0, local_rows, longer, 0)
    context[...] = c_rows[...].reshape(heads, local_rows, head_dim).astype(BF16)
    for copy in writes:
        copy.wait()


def solution(mesh):
    count = mesh.shape["model"]
    assert count == 2 * CHIPS
    row_axes = ("replica", "model")
    cache_spec = P(None, row_axes, None, None)
    DMA = pltpu.SemaphoreType.DMA

    def device_step(x, cache_len, w_query, w_key, w_value, w_out, k_cache, v_cache):
        rows, width = x.shape
        layers, local_rows, seq_len, head_dim = k_cache.shape
        local_width = w_query.shape[-1]
        local_heads = local_width // head_dim
        heads = local_heads * count
        pieces = 2 * CHUNKS
        depth = width // pieces
        chip_rows = rows // CHIPS
        w_query, w_key, w_value, w_out = map(to_hbm, (w_query, w_key, w_value, w_out))
        x, k_cache, v_cache = map(to_hbm, (x, k_cache, v_cache))

        project_out = (
            pltpu.VMEM((heads, local_rows, head_dim), BF16),
            pltpu.VMEM((local_rows, 2 * head_dim), F32),
            pltpu.VMEM((CHUNKS, chip_rows, depth), BF16),
            pltpu.VMEM(k_cache.shape[1:], BF16),
            pltpu.VMEM(v_cache.shape[1:], BF16),
        )
        project_scratch = [
            pltpu.VMEM((pieces, rows, depth), BF16),
            pltpu.VMEM((width, local_width), BF16),
            pltpu.VMEM((width, 2 * head_dim), BF16),
            pltpu.VMEM((rows, local_width), F32),
            pltpu.VMEM((local_heads, rows, head_dim), BF16),
        ]
        project_sems = [DMA((pieces + 2,)), DMA((2 * PARTS,)), DMA((count,)), DMA((count,))]
        mix_scratch = [
            pltpu.VMEM((local_heads, rows, head_dim), BF16),
            pltpu.VMEM((CHUNKS, local_width, depth), BF16),
            pltpu.VMEM((CHUNKS, local_width, depth), BF16),
            pltpu.VMEM((CHUNKS, rows, depth), F32),
            pltpu.VMEM((CHUNKS, rows, depth), F32),
            pltpu.VMEM((CHUNKS, rows, depth), F32),
            pltpu.VMEM((CHUNKS, chip_rows, depth), F32),
            pltpu.VMEM((CHUNKS, chip_rows, depth), F32),
            pltpu.VMEM((CHUNKS, chip_rows, depth), F32),
            pltpu.VMEM((CHUNKS, chip_rows, depth), F32),
            DMA((pieces,)), DMA((count,)), DMA((count,)), DMA((CHUNKS,)), DMA((CHUNKS,)), DMA((CHUNKS,)), DMA((CHUNKS,)),
            DMA((2 * CHUNKS,)), DMA((2 * CHUNKS,)), DMA((3 * CHUNKS,)), DMA((3 * CHUNKS,)),
            DMA((CHUNKS,)), DMA((CHUNKS,)),
        ]

        def params(collective_id, limit):
            return pltpu.CompilerParams(collective_id=collective_id, has_side_effects=True, vmem_limit_bytes=limit * MIB)

        query, kv_new, residual, k_vmem, v_vmem = pl.pallas_call(
            functools.partial(first_kernel, count),
            out_shape=project_out,
            in_specs=[ANY_SPEC] * 6,
            out_specs=(VMEM_SPEC,) * 5,
            scratch_shapes=project_scratch + [DMA((pieces,))] + project_sems,
            compiler_params=params(0, 16),
            name="first",
        )(x, w_query, w_key, w_value, k_cache, v_cache)

        k_new_cache = v_new_cache = None
        for layer in range(layers):
            last = layer == layers - 1
            operands = [cache_len, query, kv_new, k_vmem, v_vmem]
            specs = [SMEM_SPEC] + [VMEM_SPEC] * 4
            aliases = {3: 2, 4: 3}
            if layer > 0:
                operands += [k_new_cache, v_new_cache]
                specs += [ANY_SPEC] * 2
                aliases |= {5: 0, 6: 1}
            k_new_cache, v_new_cache, _, _, context = pl.pallas_call(
                functools.partial(attention_kernel, layer),
                out_shape=(
                    pltpu.HBM(k_cache.shape, BF16),
                    pltpu.HBM(v_cache.shape, BF16),
                    pltpu.VMEM(k_cache.shape[1:], BF16),
                    pltpu.VMEM(v_cache.shape[1:], BF16),
                    pltpu.VMEM((heads, local_rows, head_dim), BF16),
                ),
                in_specs=specs,
                out_specs=(ANY_SPEC, ANY_SPEC, VMEM_SPEC, VMEM_SPEC, VMEM_SPEC),
                input_output_aliases=aliases,
                scratch_shapes=[
                    pltpu.VMEM((heads * local_rows, head_dim), F32),
                    pltpu.VMEM((heads * local_rows, head_dim), F32),
                    DMA((2 * PARTS,)),
                ],
                compiler_params=pltpu.CompilerParams(vmem_limit_bytes=16 * MIB),
                name=f"attend{layer}",
            )(*operands)
            if not last:
                query, kv_new, residual, k_vmem, v_vmem = pl.pallas_call(
                    functools.partial(mix_kernel, count, False, layer),
                    out_shape=project_out,
                    in_specs=[VMEM_SPEC] * 2 + [ANY_SPEC] * 6,
                    out_specs=(VMEM_SPEC,) * 5,
                    scratch_shapes=mix_scratch + project_scratch + project_sems,
                    compiler_params=params(1 + layer, 28),
                    name=f"mix{layer}",
                )(context, residual, w_out, w_query, w_key, w_value, k_cache, v_cache)
            else:
                hidden = pl.pallas_call(
                    functools.partial(mix_kernel, count, True, layer),
                    out_shape=pltpu.VMEM((rows, width), BF16),
                    in_specs=[VMEM_SPEC] * 2 + [ANY_SPEC],
                    out_specs=VMEM_SPEC,
                    scratch_shapes=mix_scratch,
                    compiler_params=params(1 + layer, 20),
                    name=f"mix{layer}",
                )(context, residual, w_out)
        return hidden, k_new_cache, v_new_cache

    return jax.shard_map(
        device_step,
        mesh=mesh,
        in_specs=(P("replica", None), P("replica"), P(None, None, "model"), P(), P(), P(None, "model", None), cache_spec, cache_spec),
        out_specs=(P("replica", None), cache_spec, cache_spec),
        check_vma=False,
    )
```

```python
import functools

import jax
import jax.numpy as jnp
from jax import lax
from jax.experimental import pallas as pl
from jax.experimental.pallas import tpu as pltpu
from jax.sharding import PartitionSpec as P

MESH = pl.DeviceIdType.MESH
F32 = jnp.float32
BF16 = jnp.bfloat16
CHIPS = 4
CHUNKS = 4
PARTS = 8
RING = 2
RELAYED = 4
MIB = 1 << 20

ANY_SPEC = pl.BlockSpec(memory_space=pltpu.HBM)
VMEM_SPEC = pl.BlockSpec(memory_space=pltpu.VMEM)
SMEM_SPEC = pl.BlockSpec(memory_space=pltpu.SMEM)


def to_hbm(value):
    return pltpu.with_memory_space_constraint(value, pltpu.HBM)


def to_vmem(value):
    return pltpu.with_memory_space_constraint(value, pltpu.VMEM)


def aligned(index, size):
    return pl.ds(pl.multiple_of(index * size, size), size)


class Place:
    def __init__(self, count):
        self.count = count
        self.me = lax.axis_index("model")
        self.chip = self.me // 2
        self.core = self.me % 2
        self.right = (self.chip + 1) % CHIPS
        self.left = (self.chip + CHIPS - 1) % CHIPS
        self.across = (self.chip + 2) % CHIPS
        self.to_right = self.right * 2 + self.core
        self.to_left = self.left * 2 + self.core
        self.sibling = self.chip * 2 + (1 - self.core)

    def peer(self, offset):
        return (self.me + offset) % self.count

    def origin(self, offset):
        return (self.me + self.count - offset) % self.count


def remote(src, dst, send_sem, recv_sem, device):
    return pltpu.make_async_remote_copy(
        src_ref=src, dst_ref=dst, send_sem=send_sem, recv_sem=recv_sem,
        device_id={"model": device}, device_id_type=MESH)


def signal_all(place):
    barrier = pltpu.get_barrier_semaphore()
    for offset in send_order(place.count):
        pl.semaphore_signal(barrier, inc=1, device_id={"model": place.peer(offset)}, device_id_type=MESH)


def wait_all(place):
    pl.semaphore_wait(pltpu.get_barrier_semaphore(), place.count - 1)


def weight_copies(layer, wq, wk, wv, wq_buf, wkv_buf, sems):
    pieces = sems.shape[0] - 2
    depth = wq_buf.shape[0] // pieces
    head_dim = wk.shape[-1]
    copies = [
        pltpu.make_async_copy(wq.at[layer, pl.ds(i * depth, depth), :], wq_buf.at[pl.ds(i * depth, depth), :], sems.at[i])
        for i in range(pieces)
    ]
    copies.append(pltpu.make_async_copy(wk.at[layer], wkv_buf.at[:, pl.ds(0, head_dim)], sems.at[pieces]))
    copies.append(pltpu.make_async_copy(wv.at[layer], wkv_buf.at[:, pl.ds(head_dim, head_dim)], sems.at[pieces + 1]))
    return copies


def cache_loads(layer, k_cache, v_cache, k_vmem, v_vmem, sems):
    parts = sems.shape[0] // 2
    step = k_vmem.shape[0] // parts
    copies = []
    for i in range(parts):
        part = pl.ds(i * step, step)
        copies.append(pltpu.make_async_copy(k_cache.at[layer, part], k_vmem.at[part], sems.at[2 * i]))
        copies.append(pltpu.make_async_copy(v_cache.at[layer, part], v_vmem.at[part], sems.at[2 * i + 1]))
    return copies


def add_query(piece, first, hidden, wq_buf, q_acc):
    depth = hidden.shape[-1]
    part = jnp.dot(hidden[piece], wq_buf[aligned(piece, depth), :], preferred_element_type=F32)
    q_acc[...] = part if first else q_acc[...] + part


def new_rows(place, hidden, wkv_buf, kv_new):
    pieces, rows, depth = hidden.shape
    local_rows = rows // place.count
    total = None
    for piece in range(pieces):
        mine = hidden[piece, aligned(place.me, local_rows), :]
        part = jnp.dot(mine, wkv_buf[pl.ds(piece * depth, depth), :], preferred_element_type=F32)
        total = part if total is None else total + part
    kv_new[...] = total.astype(BF16).astype(F32)


def query_copies(place, q_send, q_out, send_sems, recv_sems, incoming):
    heads = q_send.shape[0]
    local_rows = q_out.shape[1]
    copies = []
    for offset in range(1, place.count):
        source = place.origin(offset) if incoming else place.me
        target = place.peer(offset)
        copies.append(remote(
            q_send.at[:, aligned(target, local_rows), :], q_out.at[pl.ds(source * heads, heads)],
            send_sems.at[offset], recv_sems.at[offset], target))
    return copies


def send_order(count):
    return sorted(range(1, count), key=lambda offset: -min(offset, count - offset))


def exchange_query(place, q_acc, q_send, q_out, send_sems, recv_sems):
    heads, rows, head_dim = q_send.shape
    local_rows = q_out.shape[1]
    for head in range(heads):
        q_send[head] = q_acc[:, head * head_dim:(head + 1) * head_dim].astype(BF16)
    outgoing = query_copies(place, q_send, q_out, send_sems, recv_sems, False)
    for offset in send_order(place.count):
        outgoing[offset - 1].start()
    q_out[pl.ds(place.me * heads, heads)] = q_send[:, aligned(place.me, local_rows), :]
    return outgoing


def first_kernel(count, x, wq, wk, wv, k_cache, v_cache,
                 q_out, kv_new, residual, k_vmem, v_vmem,
                 hidden, wq_buf, wkv_buf, q_acc, q_send,
                 x_sems, w_sems, cache_sems, q_ssem, q_rsem):
    place = Place(count)
    pieces, rows, depth = hidden.shape
    x_copies = [
        pltpu.make_async_copy(x.at[:, pl.ds(i * depth, depth)], hidden.at[i], x_sems.at[i]) for i in range(pieces)
    ]
    w_copies = weight_copies(0, wq, wk, wv, wq_buf, wkv_buf, w_sems)
    cache_copies = cache_loads(0, k_cache, v_cache, k_vmem, v_vmem, cache_sems)
    for i in range(pieces):
        x_copies[i].start()
        w_copies[i].start()
    signal_all(place)
    w_copies[pieces].start()
    w_copies[pieces + 1].start()
    for copy in cache_copies:
        copy.start()
    for i in range(pieces):
        x_copies[i].wait()
        w_copies[i].wait()
        add_query(i, i == 0, hidden, wq_buf, q_acc)
    wait_all(place)
    outgoing = exchange_query(place, q_acc, q_send, q_out, q_ssem, q_rsem)
    chip_rows = residual.shape[1]
    for j in range(CHUNKS):
        residual[j] = hidden[place.core * CHUNKS + j, aligned(place.chip, chip_rows), :]
    w_copies[pieces].wait()
    w_copies[pieces + 1].wait()
    new_rows(place, hidden, wkv_buf, kv_new)
    for copy in query_copies(place, q_send, q_out, q_ssem, q_rsem, True):
        copy.wait_recv()
    for copy in outgoing:
        copy.wait_send()
    for copy in cache_copies:
        copy.wait()


def mix_kernel(count, last, layer, *refs):
    refs = list(refs)
    take = lambda k: [refs.pop(0) for _ in range(k)]
    context, residual, wo = take(3)
    if not last:
        wq, wk, wv, k_cache, v_cache = take(5)
        q_out, kv_new, next_residual, k_vmem, v_vmem = take(5)
    else:
        (hidden,) = take(1)
    c_recv, wo_far, wo_own, p_send, p_recv, total, s1_recv, comb, s2_left, s2_right = take(10)
    wo_sems, c_ssem, c_rsem, p_ssem, p_rsem, s1_ssem, s1_rsem = take(7)
    s2_ssem, s2_rsem, ag_ssem, ag_rsem, d2d_ssem, d2d_rsem = take(6)
    if not last:
        hidden, wq_buf, wkv_buf, q_acc, q_send, w_sems, cache_sems, q_ssem, q_rsem = take(9)
    place = Place(count)
    heads, rows, head_dim = c_recv.shape
    local_rows = rows // count
    chip_rows = rows // CHIPS
    depth = total.shape[-1]

    signal_all(place)
    wo_copies = []
    for j in range(CHUNKS):
        wo_copies.append(pltpu.make_async_copy(
            wo.at[layer, :, aligned((1 - place.core) * CHUNKS + j, depth)], wo_far.at[j], wo_sems.at[j]))
    for j in range(CHUNKS):
        wo_copies.append(pltpu.make_async_copy(
            wo.at[layer, :, aligned(place.core * CHUNKS + j, depth)], wo_own.at[j], wo_sems.at[CHUNKS + j]))
    for copy in wo_copies:
        copy.start()
    if not last:
        w_copies = weight_copies(layer + 1, wq, wk, wv, wq_buf, wkv_buf, w_sems)
        cache_copies = cache_loads(layer + 1, k_cache, v_cache, k_vmem, v_vmem, cache_sems)
        for copy in w_copies + cache_copies:
            copy.start()

    c_recv[:, aligned(place.me, local_rows), :] = context[pl.ds(place.me * heads, heads)]
    wait_all(place)

    def context_copy(offset, source):
        target = place.peer(offset)
        return remote(
            context.at[pl.ds(target * heads, heads)], c_recv.at[:, aligned(source, local_rows), :],
            c_ssem.at[offset], c_rsem.at[offset], target)

    sends = []

    def send(copy):
        copy.start()
        sends.append(copy)

    for offset in send_order(count):
        send(context_copy(offset, place.me))
    for offset in range(1, count):
        context_copy(offset, place.origin(offset)).wait_recv()

    def product(weights):
        acc = None
        for pair in range(heads // 2):
            lhs = jnp.concatenate([c_recv[2 * pair], c_recv[2 * pair + 1]], axis=1)
            part = jnp.dot(lhs, weights[pl.ds(pair * 2 * head_dim, 2 * head_dim), :], preferred_element_type=F32)
            acc = part if acc is None else acc + part
        return acc

    def pair_copy(j):
        return remote(p_send.at[j], p_recv.at[j], p_ssem.at[j], p_rsem.at[j], place.sibling)

    def block(chip):
        return aligned(chip, chip_rows)

    for j in range(CHUNKS):
        wo_copies[j].wait()
        p_send[j] = product(wo_far.at[j])
        send(pair_copy(j))

    def step_one(j):
        target = place.to_right if j % 2 == 0 else place.to_left
        if j >= RELAYED:
            target = place.across * 2 + place.core
        return remote(total.at[j, block(place.across), :], s1_recv.at[j], s1_ssem.at[j], s1_rsem.at[j], target)

    def step_two(j, rightward, source):
        target = place.to_right if rightward else place.to_left
        inbox = s2_left if rightward else s2_right
        slot = j if rightward else CHUNKS + j
        return remote(source, inbox.at[j], s2_ssem.at[slot], s2_rsem.at[slot], target)

    def direct(j):
        for rightward in (j % 2 == 1, j % 2 == 0) if j >= RELAYED else (j % 2 == 1,):
            send(step_two(j, rightward, total.at[j, block(place.right if rightward else place.left), :]))

    def combine(j):
        step_one(j).wait_recv()
        rightward = j % 2 == 0
        comb[j] = total[j, block(place.right if rightward else place.left), :] + s1_recv[j]
        send(step_two(j, rightward, comb.at[j]))

    for j in range(CHUNKS):
        wo_copies[CHUNKS + j].wait()
        total[j] = product(wo_own.at[j])
    pending = []
    for j in range(CHUNKS):
        pair_copy(j).wait_recv()
        total[j] += p_recv[j]
        send(step_one(j))
        while pending:
            direct(pending.pop())
        if 0 < j < RELAYED:
            pending.append(j)
        else:
            direct(j)
    for j in range(min(RELAYED, 2)):
        combine(j)
    while pending:
        direct(pending.pop())
    for j in range(2, RELAYED):
        combine(j)

    def piece(core, j):
        return core * CHUNKS + j

    def region(core, j, chip):
        if last:
            return hidden.at[block(chip), aligned(piece(core, j), depth)]
        return hidden.at[piece(core, j), block(chip), :]

    def gather_copy(j, way, chip):
        target = (place.to_right, place.to_left, place.across * 2 + place.core)[way]
        part = region(place.core, j, chip)
        slot = way * CHUNKS + j
        return remote(part, part, ag_ssem.at[slot], ag_rsem.at[slot], target)

    def forward_copy(j, chip):
        target = place.to_right if j % 2 == 0 else place.to_left
        part = region(place.core, j, chip)
        return remote(part, part, ag_ssem.at[2 * CHUNKS + j], ag_rsem.at[2 * CHUNKS + j], target)

    def twin_copy(j, core):
        part = hidden.at[:, aligned(piece(core, j), depth)] if last else hidden.at[piece(core, j)]
        return remote(part, part, d2d_ssem.at[j], d2d_rsem.at[j], place.sibling)

    def finish(j):
        step_two(j, True, comb.at[j]).wait_recv()
        step_two(j, False, comb.at[j]).wait_recv()
        summed = total[j, block(place.chip), :] + s2_left[j] + s2_right[j]
        if j >= RELAYED:
            step_one(j).wait_recv()
            summed = summed + s1_recv[j]
        value = (residual[j].astype(F32) + summed).astype(BF16)
        if last:
            hidden[block(place.chip), aligned(piece(place.core, j), depth)] = value
        else:
            hidden[piece(place.core, j), block(place.chip), :] = value
            next_residual[j] = value
        if j >= RING:
            send(gather_copy(j, 2, place.chip))
        send(gather_copy(j, 0, place.chip))
        send(gather_copy(j, 1, place.chip))

    def pass_on(j):
        gather_copy(j, 0, place.left).wait_recv()
        if j < RING and j % 2 == 0:
            send(forward_copy(j, place.left))
        gather_copy(j, 1, place.right).wait_recv()
        if j < RING and j % 2 == 1:
            send(forward_copy(j, place.right))

    def far_block(j):
        gather_copy(j, 2, place.across).wait_recv()
        send(twin_copy(j, place.core))

    for j in range(CHUNKS):
        finish(j)
    for j in range(RING):
        pass_on(j)
    order = list(range(RING, CHUNKS)) + list(range(RING))
    for j in order:
        if j >= RING:
            pass_on(j)
        far_block(j)
        if not last:
            for copy in w_copies if j == order[0] else ():
                copy.wait()
            add_query(piece(place.core, j), j == order[0], hidden, wq_buf, q_acc)
    for j in order:
        twin_copy(j, 1 - place.core).wait_recv()
        if not last:
            add_query(piece(1 - place.core, j), False, hidden, wq_buf, q_acc)
    if not last:
        outgoing = exchange_query(place, q_acc, q_send, q_out, q_ssem, q_rsem)
        new_rows(place, hidden, wkv_buf, kv_new)
        for copy in query_copies(place, q_send, q_out, q_ssem, q_rsem, True):
            copy.wait_recv()
        sends.extend(outgoing)
        for copy in cache_copies:
            copy.wait()
    for copy in sends:
        copy.wait_send()


GROUP = 8
SHORT = 256


def attention_kernel(layer, *refs):
    all_lens, q, kv_new, k_in, v_in = refs[:5]
    refs = refs[5:]
    if layer > 0:
        refs = refs[2:]
    k_out, v_out, k_buf, v_buf, context, q_rows, c_rows, sems = refs
    del k_in, v_in
    heads, local_rows, head_dim = q.shape
    seq_len = k_buf.shape[1]
    tile = 16
    first_row = lax.axis_index("model") * local_rows

    def length(b):
        return all_lens[first_row + b]

    writes = []
    parts = sems.shape[0] // 2
    step = local_rows // parts
    for i in range(parts):
        for b in range(i * step, (i + 1) * step):
            start = pl.multiple_of((length(b) // tile) * tile, tile)
            here = lax.broadcasted_iota(jnp.int32, (tile, head_dim), 0) == length(b) - start
            for buf, column in ((k_buf, 0), (v_buf, head_dim)):
                fresh = jnp.broadcast_to(kv_new[b:b + 1, column:column + head_dim], (tile, head_dim))
                old = buf[b, pl.ds(start, tile), :].astype(F32)
                buf[b, pl.ds(start, tile), :] = jnp.where(here, fresh, old).astype(BF16)
        part = pl.ds(i * step, step)
        writes.append(pltpu.make_async_copy(k_buf.at[part], k_out.at[layer, part], sems.at[2 * i]))
        writes.append(pltpu.make_async_copy(v_buf.at[part], v_out.at[layer, part], sems.at[2 * i + 1]))
        if i > 0:
            writes[2 * i - 2].start()
            writes[2 * i - 1].start()
    q_rows[...] = q[...].astype(F32).reshape(heads * local_rows, head_dim)
    writes[-2].start()
    writes[-1].start()

    def attend(members, span):
        rows = [pl.ds(b, heads, stride=local_rows) for b in members]
        scores = [
            lax.dot_general(
                q_rows[r, :].astype(BF16), k_buf[b, pl.ds(0, span), :], (((1,), (1,)), ((), ())),
                preferred_element_type=F32)
            for b, r in zip(members, rows)
        ]
        positions = lax.broadcasted_iota(jnp.int32, (heads, span), 1)
        scores = [jnp.where(positions <= length(b), s * (head_dim ** -0.5), -jnp.inf) for b, s in zip(members, scores)]
        tops = [jnp.max(s, axis=1, keepdims=True) for s in scores]
        powers = [jnp.exp(s - t) for s, t in zip(scores, tops)]
        sums = [jnp.sum(p, axis=1, keepdims=True) for p in powers]
        weights = [(p / t).astype(BF16) for p, t in zip(powers, sums)]
        outs = [
            jnp.dot(w, v_buf[b, pl.ds(0, span), :], preferred_element_type=F32) for b, w in zip(members, weights)
        ]
        for r, out in zip(rows, outs):
            c_rows[r, :] = out.astype(BF16).astype(F32)

    for first in range(0, local_rows, GROUP):
        attend(list(range(first, first + GROUP)), SHORT)

    spans = []
    span = 2 * SHORT
    while span < seq_len:
        spans.append(span)
        span *= 2
    spans.append(seq_len)

    def longer(b, _):
        @pl.when(length(b) >= SHORT)
        def _():
            low = SHORT
            for span in spans:
                @pl.when(jnp.logical_and(length(b) >= low, length(b) < span))
                def _(span=span):
                    attend([b], span)
                low = span
        return 0

    lax.fori_loop(0, local_rows, longer, 0)
    context[...] = c_rows[...].reshape(heads, local_rows, head_dim).astype(BF16)
    for copy in writes:
        copy.wait()


def solution(mesh):
    count = mesh.shape["model"]
    assert count == 2 * CHIPS
    row_axes = ("replica", "model")
    cache_spec = P(None, row_axes, None, None)
    DMA = pltpu.SemaphoreType.DMA

    def device_step(x, cache_len, w_query, w_key, w_value, w_out, k_cache, v_cache):
        rows, width = x.shape
        layers, local_rows, seq_len, head_dim = k_cache.shape
        local_width = w_query.shape[-1]
        local_heads = local_width // head_dim
        heads = local_heads * count
        pieces = 2 * CHUNKS
        depth = width // pieces
        chip_rows = rows // CHIPS
        w_query, w_key, w_value, w_out = map(to_hbm, (w_query, w_key, w_value, w_out))
        x, k_cache, v_cache = map(to_hbm, (x, k_cache, v_cache))

        project_out = (
            pltpu.VMEM((heads, local_rows, head_dim), BF16),
            pltpu.VMEM((local_rows, 2 * head_dim), F32),
            pltpu.VMEM((CHUNKS, chip_rows, depth), BF16),
            pltpu.VMEM(k_cache.shape[1:], BF16),
            pltpu.VMEM(v_cache.shape[1:], BF16),
        )
        project_scratch = [
            pltpu.VMEM((pieces, rows, depth), BF16),
            pltpu.VMEM((width, local_width), BF16),
            pltpu.VMEM((width, 2 * head_dim), BF16),
            pltpu.VMEM((rows, local_width), F32),
            pltpu.VMEM((local_heads, rows, head_dim), BF16),
        ]
        project_sems = [DMA((pieces + 2,)), DMA((2 * PARTS,)), DMA((count,)), DMA((count,))]
        mix_scratch = [
            pltpu.VMEM((local_heads, rows, head_dim), BF16),
            pltpu.VMEM((CHUNKS, local_width, depth), BF16),
            pltpu.VMEM((CHUNKS, local_width, depth), BF16),
            pltpu.VMEM((CHUNKS, rows, depth), F32),
            pltpu.VMEM((CHUNKS, rows, depth), F32),
            pltpu.VMEM((CHUNKS, rows, depth), F32),
            pltpu.VMEM((CHUNKS, chip_rows, depth), F32),
            pltpu.VMEM((CHUNKS, chip_rows, depth), F32),
            pltpu.VMEM((CHUNKS, chip_rows, depth), F32),
            pltpu.VMEM((CHUNKS, chip_rows, depth), F32),
            DMA((pieces,)), DMA((count,)), DMA((count,)), DMA((CHUNKS,)), DMA((CHUNKS,)), DMA((CHUNKS,)), DMA((CHUNKS,)),
            DMA((2 * CHUNKS,)), DMA((2 * CHUNKS,)), DMA((3 * CHUNKS,)), DMA((3 * CHUNKS,)),
            DMA((CHUNKS,)), DMA((CHUNKS,)),
        ]

        def params(collective_id, limit):
            return pltpu.CompilerParams(collective_id=collective_id, has_side_effects=True, vmem_limit_bytes=limit * MIB)

        query, kv_new, residual, k_vmem, v_vmem = pl.pallas_call(
            functools.partial(first_kernel, count),
            out_shape=project_out,
            in_specs=[ANY_SPEC] * 6,
            out_specs=(VMEM_SPEC,) * 5,
            scratch_shapes=project_scratch + [DMA((pieces,))] + project_sems,
            compiler_params=params(0, 16),
            name="first",
        )(x, w_query, w_key, w_value, k_cache, v_cache)

        k_new_cache = v_new_cache = None
        for layer in range(layers):
            last = layer == layers - 1
            operands = [cache_len, query, kv_new, k_vmem, v_vmem]
            specs = [SMEM_SPEC] + [VMEM_SPEC] * 4
            aliases = {3: 2, 4: 3}
            if layer > 0:
                operands += [k_new_cache, v_new_cache]
                specs += [ANY_SPEC] * 2
                aliases |= {5: 0, 6: 1}
            k_new_cache, v_new_cache, _, _, context = pl.pallas_call(
                functools.partial(attention_kernel, layer),
                out_shape=(
                    pltpu.HBM(k_cache.shape, BF16),
                    pltpu.HBM(v_cache.shape, BF16),
                    pltpu.VMEM(k_cache.shape[1:], BF16),
                    pltpu.VMEM(v_cache.shape[1:], BF16),
                    pltpu.VMEM((heads, local_rows, head_dim), BF16),
                ),
                in_specs=specs,
                out_specs=(ANY_SPEC, ANY_SPEC, VMEM_SPEC, VMEM_SPEC, VMEM_SPEC),
                input_output_aliases=aliases,
                scratch_shapes=[
                    pltpu.VMEM((heads * local_rows, head_dim), F32),
                    pltpu.VMEM((heads * local_rows, head_dim), F32),
                    DMA((2 * PARTS,)),
                ],
                compiler_params=pltpu.CompilerParams(vmem_limit_bytes=16 * MIB),
                name=f"attend{layer}",
            )(*operands)
            if not last:
                query, kv_new, residual, k_vmem, v_vmem = pl.pallas_call(
                    functools.partial(mix_kernel, count, False, layer),
                    out_shape=project_out,
                    in_specs=[VMEM_SPEC] * 2 + [ANY_SPEC] * 6,
                    out_specs=(VMEM_SPEC,) * 5,
                    scratch_shapes=mix_scratch + project_scratch + project_sems,
                    compiler_params=params(1 + layer, 28),
                    name=f"mix{layer}",
                )(context, residual, w_out, w_query, w_key, w_value, k_cache, v_cache)
            else:
                hidden = pl.pallas_call(
                    functools.partial(mix_kernel, count, True, layer),
                    out_shape=pltpu.VMEM((rows, width), BF16),
                    in_specs=[VMEM_SPEC] * 2 + [ANY_SPEC],
                    out_specs=VMEM_SPEC,
                    scratch_shapes=mix_scratch,
                    compiler_params=params(1 + layer, 20),
                    name=f"mix{layer}",
                )(context, residual, w_out)
        return hidden, k_new_cache, v_new_cache

    return jax.shard_map(
        device_step,
        mesh=mesh,
        in_specs=(P("replica", None), P("replica"), P(None, None, "model"), P(), P(), P(None, "model", None), cache_spec, cache_spec),
        out_specs=(P("replica", None), cache_spec, cache_spec),
        check_vma=False,
    )
```

```python
import functools

import jax
import jax.numpy as jnp
from jax import lax
from jax.experimental import pallas as pl
from jax.experimental.pallas import tpu as pltpu
from jax.sharding import PartitionSpec as P

MESH = pl.DeviceIdType.MESH
F32 = jnp.float32
BF16 = jnp.bfloat16
CHIPS = 4
CHUNKS = 4
PARTS = 8
RING = 2
RELAYED = 4
MIB = 1 << 20

ANY_SPEC = pl.BlockSpec(memory_space=pltpu.HBM)
VMEM_SPEC = pl.BlockSpec(memory_space=pltpu.VMEM)
SMEM_SPEC = pl.BlockSpec(memory_space=pltpu.SMEM)


def to_hbm(value):
    return pltpu.with_memory_space_constraint(value, pltpu.HBM)


def to_vmem(value):
    return pltpu.with_memory_space_constraint(value, pltpu.VMEM)


def aligned(index, size):
    return pl.ds(pl.multiple_of(index * size, size), size)


class Place:
    def __init__(self, count):
        self.count = count
        self.me = lax.axis_index("model")
        self.chip = self.me // 2
        self.core = self.me % 2
        self.right = (self.chip + 1) % CHIPS
        self.left = (self.chip + CHIPS - 1) % CHIPS
        self.across = (self.chip + 2) % CHIPS
        self.half = (self.core + self.chip) % 2
        self.to_right = self.right * 2 + 1 - self.core
        self.to_left = self.left * 2 + 1 - self.core
        self.sibling = self.chip * 2 + (1 - self.core)

    def peer(self, offset):
        return (self.me + offset) % self.count

    def origin(self, offset):
        return (self.me + self.count - offset) % self.count


def remote(src, dst, send_sem, recv_sem, device):
    return pltpu.make_async_remote_copy(
        src_ref=src, dst_ref=dst, send_sem=send_sem, recv_sem=recv_sem,
        device_id={"model": device}, device_id_type=MESH)


def signal_all(place):
    barrier = pltpu.get_barrier_semaphore()
    for offset in send_order(place.count):
        pl.semaphore_signal(barrier, inc=1, device_id={"model": place.peer(offset)}, device_id_type=MESH)


def wait_all(place):
    pl.semaphore_wait(pltpu.get_barrier_semaphore(), place.count - 1)


def weight_copies(layer, wq, wk, wv, wq_buf, wkv_buf, sems):
    pieces = sems.shape[0] - 2
    depth = wq_buf.shape[0] // pieces
    head_dim = wk.shape[-1]
    copies = [
        pltpu.make_async_copy(wq.at[layer, pl.ds(i * depth, depth), :], wq_buf.at[pl.ds(i * depth, depth), :], sems.at[i])
        for i in range(pieces)
    ]
    copies.append(pltpu.make_async_copy(wk.at[layer], wkv_buf.at[:, pl.ds(0, head_dim)], sems.at[pieces]))
    copies.append(pltpu.make_async_copy(wv.at[layer], wkv_buf.at[:, pl.ds(head_dim, head_dim)], sems.at[pieces + 1]))
    return copies


def cache_loads(layer, k_cache, v_cache, k_vmem, v_vmem, sems):
    parts = sems.shape[0] // 2
    step = k_vmem.shape[0] // parts
    copies = []
    for i in range(parts):
        part = pl.ds(i * step, step)
        copies.append(pltpu.make_async_copy(k_cache.at[layer, part], k_vmem.at[part], sems.at[2 * i]))
        copies.append(pltpu.make_async_copy(v_cache.at[layer, part], v_vmem.at[part], sems.at[2 * i + 1]))
    return copies


def add_query(piece, first, hidden, wq_buf, q_acc):
    depth = hidden.shape[-1]
    part = jnp.dot(hidden[piece], wq_buf[aligned(piece, depth), :], preferred_element_type=F32)
    q_acc[...] = part if first else q_acc[...] + part


def new_rows(place, hidden, wkv_buf, kv_new):
    pieces, rows, depth = hidden.shape
    local_rows = rows // place.count
    total = None
    for piece in range(pieces):
        mine = hidden[piece, aligned(place.me, local_rows), :]
        part = jnp.dot(mine, wkv_buf[pl.ds(piece * depth, depth), :], preferred_element_type=F32)
        total = part if total is None else total + part
    kv_new[...] = total.astype(BF16).astype(F32)


def query_copies(place, q_send, q_out, send_sems, recv_sems, incoming):
    heads = q_send.shape[0]
    local_rows = q_out.shape[1]
    copies = []
    for offset in range(1, place.count):
        source = place.origin(offset) if incoming else place.me
        target = place.peer(offset)
        copies.append(remote(
            q_send.at[:, aligned(target, local_rows), :], q_out.at[pl.ds(source * heads, heads)],
            send_sems.at[offset], recv_sems.at[offset], target))
    return copies


def send_order(count):
    return sorted(range(1, count), key=lambda offset: -min(offset, count - offset))


def exchange_query(place, q_acc, q_send, q_out, send_sems, recv_sems):
    heads, rows, head_dim = q_send.shape
    local_rows = q_out.shape[1]
    for head in range(heads):
        q_send[head] = q_acc[:, head * head_dim:(head + 1) * head_dim].astype(BF16)
    outgoing = query_copies(place, q_send, q_out, send_sems, recv_sems, False)
    for offset in send_order(place.count):
        outgoing[offset - 1].start()
    q_out[pl.ds(place.me * heads, heads)] = q_send[:, aligned(place.me, local_rows), :]
    return outgoing


def first_kernel(count, x, wq, wk, wv, k_cache, v_cache,
                 q_out, kv_new, residual, k_vmem, v_vmem,
                 hidden, wq_buf, wkv_buf, q_acc, q_send,
                 x_sems, w_sems, cache_sems, q_ssem, q_rsem):
    place = Place(count)
    pieces, rows, depth = hidden.shape
    x_copies = [
        pltpu.make_async_copy(x.at[:, pl.ds(i * depth, depth)], hidden.at[i], x_sems.at[i]) for i in range(pieces)
    ]
    w_copies = weight_copies(0, wq, wk, wv, wq_buf, wkv_buf, w_sems)
    cache_copies = cache_loads(0, k_cache, v_cache, k_vmem, v_vmem, cache_sems)
    for i in range(pieces):
        x_copies[i].start()
        w_copies[i].start()
    signal_all(place)
    w_copies[pieces].start()
    w_copies[pieces + 1].start()
    for copy in cache_copies:
        copy.start()
    for i in range(pieces):
        x_copies[i].wait()
        w_copies[i].wait()
        add_query(i, i == 0, hidden, wq_buf, q_acc)
    wait_all(place)
    outgoing = exchange_query(place, q_acc, q_send, q_out, q_ssem, q_rsem)
    chip_rows = residual.shape[1]
    for j in range(CHUNKS):
        residual[j] = hidden[place.half * CHUNKS + j, aligned(place.chip, chip_rows), :]
    w_copies[pieces].wait()
    w_copies[pieces + 1].wait()
    new_rows(place, hidden, wkv_buf, kv_new)
    for copy in query_copies(place, q_send, q_out, q_ssem, q_rsem, True):
        copy.wait_recv()
    for copy in outgoing:
        copy.wait_send()
    for copy in cache_copies:
        copy.wait()


def mix_kernel(count, last, layer, *refs):
    refs = list(refs)
    take = lambda k: [refs.pop(0) for _ in range(k)]
    context, residual, wo = take(3)
    if not last:
        wq, wk, wv, k_cache, v_cache = take(5)
        q_out, kv_new, next_residual, k_vmem, v_vmem = take(5)
    else:
        (hidden,) = take(1)
    c_recv, wo_far, wo_own, p_send, p_recv, total, s1_recv, comb, s2_left, s2_right = take(10)
    wo_sems, c_ssem, c_rsem, p_ssem, p_rsem, s1_ssem, s1_rsem = take(7)
    s2_ssem, s2_rsem, ag_ssem, ag_rsem, d2d_ssem, d2d_rsem = take(6)
    if not last:
        hidden, wq_buf, wkv_buf, q_acc, q_send, w_sems, cache_sems, q_ssem, q_rsem = take(9)
    place = Place(count)
    heads, rows, head_dim = c_recv.shape
    local_rows = rows // count
    chip_rows = rows // CHIPS
    depth = total.shape[-1]

    signal_all(place)
    wo_copies = []
    for j in range(CHUNKS):
        wo_copies.append(pltpu.make_async_copy(
            wo.at[layer, :, aligned((1 - place.half) * CHUNKS + j, depth)], wo_far.at[j], wo_sems.at[j]))
    for j in range(CHUNKS):
        wo_copies.append(pltpu.make_async_copy(
            wo.at[layer, :, aligned(place.half * CHUNKS + j, depth)], wo_own.at[j], wo_sems.at[CHUNKS + j]))
    for copy in wo_copies:
        copy.start()
    if not last:
        w_copies = weight_copies(layer + 1, wq, wk, wv, wq_buf, wkv_buf, w_sems)
        cache_copies = cache_loads(layer + 1, k_cache, v_cache, k_vmem, v_vmem, cache_sems)
        for copy in w_copies + cache_copies:
            copy.start()

    c_recv[:, aligned(place.me, local_rows), :] = context[pl.ds(place.me * heads, heads)]
    wait_all(place)

    def context_copy(offset, source):
        target = place.peer(offset)
        return remote(
            context.at[pl.ds(target * heads, heads)], c_recv.at[:, aligned(source, local_rows), :],
            c_ssem.at[offset], c_rsem.at[offset], target)

    sends = []

    def send(copy):
        copy.start()
        sends.append(copy)

    for offset in send_order(count):
        send(context_copy(offset, place.me))
    for offset in range(1, count):
        context_copy(offset, place.origin(offset)).wait_recv()

    def product(weights):
        acc = None
        for pair in range(heads // 2):
            lhs = jnp.concatenate([c_recv[2 * pair], c_recv[2 * pair + 1]], axis=1)
            part = jnp.dot(lhs, weights[pl.ds(pair * 2 * head_dim, 2 * head_dim), :], preferred_element_type=F32)
            acc = part if acc is None else acc + part
        return acc

    def pair_copy(j):
        return remote(p_send.at[j], p_recv.at[j], p_ssem.at[j], p_rsem.at[j], place.sibling)

    def block(chip):
        return aligned(chip, chip_rows)

    for j in range(CHUNKS):
        wo_copies[j].wait()
        p_send[j] = product(wo_far.at[j])
        send(pair_copy(j))

    def step_one(j):
        target = place.to_right if j % 2 == 0 else place.to_left
        if j >= RELAYED:
            target = place.across * 2 + place.core
        return remote(total.at[j, block(place.across), :], s1_recv.at[j], s1_ssem.at[j], s1_rsem.at[j], target)

    def step_two(j, rightward, source):
        target = place.to_right if rightward else place.to_left
        inbox = s2_left if rightward else s2_right
        slot = j if rightward else CHUNKS + j
        return remote(source, inbox.at[j], s2_ssem.at[slot], s2_rsem.at[slot], target)

    def direct(j):
        for rightward in (j % 2 == 1, j % 2 == 0) if j >= RELAYED else (j % 2 == 1,):
            send(step_two(j, rightward, total.at[j, block(place.right if rightward else place.left), :]))

    def combine(j):
        step_one(j).wait_recv()
        rightward = j % 2 == 0
        comb[j] = total[j, block(place.right if rightward else place.left), :] + s1_recv[j]
        send(step_two(j, rightward, comb.at[j]))

    for j in range(CHUNKS):
        wo_copies[CHUNKS + j].wait()
        total[j] = product(wo_own.at[j])
    pending = []
    for j in range(CHUNKS):
        pair_copy(j).wait_recv()
        total[j] += p_recv[j]
        send(step_one(j))
        while pending:
            direct(pending.pop())
        if 0 < j < RELAYED:
            pending.append(j)
        else:
            direct(j)
    for j in range(min(RELAYED, 2)):
        combine(j)
    while pending:
        direct(pending.pop())
    for j in range(2, RELAYED):
        combine(j)

    def piece(half, j):
        return half * CHUNKS + j

    def region(half, j, chip):
        if last:
            return hidden.at[block(chip), aligned(piece(half, j), depth)]
        return hidden.at[piece(half, j), block(chip), :]

    def gather_copy(j, way, chip):
        target = (place.to_right, place.to_left, place.across * 2 + place.core)[way]
        part = region(place.half, j, chip)
        slot = way * CHUNKS + j
        return remote(part, part, ag_ssem.at[slot], ag_rsem.at[slot], target)

    def forward_copy(j, chip):
        target = place.to_right if j % 2 == 0 else place.to_left
        part = region(place.half, j, chip)
        return remote(part, part, ag_ssem.at[2 * CHUNKS + j], ag_rsem.at[2 * CHUNKS + j], target)

    def twin_copy(j, half):
        part = hidden.at[:, aligned(piece(half, j), depth)] if last else hidden.at[piece(half, j)]
        return remote(part, part, d2d_ssem.at[j], d2d_rsem.at[j], place.sibling)

    def finish(j):
        step_two(j, True, comb.at[j]).wait_recv()
        step_two(j, False, comb.at[j]).wait_recv()
        summed = total[j, block(place.chip), :] + s2_left[j] + s2_right[j]
        if j >= RELAYED:
            step_one(j).wait_recv()
            summed = summed + s1_recv[j]
        value = (residual[j].astype(F32) + summed).astype(BF16)
        if last:
            hidden[block(place.chip), aligned(piece(place.half, j), depth)] = value
        else:
            hidden[piece(place.half, j), block(place.chip), :] = value
            next_residual[j] = value
        if j >= RING:
            send(gather_copy(j, 2, place.chip))
        send(gather_copy(j, 0, place.chip))
        send(gather_copy(j, 1, place.chip))

    def pass_on(j):
        gather_copy(j, 0, place.left).wait_recv()
        if j < RING and j % 2 == 0:
            send(forward_copy(j, place.left))
        gather_copy(j, 1, place.right).wait_recv()
        if j < RING and j % 2 == 1:
            send(forward_copy(j, place.right))

    def far_block(j):
        gather_copy(j, 2, place.across).wait_recv()
        send(twin_copy(j, place.half))

    for j in range(CHUNKS):
        finish(j)
    for j in range(RING):
        pass_on(j)
    order = list(range(RING, CHUNKS)) + list(range(RING))
    for j in order:
        if j >= RING:
            pass_on(j)
        far_block(j)
        if not last:
            for copy in w_copies if j == order[0] else ():
                copy.wait()
            add_query(piece(place.half, j), j == order[0], hidden, wq_buf, q_acc)
    for j in order:
        twin_copy(j, 1 - place.half).wait_recv()
        if not last:
            add_query(piece(1 - place.half, j), False, hidden, wq_buf, q_acc)
    if not last:
        outgoing = exchange_query(place, q_acc, q_send, q_out, q_ssem, q_rsem)
        new_rows(place, hidden, wkv_buf, kv_new)
        for copy in query_copies(place, q_send, q_out, q_ssem, q_rsem, True):
            copy.wait_recv()
        sends.extend(outgoing)
        for copy in cache_copies:
            copy.wait()
    for copy in sends:
        copy.wait_send()


GROUP = 8
SHORT = 256


def attention_kernel(layer, *refs):
    all_lens, q, kv_new, k_in, v_in = refs[:5]
    refs = refs[5:]
    if layer > 0:
        refs = refs[2:]
    k_out, v_out, k_buf, v_buf, context, q_rows, c_rows, sems = refs
    del k_in, v_in
    heads, local_rows, head_dim = q.shape
    seq_len = k_buf.shape[1]
    tile = 16
    first_row = lax.axis_index("model") * local_rows

    def length(b):
        return all_lens[first_row + b]

    writes = []
    parts = sems.shape[0] // 2
    step = local_rows // parts
    for i in range(parts):
        for b in range(i * step, (i + 1) * step):
            start = pl.multiple_of((length(b) // tile) * tile, tile)
            here = lax.broadcasted_iota(jnp.int32, (tile, head_dim), 0) == length(b) - start
            for buf, column in ((k_buf, 0), (v_buf, head_dim)):
                fresh = jnp.broadcast_to(kv_new[b:b + 1, column:column + head_dim], (tile, head_dim))
                old = buf[b, pl.ds(start, tile), :].astype(F32)
                buf[b, pl.ds(start, tile), :] = jnp.where(here, fresh, old).astype(BF16)
        part = pl.ds(i * step, step)
        writes.append(pltpu.make_async_copy(k_buf.at[part], k_out.at[layer, part], sems.at[2 * i]))
        writes.append(pltpu.make_async_copy(v_buf.at[part], v_out.at[layer, part], sems.at[2 * i + 1]))
        if i > 0:
            writes[2 * i - 2].start()
            writes[2 * i - 1].start()
    q_rows[...] = q[...].astype(F32).reshape(heads * local_rows, head_dim)
    writes[-2].start()
    writes[-1].start()

    def attend(members, span):
        rows = [pl.ds(b, heads, stride=local_rows) for b in members]
        scores = [
            lax.dot_general(
                q_rows[r, :].astype(BF16), k_buf[b, pl.ds(0, span), :], (((1,), (1,)), ((), ())),
                preferred_element_type=F32)
            for b, r in zip(members, rows)
        ]
        positions = lax.broadcasted_iota(jnp.int32, (heads, span), 1)
        scores = [jnp.where(positions <= length(b), s * (head_dim ** -0.5), -jnp.inf) for b, s in zip(members, scores)]
        tops = [jnp.max(s, axis=1, keepdims=True) for s in scores]
        powers = [jnp.exp(s - t) for s, t in zip(scores, tops)]
        sums = [jnp.sum(p, axis=1, keepdims=True) for p in powers]
        weights = [(p / t).astype(BF16) for p, t in zip(powers, sums)]
        outs = [
            jnp.dot(w, v_buf[b, pl.ds(0, span), :], preferred_element_type=F32) for b, w in zip(members, weights)
        ]
        for r, out in zip(rows, outs):
            c_rows[r, :] = out.astype(BF16).astype(F32)

    for first in range(0, local_rows, GROUP):
        attend(list(range(first, first + GROUP)), SHORT)

    spans = []
    span = 2 * SHORT
    while span < seq_len:
        spans.append(span)
        span *= 2
    spans.append(seq_len)

    def longer(b, _):
        @pl.when(length(b) >= SHORT)
        def _():
            low = SHORT
            for span in spans:
                @pl.when(jnp.logical_and(length(b) >= low, length(b) < span))
                def _(span=span):
                    attend([b], span)
                low = span
        return 0

    lax.fori_loop(0, local_rows, longer, 0)
    context[...] = c_rows[...].reshape(heads, local_rows, head_dim).astype(BF16)
    for copy in writes:
        copy.wait()


def solution(mesh):
    count = mesh.shape["model"]
    assert count == 2 * CHIPS
    row_axes = ("replica", "model")
    cache_spec = P(None, row_axes, None, None)
    DMA = pltpu.SemaphoreType.DMA

    def device_step(x, cache_len, w_query, w_key, w_value, w_out, k_cache, v_cache):
        rows, width = x.shape
        layers, local_rows, seq_len, head_dim = k_cache.shape
        local_width = w_query.shape[-1]
        local_heads = local_width // head_dim
        heads = local_heads * count
        pieces = 2 * CHUNKS
        depth = width // pieces
        chip_rows = rows // CHIPS
        w_query, w_key, w_value, w_out = map(to_hbm, (w_query, w_key, w_value, w_out))
        x, k_cache, v_cache = map(to_hbm, (x, k_cache, v_cache))

        project_out = (
            pltpu.VMEM((heads, local_rows, head_dim), BF16),
            pltpu.VMEM((local_rows, 2 * head_dim), F32),
            pltpu.VMEM((CHUNKS, chip_rows, depth), BF16),
            pltpu.VMEM(k_cache.shape[1:], BF16),
            pltpu.VMEM(v_cache.shape[1:], BF16),
        )
        project_scratch = [
            pltpu.VMEM((pieces, rows, depth), BF16),
            pltpu.VMEM((width, local_width), BF16),
            pltpu.VMEM((width, 2 * head_dim), BF16),
            pltpu.VMEM((rows, local_width), F32),
            pltpu.VMEM((local_heads, rows, head_dim), BF16),
        ]
        project_sems = [DMA((pieces + 2,)), DMA((2 * PARTS,)), DMA((count,)), DMA((count,))]
        mix_scratch = [
            pltpu.VMEM((local_heads, rows, head_dim), BF16),
            pltpu.VMEM((CHUNKS, local_width, depth), BF16),
            pltpu.VMEM((CHUNKS, local_width, depth), BF16),
            pltpu.VMEM((CHUNKS, rows, depth), F32),
            pltpu.VMEM((CHUNKS, rows, depth), F32),
            pltpu.VMEM((CHUNKS, rows, depth), F32),
            pltpu.VMEM((CHUNKS, chip_rows, depth), F32),
            pltpu.VMEM((CHUNKS, chip_rows, depth), F32),
            pltpu.VMEM((CHUNKS, chip_rows, depth), F32),
            pltpu.VMEM((CHUNKS, chip_rows, depth), F32),
            DMA((pieces,)), DMA((count,)), DMA((count,)), DMA((CHUNKS,)), DMA((CHUNKS,)), DMA((CHUNKS,)), DMA((CHUNKS,)),
            DMA((2 * CHUNKS,)), DMA((2 * CHUNKS,)), DMA((3 * CHUNKS,)), DMA((3 * CHUNKS,)),
            DMA((CHUNKS,)), DMA((CHUNKS,)),
        ]

        def params(collective_id, limit):
            return pltpu.CompilerParams(collective_id=collective_id, has_side_effects=True, vmem_limit_bytes=limit * MIB)

        query, kv_new, residual, k_vmem, v_vmem = pl.pallas_call(
            functools.partial(first_kernel, count),
            out_shape=project_out,
            in_specs=[ANY_SPEC] * 6,
            out_specs=(VMEM_SPEC,) * 5,
            scratch_shapes=project_scratch + [DMA((pieces,))] + project_sems,
            compiler_params=params(0, 16),
            name="first",
        )(x, w_query, w_key, w_value, k_cache, v_cache)

        k_new_cache = v_new_cache = None
        for layer in range(layers):
            last = layer == layers - 1
            operands = [cache_len, query, kv_new, k_vmem, v_vmem]
            specs = [SMEM_SPEC] + [VMEM_SPEC] * 4
            aliases = {3: 2, 4: 3}
            if layer > 0:
                operands += [k_new_cache, v_new_cache]
                specs += [ANY_SPEC] * 2
                aliases |= {5: 0, 6: 1}
            k_new_cache, v_new_cache, _, _, context = pl.pallas_call(
                functools.partial(attention_kernel, layer),
                out_shape=(
                    pltpu.HBM(k_cache.shape, BF16),
                    pltpu.HBM(v_cache.shape, BF16),
                    pltpu.VMEM(k_cache.shape[1:], BF16),
                    pltpu.VMEM(v_cache.shape[1:], BF16),
                    pltpu.VMEM((heads, local_rows, head_dim), BF16),
                ),
                in_specs=specs,
                out_specs=(ANY_SPEC, ANY_SPEC, VMEM_SPEC, VMEM_SPEC, VMEM_SPEC),
                input_output_aliases=aliases,
                scratch_shapes=[
                    pltpu.VMEM((heads * local_rows, head_dim), F32),
                    pltpu.VMEM((heads * local_rows, head_dim), F32),
                    DMA((2 * PARTS,)),
                ],
                compiler_params=pltpu.CompilerParams(vmem_limit_bytes=16 * MIB),
                name=f"attend{layer}",
            )(*operands)
            if not last:
                query, kv_new, residual, k_vmem, v_vmem = pl.pallas_call(
                    functools.partial(mix_kernel, count, False, layer),
                    out_shape=project_out,
                    in_specs=[VMEM_SPEC] * 2 + [ANY_SPEC] * 6,
                    out_specs=(VMEM_SPEC,) * 5,
                    scratch_shapes=mix_scratch + project_scratch + project_sems,
                    compiler_params=params(1 + layer, 28),
                    name=f"mix{layer}",
                )(context, residual, w_out, w_query, w_key, w_value, k_cache, v_cache)
            else:
                hidden = pl.pallas_call(
                    functools.partial(mix_kernel, count, True, layer),
                    out_shape=pltpu.VMEM((rows, width), BF16),
                    in_specs=[VMEM_SPEC] * 2 + [ANY_SPEC],
                    out_specs=VMEM_SPEC,
                    scratch_shapes=mix_scratch,
                    compiler_params=params(1 + layer, 20),
                    name=f"mix{layer}",
                )(context, residual, w_out)
        return hidden, k_new_cache, v_new_cache

    return jax.shard_map(
        device_step,
        mesh=mesh,
        in_specs=(P("replica", None), P("replica"), P(None, None, "model"), P(), P(), P(None, "model", None), cache_spec, cache_spec),
        out_specs=(P("replica", None), cache_spec, cache_spec),
        check_vma=False,
    )
```

```python
import functools

import jax
import jax.numpy as jnp
from jax import lax
from jax.experimental import pallas as pl
from jax.experimental.pallas import tpu as pltpu
from jax.sharding import PartitionSpec as P

MESH = pl.DeviceIdType.MESH
F32 = jnp.float32
BF16 = jnp.bfloat16
CHIPS = 4
CHUNKS = 4
PARTS = 8
RING = 2
RELAYED = 4
MIB = 1 << 20

ANY_SPEC = pl.BlockSpec(memory_space=pltpu.HBM)
VMEM_SPEC = pl.BlockSpec(memory_space=pltpu.VMEM)
SMEM_SPEC = pl.BlockSpec(memory_space=pltpu.SMEM)


def to_hbm(value):
    return pltpu.with_memory_space_constraint(value, pltpu.HBM)


def to_vmem(value):
    return pltpu.with_memory_space_constraint(value, pltpu.VMEM)


def aligned(index, size):
    return pl.ds(pl.multiple_of(index * size, size), size)


class Place:
    def __init__(self, count):
        self.count = count
        self.me = lax.axis_index("model")
        self.chip = self.me // 2
        self.core = self.me % 2
        self.right = (self.chip + 1) % CHIPS
        self.left = (self.chip + CHIPS - 1) % CHIPS
        self.across = (self.chip + 2) % CHIPS
        self.half = (self.core + self.chip) % 2
        self.to_right = self.right * 2 + 1 - self.core
        self.to_left = self.left * 2 + 1 - self.core
        self.sibling = self.chip * 2 + (1 - self.core)

    def peer(self, offset):
        return (self.me + offset) % self.count

    def origin(self, offset):
        return (self.me + self.count - offset) % self.count


def remote(src, dst, send_sem, recv_sem, device):
    return pltpu.make_async_remote_copy(
        src_ref=src, dst_ref=dst, send_sem=send_sem, recv_sem=recv_sem,
        device_id={"model": device}, device_id_type=MESH)


def signal_all(place):
    barrier = pltpu.get_barrier_semaphore()
    for offset in send_order(place.count):
        pl.semaphore_signal(barrier, inc=1, device_id={"model": place.peer(offset)}, device_id_type=MESH)


def wait_all(place):
    pl.semaphore_wait(pltpu.get_barrier_semaphore(), place.count - 1)


def weight_copies(layer, wq, wk, wv, wq_buf, wkv_buf, sems):
    pieces = sems.shape[0] - 2
    depth = wq_buf.shape[0] // pieces
    head_dim = wk.shape[-1]
    copies = [
        pltpu.make_async_copy(wq.at[layer, pl.ds(i * depth, depth), :], wq_buf.at[pl.ds(i * depth, depth), :], sems.at[i])
        for i in range(pieces)
    ]
    copies.append(pltpu.make_async_copy(wk.at[layer], wkv_buf.at[:, pl.ds(0, head_dim)], sems.at[pieces]))
    copies.append(pltpu.make_async_copy(wv.at[layer], wkv_buf.at[:, pl.ds(head_dim, head_dim)], sems.at[pieces + 1]))
    return copies


def cut_of(seq_len):
    return seq_len // 4 * 3


def cache_loads(layer, k_cache, v_cache, k_vmem, v_vmem, sems, span):
    parts = sems.shape[0] // 2
    step = k_vmem.shape[0] // parts
    copies = []
    for i in range(parts):
        part = pl.ds(i * step, step)
        for n, (cache, buf) in enumerate(((k_cache, k_vmem), (v_cache, v_vmem))):
            copies.append(pltpu.make_async_copy(
                cache.at[layer, part, pl.ds(0, span)], buf.at[part, pl.ds(0, span)], sems.at[2 * i + n]))
    return copies


def add_query(piece, first, hidden, wq_buf, q_acc):
    depth = hidden.shape[-1]
    part = jnp.dot(hidden[piece], wq_buf[aligned(piece, depth), :], preferred_element_type=F32)
    q_acc[...] = part if first else q_acc[...] + part


def new_rows(place, hidden, wkv_buf, kv_new):
    pieces, rows, depth = hidden.shape
    local_rows = rows // place.count
    total = None
    for piece in range(pieces):
        mine = hidden[piece, aligned(place.me, local_rows), :]
        part = jnp.dot(mine, wkv_buf[pl.ds(piece * depth, depth), :], preferred_element_type=F32)
        total = part if total is None else total + part
    kv_new[...] = total.astype(BF16).astype(F32)


def query_copies(place, q_send, q_out, send_sems, recv_sems, incoming):
    heads = q_send.shape[0]
    local_rows = q_out.shape[1]
    copies = []
    for offset in range(1, place.count):
        source = place.origin(offset) if incoming else place.me
        target = place.peer(offset)
        copies.append(remote(
            q_send.at[:, aligned(target, local_rows), :], q_out.at[pl.ds(source * heads, heads)],
            send_sems.at[offset], recv_sems.at[offset], target))
    return copies


def send_order(count):
    return sorted(range(1, count), key=lambda offset: -min(offset, count - offset))


def exchange_query(place, q_acc, q_send, q_out, send_sems, recv_sems):
    heads, rows, head_dim = q_send.shape
    local_rows = q_out.shape[1]
    for head in range(heads):
        q_send[head] = q_acc[:, head * head_dim:(head + 1) * head_dim].astype(BF16)
    outgoing = query_copies(place, q_send, q_out, send_sems, recv_sems, False)
    for offset in send_order(place.count):
        outgoing[offset - 1].start()
    q_out[pl.ds(place.me * heads, heads)] = q_send[:, aligned(place.me, local_rows), :]
    return outgoing


def first_kernel(count, x, wq, wk, wv, k_cache, v_cache,
                 q_out, kv_new, residual, k_vmem, v_vmem,
                 hidden, wq_buf, wkv_buf, q_acc, q_send,
                 x_sems, w_sems, cache_sems, q_ssem, q_rsem):
    place = Place(count)
    pieces, rows, depth = hidden.shape
    x_copies = [
        pltpu.make_async_copy(x.at[:, pl.ds(i * depth, depth)], hidden.at[i], x_sems.at[i]) for i in range(pieces)
    ]
    w_copies = weight_copies(0, wq, wk, wv, wq_buf, wkv_buf, w_sems)
    cache_copies = cache_loads(0, k_cache, v_cache, k_vmem, v_vmem, cache_sems, cut_of(k_vmem.shape[1]))
    for i in range(pieces):
        x_copies[i].start()
        w_copies[i].start()
    signal_all(place)
    w_copies[pieces].start()
    w_copies[pieces + 1].start()
    for copy in cache_copies:
        copy.start()
    for i in range(pieces):
        x_copies[i].wait()
        w_copies[i].wait()
        add_query(i, i == 0, hidden, wq_buf, q_acc)
    wait_all(place)
    outgoing = exchange_query(place, q_acc, q_send, q_out, q_ssem, q_rsem)
    chip_rows = residual.shape[1]
    for j in range(CHUNKS):
        residual[j] = hidden[place.half * CHUNKS + j, aligned(place.chip, chip_rows), :]
    w_copies[pieces].wait()
    w_copies[pieces + 1].wait()
    new_rows(place, hidden, wkv_buf, kv_new)
    for copy in query_copies(place, q_send, q_out, q_ssem, q_rsem, True):
        copy.wait_recv()
    for copy in outgoing:
        copy.wait_send()
    for copy in cache_copies:
        copy.wait()


def mix_kernel(count, last, layer, *refs):
    refs = list(refs)
    take = lambda k: [refs.pop(0) for _ in range(k)]
    context, residual, wo = take(3)
    if not last:
        wq, wk, wv, k_cache, v_cache = take(5)
        q_out, kv_new, next_residual, k_vmem, v_vmem, k_rest, v_rest = take(7)
    else:
        (hidden,) = take(1)
    c_recv, wo_far, wo_own, p_send, p_recv, total, s1_recv, comb, s2_left, s2_right = take(10)
    wo_sems, c_ssem, c_rsem, p_ssem, p_rsem, s1_ssem, s1_rsem = take(7)
    s2_ssem, s2_rsem, ag_ssem, ag_rsem, d2d_ssem, d2d_rsem = take(6)
    if not last:
        hidden, wq_buf, wkv_buf, q_acc, q_send, w_sems, cache_sems, q_ssem, q_rsem, rest_sems = take(10)
    place = Place(count)
    heads, rows, head_dim = c_recv.shape
    local_rows = rows // count
    chip_rows = rows // CHIPS
    depth = total.shape[-1]

    signal_all(place)
    wo_copies = []
    for j in range(CHUNKS):
        wo_copies.append(pltpu.make_async_copy(
            wo.at[layer, :, aligned((1 - place.half) * CHUNKS + j, depth)], wo_far.at[j], wo_sems.at[j]))
    for j in range(CHUNKS):
        wo_copies.append(pltpu.make_async_copy(
            wo.at[layer, :, aligned(place.half * CHUNKS + j, depth)], wo_own.at[j], wo_sems.at[CHUNKS + j]))
    for copy in wo_copies:
        copy.start()
    if not last:
        w_copies = weight_copies(layer + 1, wq, wk, wv, wq_buf, wkv_buf, w_sems)
        cache_copies = cache_loads(layer + 1, k_cache, v_cache, k_vmem, v_vmem, cache_sems, k_vmem.shape[1])
        cut, rest = cut_of(k_vmem.shape[1]), k_rest.shape[1]
        for n, (cache, buf) in enumerate(((k_cache, k_rest), (v_cache, v_rest))):
            cache_copies.append(pltpu.make_async_copy(cache.at[layer, :, pl.ds(cut, rest)], buf, rest_sems.at[n]))
        for copy in w_copies + cache_copies:
            copy.start()

    c_recv[:, aligned(place.me, local_rows), :] = context[pl.ds(place.me * heads, heads)]
    wait_all(place)

    def context_copy(offset, source):
        target = place.peer(offset)
        return remote(
            context.at[pl.ds(target * heads, heads)], c_recv.at[:, aligned(source, local_rows), :],
            c_ssem.at[offset], c_rsem.at[offset], target)

    sends = []

    def send(copy):
        copy.start()
        sends.append(copy)

    for offset in send_order(count):
        send(context_copy(offset, place.me))
    for offset in range(1, count):
        context_copy(offset, place.origin(offset)).wait_recv()

    def product(weights):
        acc = None
        for pair in range(heads // 2):
            lhs = jnp.concatenate([c_recv[2 * pair], c_recv[2 * pair + 1]], axis=1)
            part = jnp.dot(lhs, weights[pl.ds(pair * 2 * head_dim, 2 * head_dim), :], preferred_element_type=F32)
            acc = part if acc is None else acc + part
        return acc

    def pair_copy(j):
        return remote(p_send.at[j], p_recv.at[j], p_ssem.at[j], p_rsem.at[j], place.sibling)

    def block(chip):
        return aligned(chip, chip_rows)

    for j in range(CHUNKS):
        wo_copies[j].wait()
        p_send[j] = product(wo_far.at[j])
        send(pair_copy(j))

    def step_one(j):
        target = place.to_right if j % 2 == 0 else place.to_left
        if j >= RELAYED:
            target = place.across * 2 + place.core
        return remote(total.at[j, block(place.across), :], s1_recv.at[j], s1_ssem.at[j], s1_rsem.at[j], target)

    def step_two(j, rightward, source):
        target = place.to_right if rightward else place.to_left
        inbox = s2_left if rightward else s2_right
        slot = j if rightward else CHUNKS + j
        return remote(source, inbox.at[j], s2_ssem.at[slot], s2_rsem.at[slot], target)

    def direct(j):
        for rightward in (j % 2 == 1, j % 2 == 0) if j >= RELAYED else (j % 2 == 1,):
            send(step_two(j, rightward, total.at[j, block(place.right if rightward else place.left), :]))

    def combine(j):
        step_one(j).wait_recv()
        rightward = j % 2 == 0
        comb[j] = total[j, block(place.right if rightward else place.left), :] + s1_recv[j]
        send(step_two(j, rightward, comb.at[j]))

    for j in range(CHUNKS):
        wo_copies[CHUNKS + j].wait()
        total[j] = product(wo_own.at[j])
    pending = []
    for j in range(CHUNKS):
        pair_copy(j).wait_recv()
        total[j] += p_recv[j]
        send(step_one(j))
        while pending:
            direct(pending.pop())
        if 0 < j < RELAYED:
            pending.append(j)
        else:
            direct(j)
    for j in range(min(RELAYED, 2)):
        combine(j)
    while pending:
        direct(pending.pop())
    for j in range(2, RELAYED):
        combine(j)

    def piece(half, j):
        return half * CHUNKS + j

    def region(half, j, chip):
        if last:
            return hidden.at[block(chip), aligned(piece(half, j), depth)]
        return hidden.at[piece(half, j), block(chip), :]

    def gather_copy(j, way, chip):
        target = (place.to_right, place.to_left, place.across * 2 + place.core)[way]
        part = region(place.half, j, chip)
        slot = way * CHUNKS + j
        return remote(part, part, ag_ssem.at[slot], ag_rsem.at[slot], target)

    def forward_copy(j, chip):
        target = place.to_right if j % 2 == 0 else place.to_left
        part = region(place.half, j, chip)
        return remote(part, part, ag_ssem.at[2 * CHUNKS + j], ag_rsem.at[2 * CHUNKS + j], target)

    def twin_copy(j, half):
        part = hidden.at[:, aligned(piece(half, j), depth)] if last else hidden.at[piece(half, j)]
        return remote(part, part, d2d_ssem.at[j], d2d_rsem.at[j], place.sibling)

    def finish(j):
        step_two(j, True, comb.at[j]).wait_recv()
        step_two(j, False, comb.at[j]).wait_recv()
        summed = total[j, block(place.chip), :] + s2_left[j] + s2_right[j]
        if j >= RELAYED:
            step_one(j).wait_recv()
            summed = summed + s1_recv[j]
        value = (residual[j].astype(F32) + summed).astype(BF16)
        if last:
            hidden[block(place.chip), aligned(piece(place.half, j), depth)] = value
        else:
            hidden[piece(place.half, j), block(place.chip), :] = value
            next_residual[j] = value
        if j >= RING:
            send(gather_copy(j, 2, place.chip))
        send(gather_copy(j, 0, place.chip))
        send(gather_copy(j, 1, place.chip))

    def pass_on(j):
        gather_copy(j, 0, place.left).wait_recv()
        if j < RING and j % 2 == 0:
            send(forward_copy(j, place.left))
        gather_copy(j, 1, place.right).wait_recv()
        if j < RING and j % 2 == 1:
            send(forward_copy(j, place.right))

    def far_block(j):
        gather_copy(j, 2, place.across).wait_recv()
        send(twin_copy(j, place.half))

    for j in range(CHUNKS):
        finish(j)
    for j in range(RING):
        pass_on(j)
    order = list(range(RING, CHUNKS)) + list(range(RING))
    for j in order:
        if j >= RING:
            pass_on(j)
        far_block(j)
        if not last:
            for copy in w_copies if j == order[0] else ():
                copy.wait()
            add_query(piece(place.half, j), j == order[0], hidden, wq_buf, q_acc)
    for j in order:
        twin_copy(j, 1 - place.half).wait_recv()
        if not last:
            add_query(piece(1 - place.half, j), False, hidden, wq_buf, q_acc)
    if not last:
        outgoing = exchange_query(place, q_acc, q_send, q_out, q_ssem, q_rsem)
        new_rows(place, hidden, wkv_buf, kv_new)
        for copy in query_copies(place, q_send, q_out, q_ssem, q_rsem, True):
            copy.wait_recv()
        sends.extend(outgoing)
        for copy in cache_copies:
            copy.wait()
    for copy in sends:
        copy.wait_send()


GROUP = 8
SHORT = 256


def attention_kernel(layer, *refs):
    all_lens, q, kv_new, k_in, v_in = refs[:5]
    del k_in, v_in
    refs = refs[5:]
    first = layer == 0
    if first:
        k_cache, v_cache = refs[:2]
        refs = refs[2:]
    else:
        k_rest, v_rest = refs[2:4]
        refs = refs[4:]
    k_out, v_out, k_buf, v_buf, context, q_rows, c_rows, sems, load_sems, rest_sems = refs
    heads, local_rows, head_dim = q.shape
    seq_len = k_buf.shape[1]
    cut = cut_of(seq_len)
    rest = pl.ds(cut, seq_len - cut)
    tile = 16
    first_row = lax.axis_index("model") * local_rows

    def length(b):
        return all_lens[first_row + b]

    def rest_loads(b):
        return [
            pltpu.make_async_copy(cache.at[0, b, rest], buf.at[b, rest], load_sems.at[2 * b + n])
            for n, (cache, buf) in enumerate(((k_cache, k_buf), (v_cache, v_buf)))
        ]

    def rest_writes(b):
        pairs = ((k_buf, k_out), (v_buf, v_out)) if first else ((k_rest, k_out), (v_rest, v_out))
        return [
            pltpu.make_async_copy(buf.at[b, rest] if first else buf.at[b], out.at[0, b, rest], rest_sems.at[2 * b + n])
            for n, (buf, out) in enumerate(pairs)
        ]

    def each_rest(action):
        def one(b, _):
            @pl.when(length(b) >= cut if first else length(b) < cut)
            def _():
                action(b)
            return 0
        lax.fori_loop(0, local_rows, one, 0)

    def write_token(b):
        start = pl.multiple_of((length(b) // tile) * tile, tile)
        here = lax.broadcasted_iota(jnp.int32, (tile, head_dim), 0) == length(b) - start
        for buf, column in ((k_buf, 0), (v_buf, head_dim)):
            fresh = jnp.broadcast_to(kv_new[b:b + 1, column:column + head_dim], (tile, head_dim))
            old = buf[b, pl.ds(start, tile), :].astype(F32)
            buf[b, pl.ds(start, tile), :] = jnp.where(here, fresh, old).astype(BF16)

    def start_all(copies):
        for copy in copies:
            copy.start()

    def wait_copies(copies):
        for copy in copies:
            copy.wait()

    if first:
        each_rest(lambda b: start_all(rest_loads(b)))
    written = cut if first else seq_len
    writes = []
    parts = sems.shape[0] // 2
    step = local_rows // parts
    for i in range(parts):
        for b in range(i * step, (i + 1) * step):
            if first:
                pl.when(length(b) < cut)(functools.partial(write_token, b))
            else:
                write_token(b)
        part = pl.ds(i * step, step)
        for n, (buf, out) in enumerate(((k_buf, k_out), (v_buf, v_out))):
            writes.append(pltpu.make_async_copy(
                buf.at[part, pl.ds(0, written)], out.at[layer, part, pl.ds(0, written)], sems.at[2 * i + n]))
        if i > 0:
            start_all(writes[2 * i - 2:2 * i])
    q_rows[...] = q[...].astype(F32).reshape(heads * local_rows, head_dim)
    start_all(writes[-2:])
    if not first:
        each_rest(lambda b: start_all(rest_writes(b)))

    def attend(members, span):
        rows = [pl.ds(b, heads, stride=local_rows) for b in members]
        scores = [
            lax.dot_general(
                q_rows[r, :].astype(BF16), k_buf[b, pl.ds(0, span), :], (((1,), (1,)), ((), ())),
                preferred_element_type=F32)
            for b, r in zip(members, rows)
        ]
        positions = lax.broadcasted_iota(jnp.int32, (heads, span), 1)
        scores = [jnp.where(positions <= length(b), s * (head_dim ** -0.5), -jnp.inf) for b, s in zip(members, scores)]
        tops = [jnp.max(s, axis=1, keepdims=True) for s in scores]
        powers = [jnp.exp(s - t) for s, t in zip(scores, tops)]
        sums = [jnp.sum(p, axis=1, keepdims=True) for p in powers]
        weights = [(p / t).astype(BF16) for p, t in zip(powers, sums)]
        outs = [
            jnp.dot(w, v_buf[b, pl.ds(0, span), :], preferred_element_type=F32) for b, w in zip(members, weights)
        ]
        for r, out in zip(rows, outs):
            c_rows[r, :] = out.astype(BF16).astype(F32)

    for base in range(0, local_rows, GROUP):
        attend(list(range(base, base + GROUP)), SHORT)

    if first:
        for b in range(local_rows):
            @pl.when(length(b) >= cut)
            def _(b=b):
                wait_copies(rest_loads(b))
                write_token(b)
        each_rest(lambda b: start_all(rest_writes(b)))

    spans = []
    span = 2 * SHORT
    while span < cut:
        spans.append(span)
        span *= 2
    spans += [cut, seq_len]

    def longer(b, _):
        @pl.when(length(b) >= SHORT)
        def _():
            low = SHORT
            for span in spans:
                @pl.when(jnp.logical_and(length(b) >= low, length(b) < span))
                def _(span=span):
                    attend([b], span)
                low = span
        return 0

    lax.fori_loop(0, local_rows, longer, 0)
    context[...] = c_rows[...].reshape(heads, local_rows, head_dim).astype(BF16)
    each_rest(lambda b: wait_copies(rest_writes(b)))
    wait_copies(writes)


def solution(mesh):
    count = mesh.shape["model"]
    assert count == 2 * CHIPS
    row_axes = ("replica", "model")
    cache_spec = P(None, row_axes, None, None)
    DMA = pltpu.SemaphoreType.DMA

    def device_step(x, cache_len, w_query, w_key, w_value, w_out, k_cache, v_cache):
        rows, width = x.shape
        layers, local_rows, seq_len, head_dim = k_cache.shape
        local_width = w_query.shape[-1]
        local_heads = local_width // head_dim
        heads = local_heads * count
        pieces = 2 * CHUNKS
        depth = width // pieces
        chip_rows = rows // CHIPS
        rest_shape = (local_rows, seq_len - cut_of(seq_len), head_dim)
        w_query, w_key, w_value, w_out = map(to_hbm, (w_query, w_key, w_value, w_out))
        x, k_cache, v_cache = map(to_hbm, (x, k_cache, v_cache))

        project_out = (
            pltpu.VMEM((heads, local_rows, head_dim), BF16),
            pltpu.VMEM((local_rows, 2 * head_dim), F32),
            pltpu.VMEM((CHUNKS, chip_rows, depth), BF16),
            pltpu.VMEM(k_cache.shape[1:], BF16),
            pltpu.VMEM(v_cache.shape[1:], BF16),
        )
        project_scratch = [
            pltpu.VMEM((pieces, rows, depth), BF16),
            pltpu.VMEM((width, local_width), BF16),
            pltpu.VMEM((width, 2 * head_dim), BF16),
            pltpu.VMEM((rows, local_width), F32),
            pltpu.VMEM((local_heads, rows, head_dim), BF16),
        ]
        project_sems = [DMA((pieces + 2,)), DMA((2 * PARTS,)), DMA((count,)), DMA((count,))]
        mix_scratch = [
            pltpu.VMEM((local_heads, rows, head_dim), BF16),
            pltpu.VMEM((CHUNKS, local_width, depth), BF16),
            pltpu.VMEM((CHUNKS, local_width, depth), BF16),
            pltpu.VMEM((CHUNKS, rows, depth), F32),
            pltpu.VMEM((CHUNKS, rows, depth), F32),
            pltpu.VMEM((CHUNKS, rows, depth), F32),
            pltpu.VMEM((CHUNKS, chip_rows, depth), F32),
            pltpu.VMEM((CHUNKS, chip_rows, depth), F32),
            pltpu.VMEM((CHUNKS, chip_rows, depth), F32),
            pltpu.VMEM((CHUNKS, chip_rows, depth), F32),
            DMA((pieces,)), DMA((count,)), DMA((count,)), DMA((CHUNKS,)), DMA((CHUNKS,)), DMA((CHUNKS,)), DMA((CHUNKS,)),
            DMA((2 * CHUNKS,)), DMA((2 * CHUNKS,)), DMA((3 * CHUNKS,)), DMA((3 * CHUNKS,)),
            DMA((CHUNKS,)), DMA((CHUNKS,)),
        ]

        def params(collective_id, limit):
            return pltpu.CompilerParams(collective_id=collective_id, has_side_effects=True, vmem_limit_bytes=limit * MIB)

        query, kv_new, residual, k_vmem, v_vmem = pl.pallas_call(
            functools.partial(first_kernel, count),
            out_shape=project_out,
            in_specs=[ANY_SPEC] * 6,
            out_specs=(VMEM_SPEC,) * 5,
            scratch_shapes=project_scratch + [DMA((pieces,))] + project_sems,
            compiler_params=params(0, 16),
            name="first",
        )(x, w_query, w_key, w_value, k_cache, v_cache)

        k_new_cache = v_new_cache = None
        for layer in range(layers):
            last = layer == layers - 1
            operands = [cache_len, query, kv_new, k_vmem, v_vmem]
            specs = [SMEM_SPEC] + [VMEM_SPEC] * 4
            aliases = {3: 2, 4: 3}
            if layer > 0:
                operands += [k_new_cache, v_new_cache, k_rest, v_rest]
                specs += [ANY_SPEC] * 2 + [VMEM_SPEC] * 2
                aliases |= {5: 0, 6: 1}
            else:
                operands += [k_cache, v_cache]
                specs += [ANY_SPEC] * 2
            k_new_cache, v_new_cache, _, _, context = pl.pallas_call(
                functools.partial(attention_kernel, layer),
                out_shape=(
                    pltpu.HBM(k_cache.shape, BF16),
                    pltpu.HBM(v_cache.shape, BF16),
                    pltpu.VMEM(k_cache.shape[1:], BF16),
                    pltpu.VMEM(v_cache.shape[1:], BF16),
                    pltpu.VMEM((heads, local_rows, head_dim), BF16),
                ),
                in_specs=specs,
                out_specs=(ANY_SPEC, ANY_SPEC, VMEM_SPEC, VMEM_SPEC, VMEM_SPEC),
                input_output_aliases=aliases,
                scratch_shapes=[
                    pltpu.VMEM((heads * local_rows, head_dim), F32),
                    pltpu.VMEM((heads * local_rows, head_dim), F32),
                    DMA((2 * PARTS,)),
                    DMA((2 * local_rows,)),
                    DMA((2 * local_rows,)),
                ],
                compiler_params=pltpu.CompilerParams(vmem_limit_bytes=16 * MIB),
                name=f"attend{layer}",
            )(*operands)
            if not last:
                query, kv_new, residual, k_vmem, v_vmem, k_rest, v_rest = pl.pallas_call(
                    functools.partial(mix_kernel, count, False, layer),
                    out_shape=project_out + (pltpu.VMEM(rest_shape, BF16),) * 2,
                    in_specs=[VMEM_SPEC] * 2 + [ANY_SPEC] * 6,
                    out_specs=(VMEM_SPEC,) * 7,
                    scratch_shapes=mix_scratch + project_scratch + project_sems + [DMA((2,))],
                    compiler_params=params(1 + layer, 28),
                    name=f"mix{layer}",
                )(context, residual, w_out, w_query, w_key, w_value, k_cache, v_cache)
            else:
                hidden = pl.pallas_call(
                    functools.partial(mix_kernel, count, True, layer),
                    out_shape=pltpu.VMEM((rows, width), BF16),
                    in_specs=[VMEM_SPEC] * 2 + [ANY_SPEC],
                    out_specs=VMEM_SPEC,
                    scratch_shapes=mix_scratch,
                    compiler_params=params(1 + layer, 20),
                    name=f"mix{layer}",
                )(context, residual, w_out)
        return hidden, k_new_cache, v_new_cache

    return jax.shard_map(
        device_step,
        mesh=mesh,
        in_specs=(P("replica", None), P("replica"), P(None, None, "model"), P(), P(), P(None, "model", None), cache_spec, cache_spec),
        out_specs=(P("replica", None), cache_spec, cache_spec),
        check_vma=False,
    )
```

```python
import functools

import jax
import jax.numpy as jnp
from jax import lax
from jax.experimental import pallas as pl
from jax.experimental.pallas import tpu as pltpu
from jax.sharding import PartitionSpec as P

MESH = pl.DeviceIdType.MESH
F32 = jnp.float32
BF16 = jnp.bfloat16
CHIPS = 4
CHUNKS = 4
PARTS = 8
RING = 2
EARLY = 2
MIB = 1 << 20

ANY_SPEC = pl.BlockSpec(memory_space=pltpu.HBM)
VMEM_SPEC = pl.BlockSpec(memory_space=pltpu.VMEM)
SMEM_SPEC = pl.BlockSpec(memory_space=pltpu.SMEM)


def to_hbm(value):
    return pltpu.with_memory_space_constraint(value, pltpu.HBM)


def to_vmem(value):
    return pltpu.with_memory_space_constraint(value, pltpu.VMEM)


def aligned(index, size):
    return pl.ds(pl.multiple_of(index * size, size), size)


OWN, LEFT, RIGHT, ACROSS = range(4)
MIRROR = (OWN, RIGHT, LEFT, ACROSS)


class Place:
    def __init__(self, count):
        self.count = count
        self.me = lax.axis_index("model")
        self.chip = self.me // 2
        self.core = self.me % 2
        self.right = (self.chip + 1) % CHIPS
        self.left = (self.chip + CHIPS - 1) % CHIPS
        self.across = (self.chip + 2) % CHIPS
        self.half = (self.core + self.chip) % 2
        self.to_right = self.right * 2 + 1 - self.core
        self.to_left = self.left * 2 + 1 - self.core
        self.sibling = self.chip * 2 + (1 - self.core)

    def device(self, kind, cross):
        chip = (self.chip, self.left, self.right, self.across)[kind]
        return chip * 2 + (1 - self.core if cross else self.core)

    def peer(self, offset):
        return (self.me + offset) % self.count

    def origin(self, offset):
        return (self.me + self.count - offset) % self.count


def remote(src, dst, send_sem, recv_sem, device):
    return pltpu.make_async_remote_copy(
        src_ref=src, dst_ref=dst, send_sem=send_sem, recv_sem=recv_sem,
        device_id={"model": device}, device_id_type=MESH)


def signal_all(place):
    barrier = pltpu.get_barrier_semaphore()
    for offset in send_order(place.count):
        pl.semaphore_signal(barrier, inc=1, device_id={"model": place.peer(offset)}, device_id_type=MESH)


def wait_all(place):
    pl.semaphore_wait(pltpu.get_barrier_semaphore(), place.count - 1)


def weight_copies(layer, wq, wk, wv, wq_buf, wkv_buf, sems):
    pieces = sems.shape[0] - 2
    depth = wq_buf.shape[0] // pieces
    head_dim = wk.shape[-1]
    copies = [
        pltpu.make_async_copy(wq.at[layer, pl.ds(i * depth, depth), :], wq_buf.at[pl.ds(i * depth, depth), :], sems.at[i])
        for i in range(pieces)
    ]
    copies.append(pltpu.make_async_copy(wk.at[layer], wkv_buf.at[:, pl.ds(0, head_dim)], sems.at[pieces]))
    copies.append(pltpu.make_async_copy(wv.at[layer], wkv_buf.at[:, pl.ds(head_dim, head_dim)], sems.at[pieces + 1]))
    return copies


def cache_loads(layer, k_cache, v_cache, k_vmem, v_vmem, sems):
    parts = sems.shape[0] // 2
    step = k_vmem.shape[0] // parts
    copies = []
    for i in range(parts):
        part = pl.ds(i * step, step)
        copies.append(pltpu.make_async_copy(k_cache.at[layer, part], k_vmem.at[part], sems.at[2 * i]))
        copies.append(pltpu.make_async_copy(v_cache.at[layer, part], v_vmem.at[part], sems.at[2 * i + 1]))
    return copies


def add_query(piece, first, hidden, wq_buf, q_acc):
    depth = hidden.shape[-1]
    part = jnp.dot(hidden[piece], wq_buf[aligned(piece, depth), :], preferred_element_type=F32)
    q_acc[...] = part if first else q_acc[...] + part


def new_rows(place, hidden, wkv_buf, kv_new):
    pieces, rows, depth = hidden.shape
    local_rows = rows // place.count
    total = None
    for piece in range(pieces):
        mine = hidden[piece, aligned(place.me, local_rows), :]
        part = jnp.dot(mine, wkv_buf[pl.ds(piece * depth, depth), :], preferred_element_type=F32)
        total = part if total is None else total + part
    kv_new[...] = total.astype(BF16).astype(F32)


def query_copies(place, q_send, q_out, send_sems, recv_sems, incoming):
    heads = q_send.shape[0]
    local_rows = q_out.shape[1]
    copies = []
    for offset in range(1, place.count):
        source = place.origin(offset) if incoming else place.me
        target = place.peer(offset)
        copies.append(remote(
            q_send.at[:, aligned(target, local_rows), :], q_out.at[pl.ds(source * heads, heads)],
            send_sems.at[offset], recv_sems.at[offset], target))
    return copies


def send_order(count):
    return sorted(range(1, count), key=lambda offset: -min(offset, count - offset))


def exchange_query(place, q_acc, q_send, q_out, send_sems, recv_sems):
    heads, rows, head_dim = q_send.shape
    local_rows = q_out.shape[1]
    for head in range(heads):
        q_send[head] = q_acc[:, head * head_dim:(head + 1) * head_dim].astype(BF16)
    outgoing = query_copies(place, q_send, q_out, send_sems, recv_sems, False)
    for offset in send_order(place.count):
        outgoing[offset - 1].start()
    q_out[pl.ds(place.me * heads, heads)] = q_send[:, aligned(place.me, local_rows), :]
    return outgoing


def first_kernel(count, x, wq, wk, wv, k_cache, v_cache,
                 q_out, kv_new, residual, k_vmem, v_vmem,
                 hidden, wq_buf, wkv_buf, q_acc, q_send,
                 x_sems, w_sems, cache_sems, q_ssem, q_rsem):
    place = Place(count)
    pieces, rows, depth = hidden.shape
    x_copies = [
        pltpu.make_async_copy(x.at[:, pl.ds(i * depth, depth)], hidden.at[i], x_sems.at[i]) for i in range(pieces)
    ]
    w_copies = weight_copies(0, wq, wk, wv, wq_buf, wkv_buf, w_sems)
    cache_copies = cache_loads(0, k_cache, v_cache, k_vmem, v_vmem, cache_sems)
    for i in range(pieces):
        x_copies[i].start()
        w_copies[i].start()
    signal_all(place)
    w_copies[pieces].start()
    w_copies[pieces + 1].start()
    for copy in cache_copies:
        copy.start()
    for i in range(pieces):
        x_copies[i].wait()
        w_copies[i].wait()
        add_query(i, i == 0, hidden, wq_buf, q_acc)
    wait_all(place)
    outgoing = exchange_query(place, q_acc, q_send, q_out, q_ssem, q_rsem)
    chip_rows = residual.shape[1]
    for j in range(CHUNKS):
        residual[j] = hidden[place.half * CHUNKS + j, aligned(place.chip, chip_rows), :]
    w_copies[pieces].wait()
    w_copies[pieces + 1].wait()
    new_rows(place, hidden, wkv_buf, kv_new)
    for copy in query_copies(place, q_send, q_out, q_ssem, q_rsem, True):
        copy.wait_recv()
    for copy in outgoing:
        copy.wait_send()
    for copy in cache_copies:
        copy.wait()


def mix_kernel(count, last, layer, *refs):
    refs = list(refs)
    take = lambda k: [refs.pop(0) for _ in range(k)]
    context, residual, wo = take(3)
    if not last:
        wq, wk, wv, k_cache, v_cache = take(5)
        q_out, kv_new, next_residual, k_vmem, v_vmem = take(5)
    else:
        (hidden,) = take(1)
    c_recv, wo_far, wo_own, p_send, p_recv, total, s1_recv, comb, s2_left, s2_right = take(10)
    wo_sems, c_ssem, c_rsem, p_ssem, p_rsem, s1_ssem, s1_rsem = take(7)
    s2_ssem, s2_rsem, ag_ssem, ag_rsem, d2d_ssem, d2d_rsem = take(6)
    if not last:
        hidden, wq_buf, wkv_buf, q_acc, q_send, w_sems, cache_sems, q_ssem, q_rsem = take(9)
    place = Place(count)
    heads, rows, head_dim = c_recv.shape
    local_rows = rows // count
    chip_rows = rows // CHIPS
    depth = total.shape[-1]

    signal_all(place)
    wo_copies = []
    for j in range(CHUNKS):
        wo_copies.append(pltpu.make_async_copy(
            wo.at[layer, :, aligned((1 - place.half) * CHUNKS + j, depth)], wo_far.at[j], wo_sems.at[j]))
    for j in range(CHUNKS):
        wo_copies.append(pltpu.make_async_copy(
            wo.at[layer, :, aligned(place.half * CHUNKS + j, depth)], wo_own.at[j], wo_sems.at[CHUNKS + j]))
    for copy in wo_copies:
        copy.start()
    if not last:
        w_copies = weight_copies(layer + 1, wq, wk, wv, wq_buf, wkv_buf, w_sems)
        cache_copies = cache_loads(layer + 1, k_cache, v_cache, k_vmem, v_vmem, cache_sems)
        for copy in w_copies + cache_copies:
            copy.start()

    near = pl.ds(0, ACROSS * chip_rows)

    def block(kind):
        return pl.ds(kind * chip_rows, chip_rows)

    def context_rows(kind, core):
        return pl.ds(pl.multiple_of(kind * chip_rows + core * local_rows, local_rows), local_rows)

    c_recv[:, context_rows(OWN, place.core), :] = context[pl.ds(place.me * heads, heads)]
    wait_all(place)

    def context_copy(kind, cross, incoming):
        target = place.device(kind, cross)
        sender = (1 - place.core if cross else place.core) if incoming else place.core
        seen = kind if incoming else MIRROR[kind]
        return remote(
            context.at[pl.ds(target * heads, heads)], c_recv.at[:, context_rows(seen, sender), :],
            c_ssem.at[2 * kind + cross], c_rsem.at[2 * seen + cross], target)

    sends = []

    def send(copy):
        copy.start()
        sends.append(copy)

    for kind in (ACROSS, RIGHT, LEFT):
        for cross in range(2):
            send(context_copy(kind, cross, False))
    send(context_copy(OWN, 1, False))

    def product(weights, rows_of):
        acc = None
        for pair in range(heads // 2):
            lhs = jnp.concatenate([c_recv[2 * pair, rows_of], c_recv[2 * pair + 1, rows_of]], axis=1)
            part = jnp.dot(lhs, weights[pl.ds(pair * 2 * head_dim, 2 * head_dim), :], preferred_element_type=F32)
            acc = part if acc is None else acc + part
        return acc

    def pair_copy(j, far):
        part = block(ACROSS) if far else near
        slot = far * CHUNKS + j
        return remote(p_send.at[j, part], p_recv.at[j, part], p_ssem.at[slot], p_rsem.at[slot], place.sibling)

    context_copy(OWN, 1, True).wait_recv()
    for kind in (LEFT, RIGHT):
        for cross in range(2):
            context_copy(kind, cross, True).wait_recv()
    for j in range(CHUNKS):
        wo_copies[j].wait()
        p_send[j, near] = product(wo_far.at[j], near)
        send(pair_copy(j, 0))
    for j in range(CHUNKS):
        wo_copies[CHUNKS + j].wait()
        total[j, near] = product(wo_own.at[j], near)
    for cross in range(2):
        context_copy(ACROSS, cross, True).wait_recv()
    for j in range(CHUNKS):
        p_send[j, block(ACROSS)] = product(wo_far.at[j], block(ACROSS))
        send(pair_copy(j, 1))

    def step_one(j):
        target = place.to_right if j % 2 == 0 else place.to_left
        return remote(total.at[j, block(ACROSS)], s1_recv.at[j], s1_ssem.at[j], s1_rsem.at[j], target)

    def step_two(j, rightward, source):
        target = place.to_right if rightward else place.to_left
        inbox = s2_left if rightward else s2_right
        slot = j if rightward else CHUNKS + j
        return remote(source, inbox.at[j], s2_ssem.at[slot], s2_rsem.at[slot], target)

    def direct(j):
        rightward = j % 2 == 1
        send(step_two(j, rightward, total.at[j, block(RIGHT if rightward else LEFT)]))

    def combine(j):
        step_one(j).wait_recv()
        rightward = j % 2 == 0
        comb[j] = total[j, block(RIGHT if rightward else LEFT)] + s1_recv[j]
        send(step_two(j, rightward, comb.at[j]))

    for j in range(CHUNKS):
        pair_copy(j, 0).wait_recv()
        total[j, near] += p_recv[j, near]
        if j < EARLY:
            direct(j)
    for j in range(CHUNKS):
        total[j, block(ACROSS)] = product(wo_own.at[j], block(ACROSS))
    for j in range(CHUNKS):
        pair_copy(j, 1).wait_recv()
        total[j, block(ACROSS)] += p_recv[j, block(ACROSS)]
        send(step_one(j))
    for j in range(EARLY, CHUNKS):
        direct(j)
    for j in range(CHUNKS):
        combine(j)

    def chip_block(chip):
        return aligned(chip, chip_rows)

    def piece(half, j):
        return half * CHUNKS + j

    def region(half, j, chip):
        if last:
            return hidden.at[chip_block(chip), aligned(piece(half, j), depth)]
        return hidden.at[piece(half, j), chip_block(chip), :]

    def gather_copy(j, way, chip):
        target = (place.to_right, place.to_left, place.across * 2 + place.core)[way]
        part = region(place.half, j, chip)
        slot = way * CHUNKS + j
        return remote(part, part, ag_ssem.at[slot], ag_rsem.at[slot], target)

    def forward_copy(j, chip):
        target = place.to_right if j % 2 == 0 else place.to_left
        part = region(place.half, j, chip)
        return remote(part, part, ag_ssem.at[2 * CHUNKS + j], ag_rsem.at[2 * CHUNKS + j], target)

    def twin_copy(j, half):
        part = hidden.at[:, aligned(piece(half, j), depth)] if last else hidden.at[piece(half, j)]
        return remote(part, part, d2d_ssem.at[j], d2d_rsem.at[j], place.sibling)

    def finish(j):
        step_two(j, True, comb.at[j]).wait_recv()
        step_two(j, False, comb.at[j]).wait_recv()
        summed = total[j, block(OWN)] + s2_left[j] + s2_right[j]
        value = (residual[j].astype(F32) + summed).astype(BF16)
        if last:
            hidden[chip_block(place.chip), aligned(piece(place.half, j), depth)] = value
        else:
            hidden[piece(place.half, j), chip_block(place.chip), :] = value
            next_residual[j] = value
        if j >= RING:
            send(gather_copy(j, 2, place.chip))
        send(gather_copy(j, 0, place.chip))
        send(gather_copy(j, 1, place.chip))

    def pass_on(j):
        gather_copy(j, 0, place.left).wait_recv()
        if j < RING and j % 2 == 0:
            send(forward_copy(j, place.left))
        gather_copy(j, 1, place.right).wait_recv()
        if j < RING and j % 2 == 1:
            send(forward_copy(j, place.right))

    def far_block(j):
        gather_copy(j, 2, place.across).wait_recv()
        send(twin_copy(j, place.half))

    for j in range(CHUNKS):
        finish(j)
    for j in range(RING):
        pass_on(j)
    order = list(range(RING, CHUNKS)) + list(range(RING))
    for j in order:
        if j >= RING:
            pass_on(j)
        far_block(j)
        if not last:
            for copy in w_copies if j == order[0] else ():
                copy.wait()
            add_query(piece(place.half, j), j == order[0], hidden, wq_buf, q_acc)
    for j in order:
        twin_copy(j, 1 - place.half).wait_recv()
        if not last:
            add_query(piece(1 - place.half, j), False, hidden, wq_buf, q_acc)
    if not last:
        outgoing = exchange_query(place, q_acc, q_send, q_out, q_ssem, q_rsem)
        new_rows(place, hidden, wkv_buf, kv_new)
        for copy in query_copies(place, q_send, q_out, q_ssem, q_rsem, True):
            copy.wait_recv()
        sends.extend(outgoing)
        for copy in cache_copies:
            copy.wait()
    for copy in sends:
        copy.wait_send()


GROUP = 8
SHORT = 256


def attention_kernel(layer, *refs):
    all_lens, q, kv_new, k_in, v_in = refs[:5]
    refs = refs[5:]
    if layer > 0:
        refs = refs[2:]
    k_out, v_out, k_buf, v_buf, context, q_rows, c_rows, sems = refs
    del k_in, v_in
    heads, local_rows, head_dim = q.shape
    seq_len = k_buf.shape[1]
    tile = 16
    first_row = lax.axis_index("model") * local_rows

    def length(b):
        return all_lens[first_row + b]

    writes = []
    parts = sems.shape[0] // 2
    step = local_rows // parts
    for i in range(parts):
        for b in range(i * step, (i + 1) * step):
            start = pl.multiple_of((length(b) // tile) * tile, tile)
            here = lax.broadcasted_iota(jnp.int32, (tile, head_dim), 0) == length(b) - start
            for buf, column in ((k_buf, 0), (v_buf, head_dim)):
                fresh = jnp.broadcast_to(kv_new[b:b + 1, column:column + head_dim], (tile, head_dim))
                old = buf[b, pl.ds(start, tile), :].astype(F32)
                buf[b, pl.ds(start, tile), :] = jnp.where(here, fresh, old).astype(BF16)
        part = pl.ds(i * step, step)
        writes.append(pltpu.make_async_copy(k_buf.at[part], k_out.at[layer, part], sems.at[2 * i]))
        writes.append(pltpu.make_async_copy(v_buf.at[part], v_out.at[layer, part], sems.at[2 * i + 1]))
        if i > 0:
            writes[2 * i - 2].start()
            writes[2 * i - 1].start()
    q_rows[...] = q[...].astype(F32).reshape(heads * local_rows, head_dim)
    writes[-2].start()
    writes[-1].start()

    def attend(members, span):
        rows = [pl.ds(b, heads, stride=local_rows) for b in members]
        scores = [
            lax.dot_general(
                q_rows[r, :].astype(BF16), k_buf[b, pl.ds(0, span), :], (((1,), (1,)), ((), ())),
                preferred_element_type=F32)
            for b, r in zip(members, rows)
        ]
        positions = lax.broadcasted_iota(jnp.int32, (heads, span), 1)
        scores = [jnp.where(positions <= length(b), s * (head_dim ** -0.5), -jnp.inf) for b, s in zip(members, scores)]
        tops = [jnp.max(s, axis=1, keepdims=True) for s in scores]
        powers = [jnp.exp(s - t) for s, t in zip(scores, tops)]
        sums = [jnp.sum(p, axis=1, keepdims=True) for p in powers]
        weights = [(p / t).astype(BF16) for p, t in zip(powers, sums)]
        outs = [
            jnp.dot(w, v_buf[b, pl.ds(0, span), :], preferred_element_type=F32) for b, w in zip(members, weights)
        ]
        for r, out in zip(rows, outs):
            c_rows[r, :] = out.astype(BF16).astype(F32)

    for first in range(0, local_rows, GROUP):
        attend(list(range(first, first + GROUP)), SHORT)

    spans = []
    span = 2 * SHORT
    while span < seq_len:
        spans.append(span)
        span *= 2
    spans.append(seq_len)

    def longer(b, _):
        @pl.when(length(b) >= SHORT)
        def _():
            low = SHORT
            for span in spans:
                @pl.when(jnp.logical_and(length(b) >= low, length(b) < span))
                def _(span=span):
                    attend([b], span)
                low = span
        return 0

    lax.fori_loop(0, local_rows, longer, 0)
    context[...] = c_rows[...].reshape(heads, local_rows, head_dim).astype(BF16)
    for copy in writes:
        copy.wait()


def solution(mesh):
    count = mesh.shape["model"]
    assert count == 2 * CHIPS
    row_axes = ("replica", "model")
    cache_spec = P(None, row_axes, None, None)
    DMA = pltpu.SemaphoreType.DMA

    def device_step(x, cache_len, w_query, w_key, w_value, w_out, k_cache, v_cache):
        rows, width = x.shape
        layers, local_rows, seq_len, head_dim = k_cache.shape
        local_width = w_query.shape[-1]
        local_heads = local_width // head_dim
        heads = local_heads * count
        pieces = 2 * CHUNKS
        depth = width // pieces
        chip_rows = rows // CHIPS
        w_query, w_key, w_value, w_out = map(to_hbm, (w_query, w_key, w_value, w_out))
        x, k_cache, v_cache = map(to_hbm, (x, k_cache, v_cache))

        project_out = (
            pltpu.VMEM((heads, local_rows, head_dim), BF16),
            pltpu.VMEM((local_rows, 2 * head_dim), F32),
            pltpu.VMEM((CHUNKS, chip_rows, depth), BF16),
            pltpu.VMEM(k_cache.shape[1:], BF16),
            pltpu.VMEM(v_cache.shape[1:], BF16),
        )
        project_scratch = [
            pltpu.VMEM((pieces, rows, depth), BF16),
            pltpu.VMEM((width, local_width), BF16),
            pltpu.VMEM((width, 2 * head_dim), BF16),
            pltpu.VMEM((rows, local_width), F32),
            pltpu.VMEM((local_heads, rows, head_dim), BF16),
        ]
        project_sems = [DMA((pieces + 2,)), DMA((2 * PARTS,)), DMA((count,)), DMA((count,))]
        mix_scratch = [
            pltpu.VMEM((local_heads, rows, head_dim), BF16),
            pltpu.VMEM((CHUNKS, local_width, depth), BF16),
            pltpu.VMEM((CHUNKS, local_width, depth), BF16),
            pltpu.VMEM((CHUNKS, rows, depth), F32),
            pltpu.VMEM((CHUNKS, rows, depth), F32),
            pltpu.VMEM((CHUNKS, rows, depth), F32),
            pltpu.VMEM((CHUNKS, chip_rows, depth), F32),
            pltpu.VMEM((CHUNKS, chip_rows, depth), F32),
            pltpu.VMEM((CHUNKS, chip_rows, depth), F32),
            pltpu.VMEM((CHUNKS, chip_rows, depth), F32),
            DMA((pieces,)), DMA((count,)), DMA((count,)), DMA((pieces,)), DMA((pieces,)), DMA((CHUNKS,)), DMA((CHUNKS,)),
            DMA((2 * CHUNKS,)), DMA((2 * CHUNKS,)), DMA((3 * CHUNKS,)), DMA((3 * CHUNKS,)),
            DMA((CHUNKS,)), DMA((CHUNKS,)),
        ]

        def params(collective_id, limit):
            return pltpu.CompilerParams(collective_id=collective_id, has_side_effects=True, vmem_limit_bytes=limit * MIB)

        query, kv_new, residual, k_vmem, v_vmem = pl.pallas_call(
            functools.partial(first_kernel, count),
            out_shape=project_out,
            in_specs=[ANY_SPEC] * 6,
            out_specs=(VMEM_SPEC,) * 5,
            scratch_shapes=project_scratch + [DMA((pieces,))] + project_sems,
            compiler_params=params(0, 16),
            name="first",
        )(x, w_query, w_key, w_value, k_cache, v_cache)

        k_new_cache = v_new_cache = None
        for layer in range(layers):
            last = layer == layers - 1
            operands = [cache_len, query, kv_new, k_vmem, v_vmem]
            specs = [SMEM_SPEC] + [VMEM_SPEC] * 4
            aliases = {3: 2, 4: 3}
            if layer > 0:
                operands += [k_new_cache, v_new_cache]
                specs += [ANY_SPEC] * 2
                aliases |= {5: 0, 6: 1}
            k_new_cache, v_new_cache, _, _, context = pl.pallas_call(
                functools.partial(attention_kernel, layer),
                out_shape=(
                    pltpu.HBM(k_cache.shape, BF16),
                    pltpu.HBM(v_cache.shape, BF16),
                    pltpu.VMEM(k_cache.shape[1:], BF16),
                    pltpu.VMEM(v_cache.shape[1:], BF16),
                    pltpu.VMEM((heads, local_rows, head_dim), BF16),
                ),
                in_specs=specs,
                out_specs=(ANY_SPEC, ANY_SPEC, VMEM_SPEC, VMEM_SPEC, VMEM_SPEC),
                input_output_aliases=aliases,
                scratch_shapes=[
                    pltpu.VMEM((heads * local_rows, head_dim), F32),
                    pltpu.VMEM((heads * local_rows, head_dim), F32),
                    DMA((2 * PARTS,)),
                ],
                compiler_params=pltpu.CompilerParams(vmem_limit_bytes=16 * MIB),
                name=f"attend{layer}",
            )(*operands)
            if not last:
                query, kv_new, residual, k_vmem, v_vmem = pl.pallas_call(
                    functools.partial(mix_kernel, count, False, layer),
                    out_shape=project_out,
                    in_specs=[VMEM_SPEC] * 2 + [ANY_SPEC] * 6,
                    out_specs=(VMEM_SPEC,) * 5,
                    scratch_shapes=mix_scratch + project_scratch + project_sems,
                    compiler_params=params(1 + layer, 28),
                    name=f"mix{layer}",
                )(context, residual, w_out, w_query, w_key, w_value, k_cache, v_cache)
            else:
                hidden = pl.pallas_call(
                    functools.partial(mix_kernel, count, True, layer),
                    out_shape=pltpu.VMEM((rows, width), BF16),
                    in_specs=[VMEM_SPEC] * 2 + [ANY_SPEC],
                    out_specs=VMEM_SPEC,
                    scratch_shapes=mix_scratch,
                    compiler_params=params(1 + layer, 20),
                    name=f"mix{layer}",
                )(context, residual, w_out)
        return hidden, k_new_cache, v_new_cache

    return jax.shard_map(
        device_step,
        mesh=mesh,
        in_specs=(P("replica", None), P("replica"), P(None, None, "model"), P(), P(), P(None, "model", None), cache_spec, cache_spec),
        out_specs=(P("replica", None), cache_spec, cache_spec),
        check_vma=False,
    )
```

```python
import functools

import jax
import jax.numpy as jnp
from jax import lax
from jax.experimental import pallas as pl
from jax.experimental.pallas import tpu as pltpu
from jax.sharding import PartitionSpec as P

MESH = pl.DeviceIdType.MESH
F32 = jnp.float32
BF16 = jnp.bfloat16
CHIPS = 4
CHUNKS = 4
PARTS = 8
RING = 4
RELAYED = 4
MIB = 1 << 20

ANY_SPEC = pl.BlockSpec(memory_space=pltpu.HBM)
VMEM_SPEC = pl.BlockSpec(memory_space=pltpu.VMEM)
SMEM_SPEC = pl.BlockSpec(memory_space=pltpu.SMEM)


def to_hbm(value):
    return pltpu.with_memory_space_constraint(value, pltpu.HBM)


def to_vmem(value):
    return pltpu.with_memory_space_constraint(value, pltpu.VMEM)


def aligned(index, size):
    return pl.ds(pl.multiple_of(index * size, size), size)


class Place:
    def __init__(self, count):
        self.count = count
        self.me = lax.axis_index("model")
        self.chip = self.me // 2
        self.core = self.me % 2
        self.right = (self.chip + 1) % CHIPS
        self.left = (self.chip + CHIPS - 1) % CHIPS
        self.across = (self.chip + 2) % CHIPS
        self.half = (self.core + self.chip) % 2
        self.to_right = self.right * 2 + 1 - self.core
        self.to_left = self.left * 2 + 1 - self.core
        self.sibling = self.chip * 2 + (1 - self.core)

    def peer(self, offset):
        return (self.me + offset) % self.count

    def origin(self, offset):
        return (self.me + self.count - offset) % self.count


def remote(src, dst, send_sem, recv_sem, device):
    return pltpu.make_async_remote_copy(
        src_ref=src, dst_ref=dst, send_sem=send_sem, recv_sem=recv_sem,
        device_id={"model": device}, device_id_type=MESH)


def signal_all(place):
    barrier = pltpu.get_barrier_semaphore()
    for offset in send_order(place.count):
        pl.semaphore_signal(barrier, inc=1, device_id={"model": place.peer(offset)}, device_id_type=MESH)


def wait_all(place):
    pl.semaphore_wait(pltpu.get_barrier_semaphore(), place.count - 1)


def weight_copies(layer, wq, wk, wv, wq_buf, wkv_buf, sems):
    pieces = sems.shape[0] - 2
    depth = wq_buf.shape[0] // pieces
    head_dim = wk.shape[-1]
    copies = [
        pltpu.make_async_copy(wq.at[layer, pl.ds(i * depth, depth), :], wq_buf.at[pl.ds(i * depth, depth), :], sems.at[i])
        for i in range(pieces)
    ]
    copies.append(pltpu.make_async_copy(wk.at[layer], wkv_buf.at[:, pl.ds(0, head_dim)], sems.at[pieces]))
    copies.append(pltpu.make_async_copy(wv.at[layer], wkv_buf.at[:, pl.ds(head_dim, head_dim)], sems.at[pieces + 1]))
    return copies


def cache_loads(layer, k_cache, v_cache, k_vmem, v_vmem, sems):
    parts = sems.shape[0] // 2
    step = k_vmem.shape[0] // parts
    copies = []
    for i in range(parts):
        part = pl.ds(i * step, step)
        copies.append(pltpu.make_async_copy(k_cache.at[layer, part], k_vmem.at[part], sems.at[2 * i]))
        copies.append(pltpu.make_async_copy(v_cache.at[layer, part], v_vmem.at[part], sems.at[2 * i + 1]))
    return copies


def add_query(piece, first, hidden, wq_buf, q_acc):
    depth = hidden.shape[-1]
    part = jnp.dot(hidden[piece], wq_buf[aligned(piece, depth), :], preferred_element_type=F32)
    q_acc[...] = part if first else q_acc[...] + part


def new_rows(place, hidden, wkv_buf, kv_new):
    pieces, rows, depth = hidden.shape
    local_rows = rows // place.count
    total = None
    for piece in range(pieces):
        mine = hidden[piece, aligned(place.me, local_rows), :]
        part = jnp.dot(mine, wkv_buf[pl.ds(piece * depth, depth), :], preferred_element_type=F32)
        total = part if total is None else total + part
    kv_new[...] = total.astype(BF16).astype(F32)


def query_copies(place, q_send, q_out, send_sems, recv_sems, incoming):
    heads = q_send.shape[0]
    local_rows = q_out.shape[1]
    copies = []
    for offset in range(1, place.count):
        source = place.origin(offset) if incoming else place.me
        target = place.peer(offset)
        copies.append(remote(
            q_send.at[:, aligned(target, local_rows), :], q_out.at[pl.ds(source * heads, heads)],
            send_sems.at[offset], recv_sems.at[offset], target))
    return copies


def send_order(count):
    return sorted(range(1, count), key=lambda offset: -min(offset, count - offset))


def exchange_query(place, q_acc, q_send, q_out, send_sems, recv_sems):
    heads, rows, head_dim = q_send.shape
    local_rows = q_out.shape[1]
    for head in range(heads):
        q_send[head] = q_acc[:, head * head_dim:(head + 1) * head_dim].astype(BF16)
    outgoing = query_copies(place, q_send, q_out, send_sems, recv_sems, False)
    for offset in send_order(place.count):
        outgoing[offset - 1].start()
    q_out[pl.ds(place.me * heads, heads)] = q_send[:, aligned(place.me, local_rows), :]
    return outgoing


def first_kernel(count, x, wq, wk, wv, k_cache, v_cache,
                 q_out, kv_new, residual, k_vmem, v_vmem,
                 hidden, wq_buf, wkv_buf, q_acc, q_send,
                 x_sems, w_sems, cache_sems, q_ssem, q_rsem):
    place = Place(count)
    pieces, rows, depth = hidden.shape
    x_copies = [
        pltpu.make_async_copy(x.at[:, pl.ds(i * depth, depth)], hidden.at[i], x_sems.at[i]) for i in range(pieces)
    ]
    w_copies = weight_copies(0, wq, wk, wv, wq_buf, wkv_buf, w_sems)
    cache_copies = cache_loads(0, k_cache, v_cache, k_vmem, v_vmem, cache_sems)
    for i in range(pieces):
        x_copies[i].start()
        w_copies[i].start()
    signal_all(place)
    w_copies[pieces].start()
    w_copies[pieces + 1].start()
    for copy in cache_copies:
        copy.start()
    for i in range(pieces):
        x_copies[i].wait()
        w_copies[i].wait()
        add_query(i, i == 0, hidden, wq_buf, q_acc)
    wait_all(place)
    outgoing = exchange_query(place, q_acc, q_send, q_out, q_ssem, q_rsem)
    chip_rows = residual.shape[1]
    for j in range(CHUNKS):
        residual[j] = hidden[place.half * CHUNKS + j, aligned(place.chip, chip_rows), :]
    w_copies[pieces].wait()
    w_copies[pieces + 1].wait()
    new_rows(place, hidden, wkv_buf, kv_new)
    for copy in query_copies(place, q_send, q_out, q_ssem, q_rsem, True):
        copy.wait_recv()
    for copy in outgoing:
        copy.wait_send()
    for copy in cache_copies:
        copy.wait()


def mix_kernel(count, last, layer, *refs):
    refs = list(refs)
    take = lambda k: [refs.pop(0) for _ in range(k)]
    context, residual, wo = take(3)
    if not last:
        wq, wk, wv, k_cache, v_cache = take(5)
        q_out, kv_new, next_residual, k_vmem, v_vmem = take(5)
    else:
        (hidden,) = take(1)
    c_recv, wo_far, wo_own, p_send, p_recv, total, s1_recv, comb, s2_left, s2_right = take(10)
    wo_sems, c_ssem, c_rsem, p_ssem, p_rsem, s1_ssem, s1_rsem = take(7)
    s2_ssem, s2_rsem, ag_ssem, ag_rsem, d2d_ssem, d2d_rsem = take(6)
    if not last:
        hidden, wq_buf, wkv_buf, q_acc, q_send, w_sems, cache_sems, q_ssem, q_rsem = take(9)
    place = Place(count)
    heads, rows, head_dim = c_recv.shape
    local_rows = rows // count
    chip_rows = rows // CHIPS
    depth = total.shape[-1]

    signal_all(place)
    wo_copies = []
    for j in range(CHUNKS):
        wo_copies.append(pltpu.make_async_copy(
            wo.at[layer, :, aligned((1 - place.half) * CHUNKS + j, depth)], wo_far.at[j], wo_sems.at[j]))
    for j in range(CHUNKS):
        wo_copies.append(pltpu.make_async_copy(
            wo.at[layer, :, aligned(place.half * CHUNKS + j, depth)], wo_own.at[j], wo_sems.at[CHUNKS + j]))
    for copy in wo_copies:
        copy.start()
    if not last:
        w_copies = weight_copies(layer + 1, wq, wk, wv, wq_buf, wkv_buf, w_sems)
        cache_copies = cache_loads(layer + 1, k_cache, v_cache, k_vmem, v_vmem, cache_sems)
        for copy in w_copies + cache_copies:
            copy.start()

    c_recv[:, aligned(place.me, local_rows), :] = context[pl.ds(place.me * heads, heads)]
    wait_all(place)

    def context_copy(offset, source):
        target = place.peer(offset)
        return remote(
            context.at[pl.ds(target * heads, heads)], c_recv.at[:, aligned(source, local_rows), :],
            c_ssem.at[offset], c_rsem.at[offset], target)

    sends = []

    def send(copy):
        copy.start()
        sends.append(copy)

    for offset in send_order(count):
        send(context_copy(offset, place.me))
    for offset in range(1, count):
        context_copy(offset, place.origin(offset)).wait_recv()

    def product(weights):
        acc = None
        for pair in range(heads // 2):
            lhs = jnp.concatenate([c_recv[2 * pair], c_recv[2 * pair + 1]], axis=1)
            part = jnp.dot(lhs, weights[pl.ds(pair * 2 * head_dim, 2 * head_dim), :], preferred_element_type=F32)
            acc = part if acc is None else acc + part
        return acc

    def pair_copy(j):
        return remote(p_send.at[j], p_recv.at[j], p_ssem.at[j], p_rsem.at[j], place.sibling)

    def block(chip):
        return aligned(chip, chip_rows)

    for j in range(CHUNKS):
        wo_copies[j].wait()
        p_send[j] = product(wo_far.at[j])
        send(pair_copy(j))

    def step_one(j):
        target = place.to_right if j % 2 == 0 else place.to_left
        if j >= RELAYED:
            target = place.across * 2 + place.core
        return remote(total.at[j, block(place.across), :], s1_recv.at[j], s1_ssem.at[j], s1_rsem.at[j], target)

    def step_two(j, rightward, source):
        target = place.to_right if rightward else place.to_left
        inbox = s2_left if rightward else s2_right
        slot = j if rightward else CHUNKS + j
        return remote(source, inbox.at[j], s2_ssem.at[slot], s2_rsem.at[slot], target)

    def direct(j):
        for rightward in (j % 2 == 1, j % 2 == 0) if j >= RELAYED else (j % 2 == 1,):
            send(step_two(j, rightward, total.at[j, block(place.right if rightward else place.left), :]))

    def combine(j):
        step_one(j).wait_recv()
        rightward = j % 2 == 0
        comb[j] = total[j, block(place.right if rightward else place.left), :] + s1_recv[j]
        send(step_two(j, rightward, comb.at[j]))

    for j in range(CHUNKS):
        wo_copies[CHUNKS + j].wait()
        total[j] = product(wo_own.at[j])
    pending = []
    for j in range(CHUNKS):
        pair_copy(j).wait_recv()
        total[j] += p_recv[j]
        send(step_one(j))
        while pending:
            direct(pending.pop())
        if 0 < j < RELAYED:
            pending.append(j)
        else:
            direct(j)
    for j in range(min(RELAYED, 2)):
        combine(j)
    while pending:
        direct(pending.pop())
    for j in range(2, RELAYED):
        combine(j)

    def piece(half, j):
        return half * CHUNKS + j

    def region(half, j, chip):
        if last:
            return hidden.at[block(chip), aligned(piece(half, j), depth)]
        return hidden.at[piece(half, j), block(chip), :]

    def gather_copy(j, way, chip):
        target = (place.to_right, place.to_left, place.across * 2 + place.core)[way]
        part = region(place.half, j, chip)
        slot = way * CHUNKS + j
        return remote(part, part, ag_ssem.at[slot], ag_rsem.at[slot], target)

    def forward_copy(j, chip):
        target = place.to_right if j % 2 == 0 else place.to_left
        part = region(place.half, j, chip)
        return remote(part, part, ag_ssem.at[2 * CHUNKS + j], ag_rsem.at[2 * CHUNKS + j], target)

    def twin_copy(j, half):
        part = hidden.at[:, aligned(piece(half, j), depth)] if last else hidden.at[piece(half, j)]
        return remote(part, part, d2d_ssem.at[j], d2d_rsem.at[j], place.sibling)

    def finish(j):
        step_two(j, True, comb.at[j]).wait_recv()
        step_two(j, False, comb.at[j]).wait_recv()
        summed = total[j, block(place.chip), :] + s2_left[j] + s2_right[j]
        if j >= RELAYED:
            step_one(j).wait_recv()
            summed = summed + s1_recv[j]
        value = (residual[j].astype(F32) + summed).astype(BF16)
        if last:
            hidden[block(place.chip), aligned(piece(place.half, j), depth)] = value
        else:
            hidden[piece(place.half, j), block(place.chip), :] = value
            next_residual[j] = value
        if j >= RING:
            send(gather_copy(j, 2, place.chip))
        send(gather_copy(j, 0, place.chip))
        send(gather_copy(j, 1, place.chip))

    def pass_on(j):
        gather_copy(j, 0, place.left).wait_recv()
        if j < RING and j % 2 == 0:
            send(forward_copy(j, place.left))
        gather_copy(j, 1, place.right).wait_recv()
        if j < RING and j % 2 == 1:
            send(forward_copy(j, place.right))

    def far_block(j):
        gather_copy(j, 2, place.across).wait_recv()
        send(twin_copy(j, place.half))

    for j in range(CHUNKS):
        finish(j)
    for j in range(RING):
        pass_on(j)
    order = list(range(RING, CHUNKS)) + list(range(RING))
    for j in order:
        if j >= RING:
            pass_on(j)
        far_block(j)
        if not last:
            for copy in w_copies if j == order[0] else ():
                copy.wait()
            add_query(piece(place.half, j), j == order[0], hidden, wq_buf, q_acc)
    for j in order:
        twin_copy(j, 1 - place.half).wait_recv()
        if not last:
            add_query(piece(1 - place.half, j), False, hidden, wq_buf, q_acc)
    if not last:
        outgoing = exchange_query(place, q_acc, q_send, q_out, q_ssem, q_rsem)
        new_rows(place, hidden, wkv_buf, kv_new)
        for copy in query_copies(place, q_send, q_out, q_ssem, q_rsem, True):
            copy.wait_recv()
        sends.extend(outgoing)
        for copy in cache_copies:
            copy.wait()
    for copy in sends:
        copy.wait_send()


GROUP = 8
SHORT = 256


def attention_kernel(layer, *refs):
    all_lens, q, kv_new, k_in, v_in = refs[:5]
    refs = refs[5:]
    if layer > 0:
        refs = refs[2:]
    k_out, v_out, k_buf, v_buf, context, q_rows, c_rows, sems = refs
    del k_in, v_in
    heads, local_rows, head_dim = q.shape
    seq_len = k_buf.shape[1]
    tile = 16
    first_row = lax.axis_index("model") * local_rows

    def length(b):
        return all_lens[first_row + b]

    writes = []
    parts = sems.shape[0] // 2
    step = local_rows // parts
    for i in range(parts):
        for b in range(i * step, (i + 1) * step):
            start = pl.multiple_of((length(b) // tile) * tile, tile)
            here = lax.broadcasted_iota(jnp.int32, (tile, head_dim), 0) == length(b) - start
            for buf, column in ((k_buf, 0), (v_buf, head_dim)):
                fresh = jnp.broadcast_to(kv_new[b:b + 1, column:column + head_dim], (tile, head_dim))
                old = buf[b, pl.ds(start, tile), :].astype(F32)
                buf[b, pl.ds(start, tile), :] = jnp.where(here, fresh, old).astype(BF16)
        part = pl.ds(i * step, step)
        writes.append(pltpu.make_async_copy(k_buf.at[part], k_out.at[layer, part], sems.at[2 * i]))
        writes.append(pltpu.make_async_copy(v_buf.at[part], v_out.at[layer, part], sems.at[2 * i + 1]))
        if i > 0:
            writes[2 * i - 2].start()
            writes[2 * i - 1].start()
    q_rows[...] = q[...].astype(F32).reshape(heads * local_rows, head_dim)
    writes[-2].start()
    writes[-1].start()

    def attend(members, span):
        rows = [pl.ds(b, heads, stride=local_rows) for b in members]
        scores = [
            lax.dot_general(
                q_rows[r, :].astype(BF16), k_buf[b, pl.ds(0, span), :], (((1,), (1,)), ((), ())),
                preferred_element_type=F32)
            for b, r in zip(members, rows)
        ]
        positions = lax.broadcasted_iota(jnp.int32, (heads, span), 1)
        scores = [jnp.where(positions <= length(b), s * (head_dim ** -0.5), -jnp.inf) for b, s in zip(members, scores)]
        tops = [jnp.max(s, axis=1, keepdims=True) for s in scores]
        powers = [jnp.exp(s - t) for s, t in zip(scores, tops)]
        sums = [jnp.sum(p, axis=1, keepdims=True) for p in powers]
        weights = [(p / t).astype(BF16) for p, t in zip(powers, sums)]
        outs = [
            jnp.dot(w, v_buf[b, pl.ds(0, span), :], preferred_element_type=F32) for b, w in zip(members, weights)
        ]
        for r, out in zip(rows, outs):
            c_rows[r, :] = out.astype(BF16).astype(F32)

    for first in range(0, local_rows, GROUP):
        attend(list(range(first, first + GROUP)), SHORT)

    spans = []
    span = 2 * SHORT
    while span < seq_len:
        spans.append(span)
        span *= 2
    spans.append(seq_len)

    def longer(b, _):
        @pl.when(length(b) >= SHORT)
        def _():
            low = SHORT
            for span in spans:
                @pl.when(jnp.logical_and(length(b) >= low, length(b) < span))
                def _(span=span):
                    attend([b], span)
                low = span
        return 0

    lax.fori_loop(0, local_rows, longer, 0)
    context[...] = c_rows[...].reshape(heads, local_rows, head_dim).astype(BF16)
    for copy in writes:
        copy.wait()


def solution(mesh):
    count = mesh.shape["model"]
    assert count == 2 * CHIPS
    row_axes = ("replica", "model")
    cache_spec = P(None, row_axes, None, None)
    DMA = pltpu.SemaphoreType.DMA

    def device_step(x, cache_len, w_query, w_key, w_value, w_out, k_cache, v_cache):
        rows, width = x.shape
        layers, local_rows, seq_len, head_dim = k_cache.shape
        local_width = w_query.shape[-1]
        local_heads = local_width // head_dim
        heads = local_heads * count
        pieces = 2 * CHUNKS
        depth = width // pieces
        chip_rows = rows // CHIPS
        w_query, w_key, w_value, w_out = map(to_hbm, (w_query, w_key, w_value, w_out))
        x, k_cache, v_cache = map(to_hbm, (x, k_cache, v_cache))

        project_out = (
            pltpu.VMEM((heads, local_rows, head_dim), BF16),
            pltpu.VMEM((local_rows, 2 * head_dim), F32),
            pltpu.VMEM((CHUNKS, chip_rows, depth), BF16),
            pltpu.VMEM(k_cache.shape[1:], BF16),
            pltpu.VMEM(v_cache.shape[1:], BF16),
        )
        project_scratch = [
            pltpu.VMEM((pieces, rows, depth), BF16),
            pltpu.VMEM((width, local_width), BF16),
            pltpu.VMEM((width, 2 * head_dim), BF16),
            pltpu.VMEM((rows, local_width), F32),
            pltpu.VMEM((local_heads, rows, head_dim), BF16),
        ]
        project_sems = [DMA((pieces + 2,)), DMA((2 * PARTS,)), DMA((count,)), DMA((count,))]
        mix_scratch = [
            pltpu.VMEM((local_heads, rows, head_dim), BF16),
            pltpu.VMEM((CHUNKS, local_width, depth), BF16),
            pltpu.VMEM((CHUNKS, local_width, depth), BF16),
            pltpu.VMEM((CHUNKS, rows, depth), F32),
            pltpu.VMEM((CHUNKS, rows, depth), F32),
            pltpu.VMEM((CHUNKS, rows, depth), F32),
            pltpu.VMEM((CHUNKS, chip_rows, depth), F32),
            pltpu.VMEM((CHUNKS, chip_rows, depth), F32),
            pltpu.VMEM((CHUNKS, chip_rows, depth), F32),
            pltpu.VMEM((CHUNKS, chip_rows, depth), F32),
            DMA((pieces,)), DMA((count,)), DMA((count,)), DMA((CHUNKS,)), DMA((CHUNKS,)), DMA((CHUNKS,)), DMA((CHUNKS,)),
            DMA((2 * CHUNKS,)), DMA((2 * CHUNKS,)), DMA((3 * CHUNKS,)), DMA((3 * CHUNKS,)),
            DMA((CHUNKS,)), DMA((CHUNKS,)),
        ]

        def params(collective_id, limit):
            return pltpu.CompilerParams(collective_id=collective_id, has_side_effects=True, vmem_limit_bytes=limit * MIB)

        query, kv_new, residual, k_vmem, v_vmem = pl.pallas_call(
            functools.partial(first_kernel, count),
            out_shape=project_out,
            in_specs=[ANY_SPEC] * 6,
            out_specs=(VMEM_SPEC,) * 5,
            scratch_shapes=project_scratch + [DMA((pieces,))] + project_sems,
            compiler_params=params(0, 16),
            name="first",
        )(x, w_query, w_key, w_value, k_cache, v_cache)

        k_new_cache = v_new_cache = None
        for layer in range(layers):
            last = layer == layers - 1
            operands = [cache_len, query, kv_new, k_vmem, v_vmem]
            specs = [SMEM_SPEC] + [VMEM_SPEC] * 4
            aliases = {3: 2, 4: 3}
            if layer > 0:
                operands += [k_new_cache, v_new_cache]
                specs += [ANY_SPEC] * 2
                aliases |= {5: 0, 6: 1}
            k_new_cache, v_new_cache, _, _, context = pl.pallas_call(
                functools.partial(attention_kernel, layer),
                out_shape=(
                    pltpu.HBM(k_cache.shape, BF16),
                    pltpu.HBM(v_cache.shape, BF16),
                    pltpu.VMEM(k_cache.shape[1:], BF16),
                    pltpu.VMEM(v_cache.shape[1:], BF16),
                    pltpu.VMEM((heads, local_rows, head_dim), BF16),
                ),
                in_specs=specs,
                out_specs=(ANY_SPEC, ANY_SPEC, VMEM_SPEC, VMEM_SPEC, VMEM_SPEC),
                input_output_aliases=aliases,
                scratch_shapes=[
                    pltpu.VMEM((heads * local_rows, head_dim), F32),
                    pltpu.VMEM((heads * local_rows, head_dim), F32),
                    DMA((2 * PARTS,)),
                ],
                compiler_params=pltpu.CompilerParams(vmem_limit_bytes=16 * MIB),
                name=f"attend{layer}",
            )(*operands)
            if not last:
                query, kv_new, residual, k_vmem, v_vmem = pl.pallas_call(
                    functools.partial(mix_kernel, count, False, layer),
                    out_shape=project_out,
                    in_specs=[VMEM_SPEC] * 2 + [ANY_SPEC] * 6,
                    out_specs=(VMEM_SPEC,) * 5,
                    scratch_shapes=mix_scratch + project_scratch + project_sems,
                    compiler_params=params(1 + layer, 28),
                    name=f"mix{layer}",
                )(context, residual, w_out, w_query, w_key, w_value, k_cache, v_cache)
            else:
                hidden = pl.pallas_call(
                    functools.partial(mix_kernel, count, True, layer),
                    out_shape=pltpu.VMEM((rows, width), BF16),
                    in_specs=[VMEM_SPEC] * 2 + [ANY_SPEC],
                    out_specs=VMEM_SPEC,
                    scratch_shapes=mix_scratch,
                    compiler_params=params(1 + layer, 20),
                    name=f"mix{layer}",
                )(context, residual, w_out)
        return hidden, k_new_cache, v_new_cache

    return jax.shard_map(
        device_step,
        mesh=mesh,
        in_specs=(P("replica", None), P("replica"), P(None, None, "model"), P(), P(), P(None, "model", None), cache_spec, cache_spec),
        out_specs=(P("replica", None), cache_spec, cache_spec),
        check_vma=False,
    )
```

```python
import functools

import jax
import jax.numpy as jnp
from jax import lax
from jax.experimental import pallas as pl
from jax.experimental.pallas import tpu as pltpu
from jax.sharding import PartitionSpec as P

MESH = pl.DeviceIdType.MESH
F32 = jnp.float32
BF16 = jnp.bfloat16
CHIPS = 4
CHUNKS = 4
PARTS = 8
RING = 0
RELAYED = 4
MIB = 1 << 20

ANY_SPEC = pl.BlockSpec(memory_space=pltpu.HBM)
VMEM_SPEC = pl.BlockSpec(memory_space=pltpu.VMEM)
SMEM_SPEC = pl.BlockSpec(memory_space=pltpu.SMEM)


def to_hbm(value):
    return pltpu.with_memory_space_constraint(value, pltpu.HBM)


def to_vmem(value):
    return pltpu.with_memory_space_constraint(value, pltpu.VMEM)


def aligned(index, size):
    return pl.ds(pl.multiple_of(index * size, size), size)


class Place:
    def __init__(self, count):
        self.count = count
        self.me = lax.axis_index("model")
        self.chip = self.me // 2
        self.core = self.me % 2
        self.right = (self.chip + 1) % CHIPS
        self.left = (self.chip + CHIPS - 1) % CHIPS
        self.across = (self.chip + 2) % CHIPS
        self.half = (self.core + self.chip) % 2
        self.to_right = self.right * 2 + 1 - self.core
        self.to_left = self.left * 2 + 1 - self.core
        self.sibling = self.chip * 2 + (1 - self.core)

    def peer(self, offset):
        return (self.me + offset) % self.count

    def origin(self, offset):
        return (self.me + self.count - offset) % self.count


def remote(src, dst, send_sem, recv_sem, device):
    return pltpu.make_async_remote_copy(
        src_ref=src, dst_ref=dst, send_sem=send_sem, recv_sem=recv_sem,
        device_id={"model": device}, device_id_type=MESH)


def signal_all(place):
    barrier = pltpu.get_barrier_semaphore()
    for offset in send_order(place.count):
        pl.semaphore_signal(barrier, inc=1, device_id={"model": place.peer(offset)}, device_id_type=MESH)


def wait_all(place):
    pl.semaphore_wait(pltpu.get_barrier_semaphore(), place.count - 1)


def weight_copies(layer, wq, wk, wv, wq_buf, wkv_buf, sems):
    pieces = sems.shape[0] - 2
    depth = wq_buf.shape[0] // pieces
    head_dim = wk.shape[-1]
    copies = [
        pltpu.make_async_copy(wq.at[layer, pl.ds(i * depth, depth), :], wq_buf.at[pl.ds(i * depth, depth), :], sems.at[i])
        for i in range(pieces)
    ]
    copies.append(pltpu.make_async_copy(wk.at[layer], wkv_buf.at[:, pl.ds(0, head_dim)], sems.at[pieces]))
    copies.append(pltpu.make_async_copy(wv.at[layer], wkv_buf.at[:, pl.ds(head_dim, head_dim)], sems.at[pieces + 1]))
    return copies


def cache_loads(layer, k_cache, v_cache, k_vmem, v_vmem, sems):
    parts = sems.shape[0] // 2
    step = k_vmem.shape[0] // parts
    copies = []
    for i in range(parts):
        part = pl.ds(i * step, step)
        copies.append(pltpu.make_async_copy(k_cache.at[layer, part], k_vmem.at[part], sems.at[2 * i]))
        copies.append(pltpu.make_async_copy(v_cache.at[layer, part], v_vmem.at[part], sems.at[2 * i + 1]))
    return copies


def add_query(piece, first, hidden, wq_buf, q_acc):
    depth = hidden.shape[-1]
    part = jnp.dot(hidden[piece], wq_buf[aligned(piece, depth), :], preferred_element_type=F32)
    q_acc[...] = part if first else q_acc[...] + part


def new_rows(place, hidden, wkv_buf, kv_new):
    pieces, rows, depth = hidden.shape
    local_rows = rows // place.count
    total = None
    for piece in range(pieces):
        mine = hidden[piece, aligned(place.me, local_rows), :]
        part = jnp.dot(mine, wkv_buf[pl.ds(piece * depth, depth), :], preferred_element_type=F32)
        total = part if total is None else total + part
    kv_new[...] = total.astype(BF16).astype(F32)


def query_copies(place, q_send, q_out, send_sems, recv_sems, incoming):
    heads = q_send.shape[0]
    local_rows = q_out.shape[1]
    copies = []
    for offset in range(1, place.count):
        source = place.origin(offset) if incoming else place.me
        target = place.peer(offset)
        copies.append(remote(
            q_send.at[:, aligned(target, local_rows), :], q_out.at[pl.ds(source * heads, heads)],
            send_sems.at[offset], recv_sems.at[offset], target))
    return copies


def send_order(count):
    return sorted(range(1, count), key=lambda offset: -min(offset, count - offset))


def exchange_query(place, q_acc, q_send, q_out, send_sems, recv_sems):
    heads, rows, head_dim = q_send.shape
    local_rows = q_out.shape[1]
    for head in range(heads):
        q_send[head] = q_acc[:, head * head_dim:(head + 1) * head_dim].astype(BF16)
    outgoing = query_copies(place, q_send, q_out, send_sems, recv_sems, False)
    for offset in send_order(place.count):
        outgoing[offset - 1].start()
    q_out[pl.ds(place.me * heads, heads)] = q_send[:, aligned(place.me, local_rows), :]
    return outgoing


def first_kernel(count, x, wq, wk, wv, k_cache, v_cache,
                 q_out, kv_new, residual, k_vmem, v_vmem,
                 hidden, wq_buf, wkv_buf, q_acc, q_send,
                 x_sems, w_sems, cache_sems, q_ssem, q_rsem):
    place = Place(count)
    pieces, rows, depth = hidden.shape
    x_copies = [
        pltpu.make_async_copy(x.at[:, pl.ds(i * depth, depth)], hidden.at[i], x_sems.at[i]) for i in range(pieces)
    ]
    w_copies = weight_copies(0, wq, wk, wv, wq_buf, wkv_buf, w_sems)
    cache_copies = cache_loads(0, k_cache, v_cache, k_vmem, v_vmem, cache_sems)
    for i in range(pieces):
        x_copies[i].start()
        w_copies[i].start()
    signal_all(place)
    w_copies[pieces].start()
    w_copies[pieces + 1].start()
    for copy in cache_copies:
        copy.start()
    for i in range(pieces):
        x_copies[i].wait()
        w_copies[i].wait()
        add_query(i, i == 0, hidden, wq_buf, q_acc)
    wait_all(place)
    outgoing = exchange_query(place, q_acc, q_send, q_out, q_ssem, q_rsem)
    chip_rows = residual.shape[1]
    for j in range(CHUNKS):
        residual[j] = hidden[place.half * CHUNKS + j, aligned(place.chip, chip_rows), :]
    w_copies[pieces].wait()
    w_copies[pieces + 1].wait()
    new_rows(place, hidden, wkv_buf, kv_new)
    for copy in query_copies(place, q_send, q_out, q_ssem, q_rsem, True):
        copy.wait_recv()
    for copy in outgoing:
        copy.wait_send()
    for copy in cache_copies:
        copy.wait()


def mix_kernel(count, last, layer, *refs):
    refs = list(refs)
    take = lambda k: [refs.pop(0) for _ in range(k)]
    context, residual, wo = take(3)
    if not last:
        wq, wk, wv, k_cache, v_cache = take(5)
        q_out, kv_new, next_residual, k_vmem, v_vmem = take(5)
    else:
        (hidden,) = take(1)
    c_recv, wo_far, wo_own, p_send, p_recv, total, s1_recv, comb, s2_left, s2_right = take(10)
    wo_sems, c_ssem, c_rsem, p_ssem, p_rsem, s1_ssem, s1_rsem = take(7)
    s2_ssem, s2_rsem, ag_ssem, ag_rsem, d2d_ssem, d2d_rsem = take(6)
    if not last:
        hidden, wq_buf, wkv_buf, q_acc, q_send, w_sems, cache_sems, q_ssem, q_rsem = take(9)
    place = Place(count)
    heads, rows, head_dim = c_recv.shape
    local_rows = rows // count
    chip_rows = rows // CHIPS
    depth = total.shape[-1]

    signal_all(place)
    wo_copies = []
    for j in range(CHUNKS):
        wo_copies.append(pltpu.make_async_copy(
            wo.at[layer, :, aligned((1 - place.half) * CHUNKS + j, depth)], wo_far.at[j], wo_sems.at[j]))
    for j in range(CHUNKS):
        wo_copies.append(pltpu.make_async_copy(
            wo.at[layer, :, aligned(place.half * CHUNKS + j, depth)], wo_own.at[j], wo_sems.at[CHUNKS + j]))
    for copy in wo_copies:
        copy.start()
    if not last:
        w_copies = weight_copies(layer + 1, wq, wk, wv, wq_buf, wkv_buf, w_sems)
        cache_copies = cache_loads(layer + 1, k_cache, v_cache, k_vmem, v_vmem, cache_sems)
        for copy in w_copies + cache_copies:
            copy.start()

    c_recv[:, aligned(place.me, local_rows), :] = context[pl.ds(place.me * heads, heads)]
    wait_all(place)

    def context_copy(offset, source):
        target = place.peer(offset)
        return remote(
            context.at[pl.ds(target * heads, heads)], c_recv.at[:, aligned(source, local_rows), :],
            c_ssem.at[offset], c_rsem.at[offset], target)

    sends = []

    def send(copy):
        copy.start()
        sends.append(copy)

    for offset in send_order(count):
        send(context_copy(offset, place.me))
    for offset in range(1, count):
        context_copy(offset, place.origin(offset)).wait_recv()

    def product(weights):
        acc = None
        for pair in range(heads // 2):
            lhs = jnp.concatenate([c_recv[2 * pair], c_recv[2 * pair + 1]], axis=1)
            part = jnp.dot(lhs, weights[pl.ds(pair * 2 * head_dim, 2 * head_dim), :], preferred_element_type=F32)
            acc = part if acc is None else acc + part
        return acc

    def pair_copy(j):
        return remote(p_send.at[j], p_recv.at[j], p_ssem.at[j], p_rsem.at[j], place.sibling)

    def block(chip):
        return aligned(chip, chip_rows)

    for j in range(CHUNKS):
        wo_copies[j].wait()
        p_send[j] = product(wo_far.at[j])
        send(pair_copy(j))

    def step_one(j):
        target = place.to_right if j % 2 == 0 else place.to_left
        if j >= RELAYED:
            target = place.across * 2 + place.core
        return remote(total.at[j, block(place.across), :], s1_recv.at[j], s1_ssem.at[j], s1_rsem.at[j], target)

    def step_two(j, rightward, source):
        target = place.to_right if rightward else place.to_left
        inbox = s2_left if rightward else s2_right
        slot = j if rightward else CHUNKS + j
        return remote(source, inbox.at[j], s2_ssem.at[slot], s2_rsem.at[slot], target)

    def direct(j):
        for rightward in (j % 2 == 1, j % 2 == 0) if j >= RELAYED else (j % 2 == 1,):
            send(step_two(j, rightward, total.at[j, block(place.right if rightward else place.left), :]))

    def combine(j):
        step_one(j).wait_recv()
        rightward = j % 2 == 0
        comb[j] = total[j, block(place.right if rightward else place.left), :] + s1_recv[j]
        send(step_two(j, rightward, comb.at[j]))

    for j in range(CHUNKS):
        wo_copies[CHUNKS + j].wait()
        total[j] = product(wo_own.at[j])
    pending = []
    for j in range(CHUNKS):
        pair_copy(j).wait_recv()
        total[j] += p_recv[j]
        send(step_one(j))
        while pending:
            direct(pending.pop())
        if 0 < j < RELAYED:
            pending.append(j)
        else:
            direct(j)
    for j in range(min(RELAYED, 2)):
        combine(j)
    while pending:
        direct(pending.pop())
    for j in range(2, RELAYED):
        combine(j)

    def piece(half, j):
        return half * CHUNKS + j

    def region(half, j, chip):
        if last:
            return hidden.at[block(chip), aligned(piece(half, j), depth)]
        return hidden.at[piece(half, j), block(chip), :]

    def gather_copy(j, way, chip):
        target = (place.to_right, place.to_left, place.across * 2 + place.core)[way]
        part = region(place.half, j, chip)
        slot = way * CHUNKS + j
        return remote(part, part, ag_ssem.at[slot], ag_rsem.at[slot], target)

    def forward_copy(j, chip):
        target = place.to_right if j % 2 == 0 else place.to_left
        part = region(place.half, j, chip)
        return remote(part, part, ag_ssem.at[2 * CHUNKS + j], ag_rsem.at[2 * CHUNKS + j], target)

    def twin_copy(j, half):
        part = hidden.at[:, aligned(piece(half, j), depth)] if last else hidden.at[piece(half, j)]
        return remote(part, part, d2d_ssem.at[j], d2d_rsem.at[j], place.sibling)

    def finish(j):
        step_two(j, True, comb.at[j]).wait_recv()
        step_two(j, False, comb.at[j]).wait_recv()
        summed = total[j, block(place.chip), :] + s2_left[j] + s2_right[j]
        if j >= RELAYED:
            step_one(j).wait_recv()
            summed = summed + s1_recv[j]
        value = (residual[j].astype(F32) + summed).astype(BF16)
        if last:
            hidden[block(place.chip), aligned(piece(place.half, j), depth)] = value
        else:
            hidden[piece(place.half, j), block(place.chip), :] = value
            next_residual[j] = value
        if j >= RING:
            send(gather_copy(j, 2, place.chip))
        send(gather_copy(j, 0, place.chip))
        send(gather_copy(j, 1, place.chip))

    def pass_on(j):
        gather_copy(j, 0, place.left).wait_recv()
        if j < RING and j % 2 == 0:
            send(forward_copy(j, place.left))
        gather_copy(j, 1, place.right).wait_recv()
        if j < RING and j % 2 == 1:
            send(forward_copy(j, place.right))

    def far_block(j):
        gather_copy(j, 2, place.across).wait_recv()
        send(twin_copy(j, place.half))

    for j in range(CHUNKS):
        finish(j)
    for j in range(RING):
        pass_on(j)
    order = list(range(RING, CHUNKS)) + list(range(RING))
    for j in order:
        if j >= RING:
            pass_on(j)
        far_block(j)
        if not last:
            for copy in w_copies if j == order[0] else ():
                copy.wait()
            add_query(piece(place.half, j), j == order[0], hidden, wq_buf, q_acc)
    for j in order:
        twin_copy(j, 1 - place.half).wait_recv()
        if not last:
            add_query(piece(1 - place.half, j), False, hidden, wq_buf, q_acc)
    if not last:
        outgoing = exchange_query(place, q_acc, q_send, q_out, q_ssem, q_rsem)
        new_rows(place, hidden, wkv_buf, kv_new)
        for copy in query_copies(place, q_send, q_out, q_ssem, q_rsem, True):
            copy.wait_recv()
        sends.extend(outgoing)
        for copy in cache_copies:
            copy.wait()
    for copy in sends:
        copy.wait_send()


GROUP = 8
SHORT = 256


def attention_kernel(layer, *refs):
    all_lens, q, kv_new, k_in, v_in = refs[:5]
    refs = refs[5:]
    if layer > 0:
        refs = refs[2:]
    k_out, v_out, k_buf, v_buf, context, q_rows, c_rows, sems = refs
    del k_in, v_in
    heads, local_rows, head_dim = q.shape
    seq_len = k_buf.shape[1]
    tile = 16
    first_row = lax.axis_index("model") * local_rows

    def length(b):
        return all_lens[first_row + b]

    writes = []
    parts = sems.shape[0] // 2
    step = local_rows // parts
    for i in range(parts):
        for b in range(i * step, (i + 1) * step):
            start = pl.multiple_of((length(b) // tile) * tile, tile)
            here = lax.broadcasted_iota(jnp.int32, (tile, head_dim), 0) == length(b) - start
            for buf, column in ((k_buf, 0), (v_buf, head_dim)):
                fresh = jnp.broadcast_to(kv_new[b:b + 1, column:column + head_dim], (tile, head_dim))
                old = buf[b, pl.ds(start, tile), :].astype(F32)
                buf[b, pl.ds(start, tile), :] = jnp.where(here, fresh, old).astype(BF16)
        part = pl.ds(i * step, step)
        writes.append(pltpu.make_async_copy(k_buf.at[part], k_out.at[layer, part], sems.at[2 * i]))
        writes.append(pltpu.make_async_copy(v_buf.at[part], v_out.at[layer, part], sems.at[2 * i + 1]))
        if i > 0:
            writes[2 * i - 2].start()
            writes[2 * i - 1].start()
    q_rows[...] = q[...].astype(F32).reshape(heads * local_rows, head_dim)
    writes[-2].start()
    writes[-1].start()

    def attend(members, span):
        rows = [pl.ds(b, heads, stride=local_rows) for b in members]
        scores = [
            lax.dot_general(
                q_rows[r, :].astype(BF16), k_buf[b, pl.ds(0, span), :], (((1,), (1,)), ((), ())),
                preferred_element_type=F32)
            for b, r in zip(members, rows)
        ]
        positions = lax.broadcasted_iota(jnp.int32, (heads, span), 1)
        scores = [jnp.where(positions <= length(b), s * (head_dim ** -0.5), -jnp.inf) for b, s in zip(members, scores)]
        tops = [jnp.max(s, axis=1, keepdims=True) for s in scores]
        powers = [jnp.exp(s - t) for s, t in zip(scores, tops)]
        sums = [jnp.sum(p, axis=1, keepdims=True) for p in powers]
        weights = [(p / t).astype(BF16) for p, t in zip(powers, sums)]
        outs = [
            jnp.dot(w, v_buf[b, pl.ds(0, span), :], preferred_element_type=F32) for b, w in zip(members, weights)
        ]
        for r, out in zip(rows, outs):
            c_rows[r, :] = out.astype(BF16).astype(F32)

    for first in range(0, local_rows, GROUP):
        attend(list(range(first, first + GROUP)), SHORT)

    spans = []
    span = 2 * SHORT
    while span < seq_len:
        spans.append(span)
        span *= 2
    spans.append(seq_len)

    def longer(b, _):
        @pl.when(length(b) >= SHORT)
        def _():
            low = SHORT
            for span in spans:
                @pl.when(jnp.logical_and(length(b) >= low, length(b) < span))
                def _(span=span):
                    attend([b], span)
                low = span
        return 0

    lax.fori_loop(0, local_rows, longer, 0)
    context[...] = c_rows[...].reshape(heads, local_rows, head_dim).astype(BF16)
    for copy in writes:
        copy.wait()


def solution(mesh):
    count = mesh.shape["model"]
    assert count == 2 * CHIPS
    row_axes = ("replica", "model")
    cache_spec = P(None, row_axes, None, None)
    DMA = pltpu.SemaphoreType.DMA

    def device_step(x, cache_len, w_query, w_key, w_value, w_out, k_cache, v_cache):
        rows, width = x.shape
        layers, local_rows, seq_len, head_dim = k_cache.shape
        local_width = w_query.shape[-1]
        local_heads = local_width // head_dim
        heads = local_heads * count
        pieces = 2 * CHUNKS
        depth = width // pieces
        chip_rows = rows // CHIPS
        w_query, w_key, w_value, w_out = map(to_hbm, (w_query, w_key, w_value, w_out))
        x, k_cache, v_cache = map(to_hbm, (x, k_cache, v_cache))

        project_out = (
            pltpu.VMEM((heads, local_rows, head_dim), BF16),
            pltpu.VMEM((local_rows, 2 * head_dim), F32),
            pltpu.VMEM((CHUNKS, chip_rows, depth), BF16),
            pltpu.VMEM(k_cache.shape[1:], BF16),
            pltpu.VMEM(v_cache.shape[1:], BF16),
        )
        project_scratch = [
            pltpu.VMEM((pieces, rows, depth), BF16),
            pltpu.VMEM((width, local_width), BF16),
            pltpu.VMEM((width, 2 * head_dim), BF16),
            pltpu.VMEM((rows, local_width), F32),
            pltpu.VMEM((local_heads, rows, head_dim), BF16),
        ]
        project_sems = [DMA((pieces + 2,)), DMA((2 * PARTS,)), DMA((count,)), DMA((count,))]
        mix_scratch = [
            pltpu.VMEM((local_heads, rows, head_dim), BF16),
            pltpu.VMEM((CHUNKS, local_width, depth), BF16),
            pltpu.VMEM((CHUNKS, local_width, depth), BF16),
            pltpu.VMEM((CHUNKS, rows, depth), F32),
            pltpu.VMEM((CHUNKS, rows, depth), F32),
            pltpu.VMEM((CHUNKS, rows, depth), F32),
            pltpu.VMEM((CHUNKS, chip_rows, depth), F32),
            pltpu.VMEM((CHUNKS, chip_rows, depth), F32),
            pltpu.VMEM((CHUNKS, chip_rows, depth), F32),
            pltpu.VMEM((CHUNKS, chip_rows, depth), F32),
            DMA((pieces,)), DMA((count,)), DMA((count,)), DMA((CHUNKS,)), DMA((CHUNKS,)), DMA((CHUNKS,)), DMA((CHUNKS,)),
            DMA((2 * CHUNKS,)), DMA((2 * CHUNKS,)), DMA((3 * CHUNKS,)), DMA((3 * CHUNKS,)),
            DMA((CHUNKS,)), DMA((CHUNKS,)),
        ]

        def params(collective_id, limit):
            return pltpu.CompilerParams(collective_id=collective_id, has_side_effects=True, vmem_limit_bytes=limit * MIB)

        query, kv_new, residual, k_vmem, v_vmem = pl.pallas_call(
            functools.partial(first_kernel, count),
            out_shape=project_out,
            in_specs=[ANY_SPEC] * 6,
            out_specs=(VMEM_SPEC,) * 5,
            scratch_shapes=project_scratch + [DMA((pieces,))] + project_sems,
            compiler_params=params(0, 16),
            name="first",
        )(x, w_query, w_key, w_value, k_cache, v_cache)

        k_new_cache = v_new_cache = None
        for layer in range(layers):
            last = layer == layers - 1
            operands = [cache_len, query, kv_new, k_vmem, v_vmem]
            specs = [SMEM_SPEC] + [VMEM_SPEC] * 4
            aliases = {3: 2, 4: 3}
            if layer > 0:
                operands += [k_new_cache, v_new_cache]
                specs += [ANY_SPEC] * 2
                aliases |= {5: 0, 6: 1}
            k_new_cache, v_new_cache, _, _, context = pl.pallas_call(
                functools.partial(attention_kernel, layer),
                out_shape=(
                    pltpu.HBM(k_cache.shape, BF16),
                    pltpu.HBM(v_cache.shape, BF16),
                    pltpu.VMEM(k_cache.shape[1:], BF16),
                    pltpu.VMEM(v_cache.shape[1:], BF16),
                    pltpu.VMEM((heads, local_rows, head_dim), BF16),
                ),
                in_specs=specs,
                out_specs=(ANY_SPEC, ANY_SPEC, VMEM_SPEC, VMEM_SPEC, VMEM_SPEC),
                input_output_aliases=aliases,
                scratch_shapes=[
                    pltpu.VMEM((heads * local_rows, head_dim), F32),
                    pltpu.VMEM((heads * local_rows, head_dim), F32),
                    DMA((2 * PARTS,)),
                ],
                compiler_params=pltpu.CompilerParams(vmem_limit_bytes=16 * MIB),
                name=f"attend{layer}",
            )(*operands)
            if not last:
                query, kv_new, residual, k_vmem, v_vmem = pl.pallas_call(
                    functools.partial(mix_kernel, count, False, layer),
                    out_shape=project_out,
                    in_specs=[VMEM_SPEC] * 2 + [ANY_SPEC] * 6,
                    out_specs=(VMEM_SPEC,) * 5,
                    scratch_shapes=mix_scratch + project_scratch + project_sems,
                    compiler_params=params(1 + layer, 28),
                    name=f"mix{layer}",
                )(context, residual, w_out, w_query, w_key, w_value, k_cache, v_cache)
            else:
                hidden = pl.pallas_call(
                    functools.partial(mix_kernel, count, True, layer),
                    out_shape=pltpu.VMEM((rows, width), BF16),
                    in_specs=[VMEM_SPEC] * 2 + [ANY_SPEC],
                    out_specs=VMEM_SPEC,
                    scratch_shapes=mix_scratch,
                    compiler_params=params(1 + layer, 20),
                    name=f"mix{layer}",
                )(context, residual, w_out)
        return hidden, k_new_cache, v_new_cache

    return jax.shard_map(
        device_step,
        mesh=mesh,
        in_specs=(P("replica", None), P("replica"), P(None, None, "model"), P(), P(), P(None, "model", None), cache_spec, cache_spec),
        out_specs=(P("replica", None), cache_spec, cache_spec),
        check_vma=False,
    )
```

```python
import functools

import jax
import jax.numpy as jnp
from jax import lax
from jax.experimental import pallas as pl
from jax.experimental.pallas import tpu as pltpu
from jax.sharding import PartitionSpec as P

MESH = pl.DeviceIdType.MESH
F32 = jnp.float32
BF16 = jnp.bfloat16
CHIPS = 4
CHUNKS = 2
PARTS = 8
RING = 0
RELAYED = CHUNKS
MIB = 1 << 20

ANY_SPEC = pl.BlockSpec(memory_space=pltpu.HBM)
VMEM_SPEC = pl.BlockSpec(memory_space=pltpu.VMEM)
SMEM_SPEC = pl.BlockSpec(memory_space=pltpu.SMEM)


def to_hbm(value):
    return pltpu.with_memory_space_constraint(value, pltpu.HBM)


def to_vmem(value):
    return pltpu.with_memory_space_constraint(value, pltpu.VMEM)


def aligned(index, size):
    return pl.ds(pl.multiple_of(index * size, size), size)


class Place:
    def __init__(self, count):
        self.count = count
        self.me = lax.axis_index("model")
        self.chip = self.me // 2
        self.core = self.me % 2
        self.right = (self.chip + 1) % CHIPS
        self.left = (self.chip + CHIPS - 1) % CHIPS
        self.across = (self.chip + 2) % CHIPS
        self.half = (self.core + self.chip) % 2
        self.to_right = self.right * 2 + 1 - self.core
        self.to_left = self.left * 2 + 1 - self.core
        self.sibling = self.chip * 2 + (1 - self.core)

    def peer(self, offset):
        return (self.me + offset) % self.count

    def origin(self, offset):
        return (self.me + self.count - offset) % self.count


def remote(src, dst, send_sem, recv_sem, device):
    return pltpu.make_async_remote_copy(
        src_ref=src, dst_ref=dst, send_sem=send_sem, recv_sem=recv_sem,
        device_id={"model": device}, device_id_type=MESH)


def signal_all(place):
    barrier = pltpu.get_barrier_semaphore()
    for offset in send_order(place.count):
        pl.semaphore_signal(barrier, inc=1, device_id={"model": place.peer(offset)}, device_id_type=MESH)


def wait_all(place):
    pl.semaphore_wait(pltpu.get_barrier_semaphore(), place.count - 1)


def weight_copies(layer, wq, wk, wv, wq_buf, wkv_buf, sems):
    pieces = sems.shape[0] - 2
    depth = wq_buf.shape[0] // pieces
    head_dim = wk.shape[-1]
    copies = [
        pltpu.make_async_copy(wq.at[layer, pl.ds(i * depth, depth), :], wq_buf.at[pl.ds(i * depth, depth), :], sems.at[i])
        for i in range(pieces)
    ]
    copies.append(pltpu.make_async_copy(wk.at[layer], wkv_buf.at[:, pl.ds(0, head_dim)], sems.at[pieces]))
    copies.append(pltpu.make_async_copy(wv.at[layer], wkv_buf.at[:, pl.ds(head_dim, head_dim)], sems.at[pieces + 1]))
    return copies


def cache_loads(layer, k_cache, v_cache, k_vmem, v_vmem, sems):
    parts = sems.shape[0] // 2
    step = k_vmem.shape[0] // parts
    copies = []
    for i in range(parts):
        part = pl.ds(i * step, step)
        copies.append(pltpu.make_async_copy(k_cache.at[layer, part], k_vmem.at[part], sems.at[2 * i]))
        copies.append(pltpu.make_async_copy(v_cache.at[layer, part], v_vmem.at[part], sems.at[2 * i + 1]))
    return copies


def add_query(piece, first, hidden, wq_buf, q_acc):
    depth = hidden.shape[-1]
    part = jnp.dot(hidden[piece], wq_buf[aligned(piece, depth), :], preferred_element_type=F32)
    q_acc[...] = part if first else q_acc[...] + part


def new_rows(place, hidden, wkv_buf, kv_new):
    pieces, rows, depth = hidden.shape
    local_rows = rows // place.count
    total = None
    for piece in range(pieces):
        mine = hidden[piece, aligned(place.me, local_rows), :]
        part = jnp.dot(mine, wkv_buf[pl.ds(piece * depth, depth), :], preferred_element_type=F32)
        total = part if total is None else total + part
    kv_new[...] = total.astype(BF16).astype(F32)


def query_copies(place, q_send, q_out, send_sems, recv_sems, incoming):
    heads = q_send.shape[0]
    local_rows = q_out.shape[1]
    copies = []
    for offset in range(1, place.count):
        source = place.origin(offset) if incoming else place.me
        target = place.peer(offset)
        copies.append(remote(
            q_send.at[:, aligned(target, local_rows), :], q_out.at[pl.ds(source * heads, heads)],
            send_sems.at[offset], recv_sems.at[offset], target))
    return copies


def send_order(count):
    return sorted(range(1, count), key=lambda offset: -min(offset, count - offset))


def exchange_query(place, q_acc, q_send, q_out, send_sems, recv_sems):
    heads, rows, head_dim = q_send.shape
    local_rows = q_out.shape[1]
    for head in range(heads):
        q_send[head] = q_acc[:, head * head_dim:(head + 1) * head_dim].astype(BF16)
    outgoing = query_copies(place, q_send, q_out, send_sems, recv_sems, False)
    for offset in send_order(place.count):
        outgoing[offset - 1].start()
    q_out[pl.ds(place.me * heads, heads)] = q_send[:, aligned(place.me, local_rows), :]
    return outgoing


def first_kernel(count, x, wq, wk, wv, k_cache, v_cache,
                 q_out, kv_new, residual, k_vmem, v_vmem,
                 hidden, wq_buf, wkv_buf, q_acc, q_send,
                 x_sems, w_sems, cache_sems, q_ssem, q_rsem):
    place = Place(count)
    pieces, rows, depth = hidden.shape
    x_copies = [
        pltpu.make_async_copy(x.at[:, pl.ds(i * depth, depth)], hidden.at[i], x_sems.at[i]) for i in range(pieces)
    ]
    w_copies = weight_copies(0, wq, wk, wv, wq_buf, wkv_buf, w_sems)
    cache_copies = cache_loads(0, k_cache, v_cache, k_vmem, v_vmem, cache_sems)
    for i in range(pieces):
        x_copies[i].start()
        w_copies[i].start()
    signal_all(place)
    w_copies[pieces].start()
    w_copies[pieces + 1].start()
    for copy in cache_copies:
        copy.start()
    for i in range(pieces):
        x_copies[i].wait()
        w_copies[i].wait()
        add_query(i, i == 0, hidden, wq_buf, q_acc)
    wait_all(place)
    outgoing = exchange_query(place, q_acc, q_send, q_out, q_ssem, q_rsem)
    chip_rows = residual.shape[1]
    for j in range(CHUNKS):
        residual[j] = hidden[place.half * CHUNKS + j, aligned(place.chip, chip_rows), :]
    w_copies[pieces].wait()
    w_copies[pieces + 1].wait()
    new_rows(place, hidden, wkv_buf, kv_new)
    for copy in query_copies(place, q_send, q_out, q_ssem, q_rsem, True):
        copy.wait_recv()
    for copy in outgoing:
        copy.wait_send()
    for copy in cache_copies:
        copy.wait()


def mix_kernel(count, last, layer, *refs):
    refs = list(refs)
    take = lambda k: [refs.pop(0) for _ in range(k)]
    context, residual, wo = take(3)
    if not last:
        wq, wk, wv, k_cache, v_cache = take(5)
        q_out, kv_new, next_residual, k_vmem, v_vmem = take(5)
    else:
        (hidden,) = take(1)
    c_recv, wo_far, wo_own, p_send, p_recv, total, s1_recv, comb, s2_left, s2_right = take(10)
    wo_sems, c_ssem, c_rsem, p_ssem, p_rsem, s1_ssem, s1_rsem = take(7)
    s2_ssem, s2_rsem, ag_ssem, ag_rsem, d2d_ssem, d2d_rsem = take(6)
    if not last:
        hidden, wq_buf, wkv_buf, q_acc, q_send, w_sems, cache_sems, q_ssem, q_rsem = take(9)
    place = Place(count)
    heads, rows, head_dim = c_recv.shape
    local_rows = rows // count
    chip_rows = rows // CHIPS
    depth = total.shape[-1]

    signal_all(place)
    wo_copies = []
    for j in range(CHUNKS):
        wo_copies.append(pltpu.make_async_copy(
            wo.at[layer, :, aligned((1 - place.half) * CHUNKS + j, depth)], wo_far.at[j], wo_sems.at[j]))
    for j in range(CHUNKS):
        wo_copies.append(pltpu.make_async_copy(
            wo.at[layer, :, aligned(place.half * CHUNKS + j, depth)], wo_own.at[j], wo_sems.at[CHUNKS + j]))
    for copy in wo_copies:
        copy.start()
    if not last:
        w_copies = weight_copies(layer + 1, wq, wk, wv, wq_buf, wkv_buf, w_sems)
        cache_copies = cache_loads(layer + 1, k_cache, v_cache, k_vmem, v_vmem, cache_sems)
        for copy in w_copies + cache_copies:
            copy.start()

    c_recv[:, aligned(place.me, local_rows), :] = context[pl.ds(place.me * heads, heads)]
    wait_all(place)

    def context_copy(offset, source):
        target = place.peer(offset)
        return remote(
            context.at[pl.ds(target * heads, heads)], c_recv.at[:, aligned(source, local_rows), :],
            c_ssem.at[offset], c_rsem.at[offset], target)

    sends = []

    def send(copy):
        copy.start()
        sends.append(copy)

    for offset in send_order(count):
        send(context_copy(offset, place.me))
    for offset in range(1, count):
        context_copy(offset, place.origin(offset)).wait_recv()

    def product(weights):
        acc = None
        for pair in range(heads // 2):
            lhs = jnp.concatenate([c_recv[2 * pair], c_recv[2 * pair + 1]], axis=1)
            part = jnp.dot(lhs, weights[pl.ds(pair * 2 * head_dim, 2 * head_dim), :], preferred_element_type=F32)
            acc = part if acc is None else acc + part
        return acc

    def pair_copy(j):
        return remote(p_send.at[j], p_recv.at[j], p_ssem.at[j], p_rsem.at[j], place.sibling)

    def block(chip):
        return aligned(chip, chip_rows)

    for j in range(CHUNKS):
        wo_copies[j].wait()
        p_send[j] = product(wo_far.at[j])
        send(pair_copy(j))

    def step_one(j):
        target = place.to_right if j % 2 == 0 else place.to_left
        if j >= RELAYED:
            target = place.across * 2 + place.core
        return remote(total.at[j, block(place.across), :], s1_recv.at[j], s1_ssem.at[j], s1_rsem.at[j], target)

    def step_two(j, rightward, source):
        target = place.to_right if rightward else place.to_left
        inbox = s2_left if rightward else s2_right
        slot = j if rightward else CHUNKS + j
        return remote(source, inbox.at[j], s2_ssem.at[slot], s2_rsem.at[slot], target)

    def direct(j):
        for rightward in (j % 2 == 1, j % 2 == 0) if j >= RELAYED else (j % 2 == 1,):
            send(step_two(j, rightward, total.at[j, block(place.right if rightward else place.left), :]))

    def combine(j):
        step_one(j).wait_recv()
        rightward = j % 2 == 0
        comb[j] = total[j, block(place.right if rightward else place.left), :] + s1_recv[j]
        send(step_two(j, rightward, comb.at[j]))

    for j in range(CHUNKS):
        wo_copies[CHUNKS + j].wait()
        total[j] = product(wo_own.at[j])
    pending = []
    for j in range(CHUNKS):
        pair_copy(j).wait_recv()
        total[j] += p_recv[j]
        send(step_one(j))
        while pending:
            direct(pending.pop())
        if 0 < j < RELAYED:
            pending.append(j)
        else:
            direct(j)
    for j in range(min(RELAYED, 2)):
        combine(j)
    while pending:
        direct(pending.pop())
    for j in range(2, RELAYED):
        combine(j)

    def piece(half, j):
        return half * CHUNKS + j

    def region(half, j, chip):
        if last:
            return hidden.at[block(chip), aligned(piece(half, j), depth)]
        return hidden.at[piece(half, j), block(chip), :]

    def gather_copy(j, way, chip):
        target = (place.to_right, place.to_left, place.across * 2 + place.core)[way]
        part = region(place.half, j, chip)
        slot = way * CHUNKS + j
        return remote(part, part, ag_ssem.at[slot], ag_rsem.at[slot], target)

    def forward_copy(j, chip):
        target = place.to_right if j % 2 == 0 else place.to_left
        part = region(place.half, j, chip)
        return remote(part, part, ag_ssem.at[2 * CHUNKS + j], ag_rsem.at[2 * CHUNKS + j], target)

    def twin_copy(j, half):
        part = hidden.at[:, aligned(piece(half, j), depth)] if last else hidden.at[piece(half, j)]
        return remote(part, part, d2d_ssem.at[j], d2d_rsem.at[j], place.sibling)

    def finish(j):
        step_two(j, True, comb.at[j]).wait_recv()
        step_two(j, False, comb.at[j]).wait_recv()
        summed = total[j, block(place.chip), :] + s2_left[j] + s2_right[j]
        if j >= RELAYED:
            step_one(j).wait_recv()
            summed = summed + s1_recv[j]
        value = (residual[j].astype(F32) + summed).astype(BF16)
        if last:
            hidden[block(place.chip), aligned(piece(place.half, j), depth)] = value
        else:
            hidden[piece(place.half, j), block(place.chip), :] = value
            next_residual[j] = value
        if j >= RING:
            send(gather_copy(j, 2, place.chip))
        send(gather_copy(j, 0, place.chip))
        send(gather_copy(j, 1, place.chip))

    def pass_on(j):
        gather_copy(j, 0, place.left).wait_recv()
        if j < RING and j % 2 == 0:
            send(forward_copy(j, place.left))
        gather_copy(j, 1, place.right).wait_recv()
        if j < RING and j % 2 == 1:
            send(forward_copy(j, place.right))

    def far_block(j):
        gather_copy(j, 2, place.across).wait_recv()
        send(twin_copy(j, place.half))

    for j in range(CHUNKS):
        finish(j)
    for j in range(RING):
        pass_on(j)
    order = list(range(RING, CHUNKS)) + list(range(RING))
    for j in order:
        if j >= RING:
            pass_on(j)
        far_block(j)
        if not last:
            for copy in w_copies if j == order[0] else ():
                copy.wait()
            add_query(piece(place.half, j), j == order[0], hidden, wq_buf, q_acc)
    for j in order:
        twin_copy(j, 1 - place.half).wait_recv()
        if not last:
            add_query(piece(1 - place.half, j), False, hidden, wq_buf, q_acc)
    if not last:
        outgoing = exchange_query(place, q_acc, q_send, q_out, q_ssem, q_rsem)
        new_rows(place, hidden, wkv_buf, kv_new)
        for copy in query_copies(place, q_send, q_out, q_ssem, q_rsem, True):
            copy.wait_recv()
        sends.extend(outgoing)
        for copy in cache_copies:
            copy.wait()
    for copy in sends:
        copy.wait_send()


GROUP = 8
SHORT = 256


def attention_kernel(layer, *refs):
    all_lens, q, kv_new, k_in, v_in = refs[:5]
    refs = refs[5:]
    if layer > 0:
        refs = refs[2:]
    k_out, v_out, k_buf, v_buf, context, q_rows, c_rows, sems = refs
    del k_in, v_in
    heads, local_rows, head_dim = q.shape
    seq_len = k_buf.shape[1]
    tile = 16
    first_row = lax.axis_index("model") * local_rows

    def length(b):
        return all_lens[first_row + b]

    writes = []
    parts = sems.shape[0] // 2
    step = local_rows // parts
    for i in range(parts):
        for b in range(i * step, (i + 1) * step):
            start = pl.multiple_of((length(b) // tile) * tile, tile)
            here = lax.broadcasted_iota(jnp.int32, (tile, head_dim), 0) == length(b) - start
            for buf, column in ((k_buf, 0), (v_buf, head_dim)):
                fresh = jnp.broadcast_to(kv_new[b:b + 1, column:column + head_dim], (tile, head_dim))
                old = buf[b, pl.ds(start, tile), :].astype(F32)
                buf[b, pl.ds(start, tile), :] = jnp.where(here, fresh, old).astype(BF16)
        part = pl.ds(i * step, step)
        writes.append(pltpu.make_async_copy(k_buf.at[part], k_out.at[layer, part], sems.at[2 * i]))
        writes.append(pltpu.make_async_copy(v_buf.at[part], v_out.at[layer, part], sems.at[2 * i + 1]))
        if i > 0:
            writes[2 * i - 2].start()
            writes[2 * i - 1].start()
    q_rows[...] = q[...].astype(F32).reshape(heads * local_rows, head_dim)
    writes[-2].start()
    writes[-1].start()

    def attend(members, span):
        rows = [pl.ds(b, heads, stride=local_rows) for b in members]
        scores = [
            lax.dot_general(
                q_rows[r, :].astype(BF16), k_buf[b, pl.ds(0, span), :], (((1,), (1,)), ((), ())),
                preferred_element_type=F32)
            for b, r in zip(members, rows)
        ]
        positions = lax.broadcasted_iota(jnp.int32, (heads, span), 1)
        scores = [jnp.where(positions <= length(b), s * (head_dim ** -0.5), -jnp.inf) for b, s in zip(members, scores)]
        tops = [jnp.max(s, axis=1, keepdims=True) for s in scores]
        powers = [jnp.exp(s - t) for s, t in zip(scores, tops)]
        sums = [jnp.sum(p, axis=1, keepdims=True) for p in powers]
        weights = [(p / t).astype(BF16) for p, t in zip(powers, sums)]
        outs = [
            jnp.dot(w, v_buf[b, pl.ds(0, span), :], preferred_element_type=F32) for b, w in zip(members, weights)
        ]
        for r, out in zip(rows, outs):
            c_rows[r, :] = out.astype(BF16).astype(F32)

    for first in range(0, local_rows, GROUP):
        attend(list(range(first, first + GROUP)), SHORT)

    spans = []
    span = 2 * SHORT
    while span < seq_len:
        spans.append(span)
        span *= 2
    spans.append(seq_len)

    def longer(b, _):
        @pl.when(length(b) >= SHORT)
        def _():
            low = SHORT
            for span in spans:
                @pl.when(jnp.logical_and(length(b) >= low, length(b) < span))
                def _(span=span):
                    attend([b], span)
                low = span
        return 0

    lax.fori_loop(0, local_rows, longer, 0)
    context[...] = c_rows[...].reshape(heads, local_rows, head_dim).astype(BF16)
    for copy in writes:
        copy.wait()


def solution(mesh):
    count = mesh.shape["model"]
    assert count == 2 * CHIPS
    row_axes = ("replica", "model")
    cache_spec = P(None, row_axes, None, None)
    DMA = pltpu.SemaphoreType.DMA

    def device_step(x, cache_len, w_query, w_key, w_value, w_out, k_cache, v_cache):
        rows, width = x.shape
        layers, local_rows, seq_len, head_dim = k_cache.shape
        local_width = w_query.shape[-1]
        local_heads = local_width // head_dim
        heads = local_heads * count
        pieces = 2 * CHUNKS
        depth = width // pieces
        chip_rows = rows // CHIPS
        w_query, w_key, w_value, w_out = map(to_hbm, (w_query, w_key, w_value, w_out))
        x, k_cache, v_cache = map(to_hbm, (x, k_cache, v_cache))

        project_out = (
            pltpu.VMEM((heads, local_rows, head_dim), BF16),
            pltpu.VMEM((local_rows, 2 * head_dim), F32),
            pltpu.VMEM((CHUNKS, chip_rows, depth), BF16),
            pltpu.VMEM(k_cache.shape[1:], BF16),
            pltpu.VMEM(v_cache.shape[1:], BF16),
        )
        project_scratch = [
            pltpu.VMEM((pieces, rows, depth), BF16),
            pltpu.VMEM((width, local_width), BF16),
            pltpu.VMEM((width, 2 * head_dim), BF16),
            pltpu.VMEM((rows, local_width), F32),
            pltpu.VMEM((local_heads, rows, head_dim), BF16),
        ]
        project_sems = [DMA((pieces + 2,)), DMA((2 * PARTS,)), DMA((count,)), DMA((count,))]
        mix_scratch = [
            pltpu.VMEM((local_heads, rows, head_dim), BF16),
            pltpu.VMEM((CHUNKS, local_width, depth), BF16),
            pltpu.VMEM((CHUNKS, local_width, depth), BF16),
            pltpu.VMEM((CHUNKS, rows, depth), F32),
            pltpu.VMEM((CHUNKS, rows, depth), F32),
            pltpu.VMEM((CHUNKS, rows, depth), F32),
            pltpu.VMEM((CHUNKS, chip_rows, depth), F32),
            pltpu.VMEM((CHUNKS, chip_rows, depth), F32),
            pltpu.VMEM((CHUNKS, chip_rows, depth), F32),
            pltpu.VMEM((CHUNKS, chip_rows, depth), F32),
            DMA((pieces,)), DMA((count,)), DMA((count,)), DMA((CHUNKS,)), DMA((CHUNKS,)), DMA((CHUNKS,)), DMA((CHUNKS,)),
            DMA((2 * CHUNKS,)), DMA((2 * CHUNKS,)), DMA((3 * CHUNKS,)), DMA((3 * CHUNKS,)),
            DMA((CHUNKS,)), DMA((CHUNKS,)),
        ]

        def params(collective_id, limit):
            return pltpu.CompilerParams(collective_id=collective_id, has_side_effects=True, vmem_limit_bytes=limit * MIB)

        query, kv_new, residual, k_vmem, v_vmem = pl.pallas_call(
            functools.partial(first_kernel, count),
            out_shape=project_out,
            in_specs=[ANY_SPEC] * 6,
            out_specs=(VMEM_SPEC,) * 5,
            scratch_shapes=project_scratch + [DMA((pieces,))] + project_sems,
            compiler_params=params(0, 16),
            name="first",
        )(x, w_query, w_key, w_value, k_cache, v_cache)

        k_new_cache = v_new_cache = None
        for layer in range(layers):
            last = layer == layers - 1
            operands = [cache_len, query, kv_new, k_vmem, v_vmem]
            specs = [SMEM_SPEC] + [VMEM_SPEC] * 4
            aliases = {3: 2, 4: 3}
            if layer > 0:
                operands += [k_new_cache, v_new_cache]
                specs += [ANY_SPEC] * 2
                aliases |= {5: 0, 6: 1}
            k_new_cache, v_new_cache, _, _, context = pl.pallas_call(
                functools.partial(attention_kernel, layer),
                out_shape=(
                    pltpu.HBM(k_cache.shape, BF16),
                    pltpu.HBM(v_cache.shape, BF16),
                    pltpu.VMEM(k_cache.shape[1:], BF16),
                    pltpu.VMEM(v_cache.shape[1:], BF16),
                    pltpu.VMEM((heads, local_rows, head_dim), BF16),
                ),
                in_specs=specs,
                out_specs=(ANY_SPEC, ANY_SPEC, VMEM_SPEC, VMEM_SPEC, VMEM_SPEC),
                input_output_aliases=aliases,
                scratch_shapes=[
                    pltpu.VMEM((heads * local_rows, head_dim), F32),
                    pltpu.VMEM((heads * local_rows, head_dim), F32),
                    DMA((2 * PARTS,)),
                ],
                compiler_params=pltpu.CompilerParams(vmem_limit_bytes=16 * MIB),
                name=f"attend{layer}",
            )(*operands)
            if not last:
                query, kv_new, residual, k_vmem, v_vmem = pl.pallas_call(
                    functools.partial(mix_kernel, count, False, layer),
                    out_shape=project_out,
                    in_specs=[VMEM_SPEC] * 2 + [ANY_SPEC] * 6,
                    out_specs=(VMEM_SPEC,) * 5,
                    scratch_shapes=mix_scratch + project_scratch + project_sems,
                    compiler_params=params(1 + layer, 28),
                    name=f"mix{layer}",
                )(context, residual, w_out, w_query, w_key, w_value, k_cache, v_cache)
            else:
                hidden = pl.pallas_call(
                    functools.partial(mix_kernel, count, True, layer),
                    out_shape=pltpu.VMEM((rows, width), BF16),
                    in_specs=[VMEM_SPEC] * 2 + [ANY_SPEC],
                    out_specs=VMEM_SPEC,
                    scratch_shapes=mix_scratch,
                    compiler_params=params(1 + layer, 20),
                    name=f"mix{layer}",
                )(context, residual, w_out)
        return hidden, k_new_cache, v_new_cache

    return jax.shard_map(
        device_step,
        mesh=mesh,
        in_specs=(P("replica", None), P("replica"), P(None, None, "model"), P(), P(), P(None, "model", None), cache_spec, cache_spec),
        out_specs=(P("replica", None), cache_spec, cache_spec),
        check_vma=False,
    )
```

```python
import functools

import jax
import jax.numpy as jnp
from jax import lax
from jax.experimental import pallas as pl
from jax.experimental.pallas import tpu as pltpu
from jax.sharding import PartitionSpec as P

MESH = pl.DeviceIdType.MESH
F32 = jnp.float32
BF16 = jnp.bfloat16
CHIPS = 4
CHUNKS = 4
PARTS = 8
RING = 0
RELAYED = 4
MIB = 1 << 20

ANY_SPEC = pl.BlockSpec(memory_space=pltpu.HBM)
VMEM_SPEC = pl.BlockSpec(memory_space=pltpu.VMEM)
SMEM_SPEC = pl.BlockSpec(memory_space=pltpu.SMEM)


def to_hbm(value):
    return pltpu.with_memory_space_constraint(value, pltpu.HBM)


def to_vmem(value):
    return pltpu.with_memory_space_constraint(value, pltpu.VMEM)


def aligned(index, size):
    return pl.ds(pl.multiple_of(index * size, size), size)


class Place:
    def __init__(self, count):
        self.count = count
        self.me = lax.axis_index("model")
        self.chip = self.me // 2
        self.core = self.me % 2
        self.right = (self.chip + 1) % CHIPS
        self.left = (self.chip + CHIPS - 1) % CHIPS
        self.across = (self.chip + 2) % CHIPS
        self.half = (self.core + self.chip) % 2
        self.to_right = self.right * 2 + 1 - self.core
        self.to_left = self.left * 2 + 1 - self.core
        self.sibling = self.chip * 2 + (1 - self.core)

    def peer(self, offset):
        return (self.me + offset) % self.count

    def origin(self, offset):
        return (self.me + self.count - offset) % self.count


def remote(src, dst, send_sem, recv_sem, device):
    return pltpu.make_async_remote_copy(
        src_ref=src, dst_ref=dst, send_sem=send_sem, recv_sem=recv_sem,
        device_id={"model": device}, device_id_type=MESH)


def signal_all(place):
    barrier = pltpu.get_barrier_semaphore()
    for offset in send_order(place.count):
        pl.semaphore_signal(barrier, inc=1, device_id={"model": place.peer(offset)}, device_id_type=MESH)


def wait_all(place):
    pl.semaphore_wait(pltpu.get_barrier_semaphore(), place.count - 1)


def weight_copies(layer, wq, wk, wv, wq_buf, wkv_buf, sems):
    pieces = sems.shape[0] - 2
    depth = wq_buf.shape[0] // pieces
    head_dim = wk.shape[-1]
    copies = [
        pltpu.make_async_copy(wq.at[layer, pl.ds(i * depth, depth), :], wq_buf.at[pl.ds(i * depth, depth), :], sems.at[i])
        for i in range(pieces)
    ]
    copies.append(pltpu.make_async_copy(wk.at[layer], wkv_buf.at[:, pl.ds(0, head_dim)], sems.at[pieces]))
    copies.append(pltpu.make_async_copy(wv.at[layer], wkv_buf.at[:, pl.ds(head_dim, head_dim)], sems.at[pieces + 1]))
    return copies


def cache_loads(layer, k_cache, v_cache, k_vmem, v_vmem, sems):
    parts = sems.shape[0] // 2
    step = k_vmem.shape[0] // parts
    copies = []
    for i in range(parts):
        part = pl.ds(i * step, step)
        copies.append(pltpu.make_async_copy(k_cache.at[layer, part], k_vmem.at[part], sems.at[2 * i]))
        copies.append(pltpu.make_async_copy(v_cache.at[layer, part], v_vmem.at[part], sems.at[2 * i + 1]))
    return copies


def add_query(piece, first, hidden, wq_buf, q_acc):
    depth = hidden.shape[-1]
    part = jnp.dot(hidden[piece], wq_buf[aligned(piece, depth), :], preferred_element_type=F32)
    q_acc[...] = part if first else q_acc[...] + part


def new_rows(place, hidden, wkv_buf, kv_new):
    pieces, rows, depth = hidden.shape
    local_rows = rows // place.count
    total = None
    for piece in range(pieces):
        mine = hidden[piece, aligned(place.me, local_rows), :]
        part = jnp.dot(mine, wkv_buf[pl.ds(piece * depth, depth), :], preferred_element_type=F32)
        total = part if total is None else total + part
    kv_new[...] = total.astype(BF16).astype(F32)


def query_copies(place, q_send, q_out, send_sems, recv_sems, incoming):
    heads = q_send.shape[0]
    local_rows = q_out.shape[1]
    copies = []
    for offset in range(1, place.count):
        source = place.origin(offset) if incoming else place.me
        target = place.peer(offset)
        copies.append(remote(
            q_send.at[:, aligned(target, local_rows), :], q_out.at[pl.ds(source * heads, heads)],
            send_sems.at[offset], recv_sems.at[offset], target))
    return copies


def send_order(count):
    return sorted(range(1, count), key=lambda offset: -min(offset, count - offset))


def exchange_query(place, q_acc, q_send, q_out, send_sems, recv_sems):
    heads, rows, head_dim = q_send.shape
    local_rows = q_out.shape[1]
    for head in range(heads):
        q_send[head] = q_acc[:, head * head_dim:(head + 1) * head_dim].astype(BF16)
    outgoing = query_copies(place, q_send, q_out, send_sems, recv_sems, False)
    for offset in send_order(place.count):
        outgoing[offset - 1].start()
    q_out[pl.ds(place.me * heads, heads)] = q_send[:, aligned(place.me, local_rows), :]
    return outgoing


def first_kernel(count, x, wq, wk, wv, k_cache, v_cache,
                 q_out, kv_new, residual, k_vmem, v_vmem,
                 hidden, wq_buf, wkv_buf, q_acc, q_send,
                 x_sems, w_sems, cache_sems, q_ssem, q_rsem):
    place = Place(count)
    pieces, rows, depth = hidden.shape
    x_copies = [
        pltpu.make_async_copy(x.at[:, pl.ds(i * depth, depth)], hidden.at[i], x_sems.at[i]) for i in range(pieces)
    ]
    w_copies = weight_copies(0, wq, wk, wv, wq_buf, wkv_buf, w_sems)
    cache_copies = cache_loads(0, k_cache, v_cache, k_vmem, v_vmem, cache_sems)
    for i in range(pieces):
        x_copies[i].start()
        w_copies[i].start()
    signal_all(place)
    w_copies[pieces].start()
    w_copies[pieces + 1].start()
    for copy in cache_copies:
        copy.start()
    for i in range(pieces):
        x_copies[i].wait()
        w_copies[i].wait()
        add_query(i, i == 0, hidden, wq_buf, q_acc)
    wait_all(place)
    outgoing = exchange_query(place, q_acc, q_send, q_out, q_ssem, q_rsem)
    chip_rows = residual.shape[1]
    for j in range(CHUNKS):
        residual[j] = hidden[place.half * CHUNKS + j, aligned(place.chip, chip_rows), :]
    w_copies[pieces].wait()
    w_copies[pieces + 1].wait()
    new_rows(place, hidden, wkv_buf, kv_new)
    for copy in query_copies(place, q_send, q_out, q_ssem, q_rsem, True):
        copy.wait_recv()
    for copy in outgoing:
        copy.wait_send()
    for copy in cache_copies:
        copy.wait()


def mix_kernel(count, last, layer, *refs):
    refs = list(refs)
    take = lambda k: [refs.pop(0) for _ in range(k)]
    context, residual, wo = take(3)
    if not last:
        wq, wk, wv, k_cache, v_cache = take(5)
        q_out, kv_new, next_residual, k_vmem, v_vmem = take(5)
    else:
        (hidden,) = take(1)
    c_recv, wo_far, wo_own, p_send, p_recv, total, s1_recv, comb, s2_left, s2_right = take(10)
    wo_sems, c_ssem, c_rsem, p_ssem, p_rsem, s1_ssem, s1_rsem = take(7)
    s2_ssem, s2_rsem, ag_ssem, ag_rsem, d2d_ssem, d2d_rsem = take(6)
    if not last:
        hidden, wq_buf, wkv_buf, q_acc, q_send, w_sems, cache_sems, q_ssem, q_rsem = take(9)
    place = Place(count)
    heads, rows, head_dim = c_recv.shape
    local_rows = rows // count
    chip_rows = rows // CHIPS
    depth = total.shape[-1]

    signal_all(place)
    wo_copies = []
    for j in range(CHUNKS):
        wo_copies.append(pltpu.make_async_copy(
            wo.at[layer, :, aligned((1 - place.half) * CHUNKS + j, depth)], wo_far.at[j], wo_sems.at[j]))
    for j in range(CHUNKS):
        wo_copies.append(pltpu.make_async_copy(
            wo.at[layer, :, aligned(place.half * CHUNKS + j, depth)], wo_own.at[j], wo_sems.at[CHUNKS + j]))
    for copy in wo_copies:
        copy.start()
    if not last:
        w_copies = weight_copies(layer + 1, wq, wk, wv, wq_buf, wkv_buf, w_sems)
        cache_copies = cache_loads(layer + 1, k_cache, v_cache, k_vmem, v_vmem, cache_sems)
        for copy in w_copies + cache_copies:
            copy.start()

    c_recv[:, aligned(place.me, local_rows), :] = context[pl.ds(place.me * heads, heads)]
    wait_all(place)

    def context_copy(offset, source):
        target = place.peer(offset)
        return remote(
            context.at[pl.ds(target * heads, heads)], c_recv.at[:, aligned(source, local_rows), :],
            c_ssem.at[offset], c_rsem.at[offset], target)

    sends = []

    def send(copy):
        copy.start()
        sends.append(copy)

    for offset in send_order(count):
        send(context_copy(offset, place.me))
    for offset in range(1, count):
        context_copy(offset, place.origin(offset)).wait_recv()

    def product(weights):
        acc = None
        for pair in range(heads // 2):
            lhs = jnp.concatenate([c_recv[2 * pair], c_recv[2 * pair + 1]], axis=1)
            part = jnp.dot(lhs, weights[pl.ds(pair * 2 * head_dim, 2 * head_dim), :], preferred_element_type=F32)
            acc = part if acc is None else acc + part
        return acc

    def pair_copy(j):
        return remote(p_send.at[j], p_recv.at[j], p_ssem.at[j], p_rsem.at[j], place.sibling)

    def block(chip):
        return aligned(chip, chip_rows)

    for j in range(CHUNKS):
        wo_copies[j].wait()
        p_send[j] = product(wo_far.at[j])
        send(pair_copy(j))

    def step_one(j):
        target = place.to_right if j % 2 == 0 else place.to_left
        if j >= RELAYED:
            target = place.across * 2 + place.core
        return remote(total.at[j, block(place.across), :], s1_recv.at[j], s1_ssem.at[j], s1_rsem.at[j], target)

    def step_two(j, rightward, source):
        target = place.to_right if rightward else place.to_left
        inbox = s2_left if rightward else s2_right
        slot = j if rightward else CHUNKS + j
        return remote(source, inbox.at[j], s2_ssem.at[slot], s2_rsem.at[slot], target)

    def direct(j):
        for rightward in (j % 2 == 1, j % 2 == 0) if j >= RELAYED else (j % 2 == 1,):
            send(step_two(j, rightward, total.at[j, block(place.right if rightward else place.left), :]))

    def combine(j):
        step_one(j).wait_recv()
        rightward = j % 2 == 0
        comb[j] = total[j, block(place.right if rightward else place.left), :] + s1_recv[j]
        send(step_two(j, rightward, comb.at[j]))

    for j in range(CHUNKS):
        wo_copies[CHUNKS + j].wait()
        total[j] = product(wo_own.at[j])
    pending = []
    for j in range(CHUNKS):
        pair_copy(j).wait_recv()
        total[j] += p_recv[j]
        send(step_one(j))
        while pending:
            direct(pending.pop())
        if 0 < j < RELAYED:
            pending.append(j)
        else:
            direct(j)
    while pending:
        direct(pending.pop())
    for j in range(RELAYED):
        combine(j)

    def piece(half, j):
        return half * CHUNKS + j

    def region(half, j, chip):
        if last:
            return hidden.at[block(chip), aligned(piece(half, j), depth)]
        return hidden.at[piece(half, j), block(chip), :]

    def gather_copy(j, way, chip):
        target = (place.to_right, place.to_left, place.across * 2 + place.core)[way]
        part = region(place.half, j, chip)
        slot = way * CHUNKS + j
        return remote(part, part, ag_ssem.at[slot], ag_rsem.at[slot], target)

    def forward_copy(j, chip):
        target = place.to_right if j % 2 == 0 else place.to_left
        part = region(place.half, j, chip)
        return remote(part, part, ag_ssem.at[2 * CHUNKS + j], ag_rsem.at[2 * CHUNKS + j], target)

    def twin_copy(j, half):
        part = hidden.at[:, aligned(piece(half, j), depth)] if last else hidden.at[piece(half, j)]
        return remote(part, part, d2d_ssem.at[j], d2d_rsem.at[j], place.sibling)

    def finish(j):
        step_two(j, True, comb.at[j]).wait_recv()
        step_two(j, False, comb.at[j]).wait_recv()
        summed = total[j, block(place.chip), :] + s2_left[j] + s2_right[j]
        if j >= RELAYED:
            step_one(j).wait_recv()
            summed = summed + s1_recv[j]
        value = (residual[j].astype(F32) + summed).astype(BF16)
        if last:
            hidden[block(place.chip), aligned(piece(place.half, j), depth)] = value
        else:
            hidden[piece(place.half, j), block(place.chip), :] = value
            next_residual[j] = value
        if j >= RING:
            send(gather_copy(j, 2, place.chip))
        send(gather_copy(j, 0, place.chip))
        send(gather_copy(j, 1, place.chip))

    def pass_on(j):
        gather_copy(j, 0, place.left).wait_recv()
        if j < RING and j % 2 == 0:
            send(forward_copy(j, place.left))
        gather_copy(j, 1, place.right).wait_recv()
        if j < RING and j % 2 == 1:
            send(forward_copy(j, place.right))

    def far_block(j):
        gather_copy(j, 2, place.across).wait_recv()
        send(twin_copy(j, place.half))

    for j in range(CHUNKS):
        finish(j)
    for j in range(RING):
        pass_on(j)
    order = list(range(RING, CHUNKS)) + list(range(RING))
    for j in order:
        if j >= RING:
            pass_on(j)
        far_block(j)
        if not last:
            for copy in w_copies if j == order[0] else ():
                copy.wait()
            add_query(piece(place.half, j), j == order[0], hidden, wq_buf, q_acc)
    for j in order:
        twin_copy(j, 1 - place.half).wait_recv()
        if not last:
            add_query(piece(1 - place.half, j), False, hidden, wq_buf, q_acc)
    if not last:
        outgoing = exchange_query(place, q_acc, q_send, q_out, q_ssem, q_rsem)
        new_rows(place, hidden, wkv_buf, kv_new)
        for copy in query_copies(place, q_send, q_out, q_ssem, q_rsem, True):
            copy.wait_recv()
        sends.extend(outgoing)
        for copy in cache_copies:
            copy.wait()
    for copy in sends:
        copy.wait_send()


GROUP = 8
SHORT = 256


def attention_kernel(layer, *refs):
    all_lens, q, kv_new, k_in, v_in = refs[:5]
    refs = refs[5:]
    if layer > 0:
        refs = refs[2:]
    k_out, v_out, k_buf, v_buf, context, q_rows, c_rows, sems = refs
    del k_in, v_in
    heads, local_rows, head_dim = q.shape
    seq_len = k_buf.shape[1]
    tile = 16
    first_row = lax.axis_index("model") * local_rows

    def length(b):
        return all_lens[first_row + b]

    writes = []
    parts = sems.shape[0] // 2
    step = local_rows // parts
    for i in range(parts):
        for b in range(i * step, (i + 1) * step):
            start = pl.multiple_of((length(b) // tile) * tile, tile)
            here = lax.broadcasted_iota(jnp.int32, (tile, head_dim), 0) == length(b) - start
            for buf, column in ((k_buf, 0), (v_buf, head_dim)):
                fresh = jnp.broadcast_to(kv_new[b:b + 1, column:column + head_dim], (tile, head_dim))
                old = buf[b, pl.ds(start, tile), :].astype(F32)
                buf[b, pl.ds(start, tile), :] = jnp.where(here, fresh, old).astype(BF16)
        part = pl.ds(i * step, step)
        writes.append(pltpu.make_async_copy(k_buf.at[part], k_out.at[layer, part], sems.at[2 * i]))
        writes.append(pltpu.make_async_copy(v_buf.at[part], v_out.at[layer, part], sems.at[2 * i + 1]))
        if i > 0:
            writes[2 * i - 2].start()
            writes[2 * i - 1].start()
    q_rows[...] = q[...].astype(F32).reshape(heads * local_rows, head_dim)
    writes[-2].start()
    writes[-1].start()

    def attend(members, span):
        rows = [pl.ds(b, heads, stride=local_rows) for b in members]
        scores = [
            lax.dot_general(
                q_rows[r, :].astype(BF16), k_buf[b, pl.ds(0, span), :], (((1,), (1,)), ((), ())),
                preferred_element_type=F32)
            for b, r in zip(members, rows)
        ]
        positions = lax.broadcasted_iota(jnp.int32, (heads, span), 1)
        scores = [jnp.where(positions <= length(b), s * (head_dim ** -0.5), -jnp.inf) for b, s in zip(members, scores)]
        tops = [jnp.max(s, axis=1, keepdims=True) for s in scores]
        powers = [jnp.exp(s - t) for s, t in zip(scores, tops)]
        sums = [jnp.sum(p, axis=1, keepdims=True) for p in powers]
        weights = [(p / t).astype(BF16) for p, t in zip(powers, sums)]
        outs = [
            jnp.dot(w, v_buf[b, pl.ds(0, span), :], preferred_element_type=F32) for b, w in zip(members, weights)
        ]
        for r, out in zip(rows, outs):
            c_rows[r, :] = out.astype(BF16).astype(F32)

    for first in range(0, local_rows, GROUP):
        attend(list(range(first, first + GROUP)), SHORT)

    spans = []
    span = 2 * SHORT
    while span < seq_len:
        spans.append(span)
        span *= 2
    spans.append(seq_len)

    def longer(b, _):
        @pl.when(length(b) >= SHORT)
        def _():
            low = SHORT
            for span in spans:
                @pl.when(jnp.logical_and(length(b) >= low, length(b) < span))
                def _(span=span):
                    attend([b], span)
                low = span
        return 0

    lax.fori_loop(0, local_rows, longer, 0)
    context[...] = c_rows[...].reshape(heads, local_rows, head_dim).astype(BF16)
    for copy in writes:
        copy.wait()


def solution(mesh):
    count = mesh.shape["model"]
    assert count == 2 * CHIPS
    row_axes = ("replica", "model")
    cache_spec = P(None, row_axes, None, None)
    DMA = pltpu.SemaphoreType.DMA

    def device_step(x, cache_len, w_query, w_key, w_value, w_out, k_cache, v_cache):
        rows, width = x.shape
        layers, local_rows, seq_len, head_dim = k_cache.shape
        local_width = w_query.shape[-1]
        local_heads = local_width // head_dim
        heads = local_heads * count
        pieces = 2 * CHUNKS
        depth = width // pieces
        chip_rows = rows // CHIPS
        w_query, w_key, w_value, w_out = map(to_hbm, (w_query, w_key, w_value, w_out))
        x, k_cache, v_cache = map(to_hbm, (x, k_cache, v_cache))

        project_out = (
            pltpu.VMEM((heads, local_rows, head_dim), BF16),
            pltpu.VMEM((local_rows, 2 * head_dim), F32),
            pltpu.VMEM((CHUNKS, chip_rows, depth), BF16),
            pltpu.VMEM(k_cache.shape[1:], BF16),
            pltpu.VMEM(v_cache.shape[1:], BF16),
        )
        project_scratch = [
            pltpu.VMEM((pieces, rows, depth), BF16),
            pltpu.VMEM((width, local_width), BF16),
            pltpu.VMEM((width, 2 * head_dim), BF16),
            pltpu.VMEM((rows, local_width), F32),
            pltpu.VMEM((local_heads, rows, head_dim), BF16),
        ]
        project_sems = [DMA((pieces + 2,)), DMA((2 * PARTS,)), DMA((count,)), DMA((count,))]
        mix_scratch = [
            pltpu.VMEM((local_heads, rows, head_dim), BF16),
            pltpu.VMEM((CHUNKS, local_width, depth), BF16),
            pltpu.VMEM((CHUNKS, local_width, depth), BF16),
            pltpu.VMEM((CHUNKS, rows, depth), F32),
            pltpu.VMEM((CHUNKS, rows, depth), F32),
            pltpu.VMEM((CHUNKS, rows, depth), F32),
            pltpu.VMEM((CHUNKS, chip_rows, depth), F32),
            pltpu.VMEM((CHUNKS, chip_rows, depth), F32),
            pltpu.VMEM((CHUNKS, chip_rows, depth), F32),
            pltpu.VMEM((CHUNKS, chip_rows, depth), F32),
            DMA((pieces,)), DMA((count,)), DMA((count,)), DMA((CHUNKS,)), DMA((CHUNKS,)), DMA((CHUNKS,)), DMA((CHUNKS,)),
            DMA((2 * CHUNKS,)), DMA((2 * CHUNKS,)), DMA((3 * CHUNKS,)), DMA((3 * CHUNKS,)),
            DMA((CHUNKS,)), DMA((CHUNKS,)),
        ]

        def params(collective_id, limit):
            return pltpu.CompilerParams(collective_id=collective_id, has_side_effects=True, vmem_limit_bytes=limit * MIB)

        query, kv_new, residual, k_vmem, v_vmem = pl.pallas_call(
            functools.partial(first_kernel, count),
            out_shape=project_out,
            in_specs=[ANY_SPEC] * 6,
            out_specs=(VMEM_SPEC,) * 5,
            scratch_shapes=project_scratch + [DMA((pieces,))] + project_sems,
            compiler_params=params(0, 16),
            name="first",
        )(x, w_query, w_key, w_value, k_cache, v_cache)

        k_new_cache = v_new_cache = None
        for layer in range(layers):
            last = layer == layers - 1
            operands = [cache_len, query, kv_new, k_vmem, v_vmem]
            specs = [SMEM_SPEC] + [VMEM_SPEC] * 4
            aliases = {3: 2, 4: 3}
            if layer > 0:
                operands += [k_new_cache, v_new_cache]
                specs += [ANY_SPEC] * 2
                aliases |= {5: 0, 6: 1}
            k_new_cache, v_new_cache, _, _, context = pl.pallas_call(
                functools.partial(attention_kernel, layer),
                out_shape=(
                    pltpu.HBM(k_cache.shape, BF16),
                    pltpu.HBM(v_cache.shape, BF16),
                    pltpu.VMEM(k_cache.shape[1:], BF16),
                    pltpu.VMEM(v_cache.shape[1:], BF16),
                    pltpu.VMEM((heads, local_rows, head_dim), BF16),
                ),
                in_specs=specs,
                out_specs=(ANY_SPEC, ANY_SPEC, VMEM_SPEC, VMEM_SPEC, VMEM_SPEC),
                input_output_aliases=aliases,
                scratch_shapes=[
                    pltpu.VMEM((heads * local_rows, head_dim), F32),
                    pltpu.VMEM((heads * local_rows, head_dim), F32),
                    DMA((2 * PARTS,)),
                ],
                compiler_params=pltpu.CompilerParams(vmem_limit_bytes=16 * MIB),
                name=f"attend{layer}",
            )(*operands)
            if not last:
                query, kv_new, residual, k_vmem, v_vmem = pl.pallas_call(
                    functools.partial(mix_kernel, count, False, layer),
                    out_shape=project_out,
                    in_specs=[VMEM_SPEC] * 2 + [ANY_SPEC] * 6,
                    out_specs=(VMEM_SPEC,) * 5,
                    scratch_shapes=mix_scratch + project_scratch + project_sems,
                    compiler_params=params(1 + layer, 28),
                    name=f"mix{layer}",
                )(context, residual, w_out, w_query, w_key, w_value, k_cache, v_cache)
            else:
                hidden = pl.pallas_call(
                    functools.partial(mix_kernel, count, True, layer),
                    out_shape=pltpu.VMEM((rows, width), BF16),
                    in_specs=[VMEM_SPEC] * 2 + [ANY_SPEC],
                    out_specs=VMEM_SPEC,
                    scratch_shapes=mix_scratch,
                    compiler_params=params(1 + layer, 20),
                    name=f"mix{layer}",
                )(context, residual, w_out)
        return hidden, k_new_cache, v_new_cache

    return jax.shard_map(
        device_step,
        mesh=mesh,
        in_specs=(P("replica", None), P("replica"), P(None, None, "model"), P(), P(), P(None, "model", None), cache_spec, cache_spec),
        out_specs=(P("replica", None), cache_spec, cache_spec),
        check_vma=False,
    )
```
